8 devices in a mesh: dp: 1 (over z), sp: 8 (over y, x, core).
Axes of the slice: x: 2, y: 2, z: 1, core: 2. Of those that a mesh axis runs over, the one named last changes fastest.
Arguments:
- latent: bfloat16 [16, 64, 64, 4], P('dp', 'sp')
- time_emb: bfloat16 [16, 1280], P('dp')
- w_in: bfloat16 [3, 3, 4, 320], replicated
- b_in: bfloat16 [320], replicated
- gn1_scale: bfloat16 [2, 320], replicated
- gn1_shift: bfloat16 [2, 320], replicated
- conv1_w: bfloat16 [2, 3, 3, 320, 320], replicated
- conv1_b: bfloat16 [2, 320], replicated
- temb_w: bfloat16 [2, 1280, 320], replicated
- temb_b: bfloat16 [2, 320], replicated
- gn2_scale: bfloat16 [2, 320], replicated
- gn2_shift: bfloat16 [2, 320], replicated
- conv2_w: bfloat16 [2, 3, 3, 320, 320], replicated
- conv2_b: bfloat16 [2, 320], replicated
- down_w: bfloat16 [3, 3, 320, 320], replicated
- down_b: bfloat16 [320], replicated
Outputs:
- output 1: bfloat16 [16, 64, 64, 320], P('dp', 'sp')
- output 2: bfloat16 [16, 64, 64, 320], P('dp', 'sp')
- output 3: bfloat16 [16, 64, 64, 320], P('dp', 'sp')
- output 4: bfloat16 [16, 32, 32, 320], P('dp', 'sp')
All inputs are finite; a program needn't handle non-finite values.
Results may differ from the reference program's by a relative error of at most 0.0134219.
Values are sent between devices in bfloat16 or wider.
A program may use at most 1 GiB of HBM per device.

```python
import jax
import jax.numpy as jnp
from jax import lax

BATCH = 16
HEIGHT = 64
WIDTH = 64
CHANNELS = 320
TEMB_DIM = 1280
LATENT_CH = 4
GROUPS = 32
LAYERS = 2
GN_EPS = 1e-5


def setup_inputs(seed: int = 0, part: int = 0) -> dict:
    part_keys = jax.random.split(jax.random.fold_in(jax.random.key(seed), part), 4)
    shared_keys = jax.random.split(jax.random.key(seed + 1), 14)
    row_pos = jnp.linspace(-1.0, 1.0, HEIGHT)[None, :, None, None]
    noise_part = jax.random.normal(part_keys[0], (BATCH, HEIGHT, WIDTH, LATENT_CH), jnp.float32)
    row_slope = 1.5 * jax.random.normal(part_keys[1], (BATCH, 1, 1, LATENT_CH), jnp.float32)
    row_curve = jax.random.normal(part_keys[2], (BATCH, 1, 1, LATENT_CH), jnp.float32)
    latent = noise_part + row_slope * row_pos + row_curve * (1.5 * row_pos * row_pos - 0.5)
    time_emb = jax.random.normal(part_keys[3], (BATCH, TEMB_DIM), jnp.float32)
    conv_std = 1.2 * (9 * CHANNELS) ** -0.5

    def draw_w(key_slot, arr_shape, spread, center):
        return (center + spread * jax.random.normal(shared_keys[key_slot], arr_shape, jnp.float32)).astype(jnp.bfloat16)

    return {
        "latent": latent.astype(jnp.bfloat16),
        "time_emb": time_emb.astype(jnp.bfloat16),
        "w_in": draw_w(0, (3, 3, LATENT_CH, CHANNELS), (9 * LATENT_CH) ** -0.5, 0.0),
        "b_in": draw_w(1, (CHANNELS,), 0.5, 0.0),
        "gn1_scale": draw_w(2, (LAYERS, CHANNELS), 0.3, 1.0),
        "gn1_shift": draw_w(3, (LAYERS, CHANNELS), 0.3, 0.0),
        "conv1_w": draw_w(4, (LAYERS, 3, 3, CHANNELS, CHANNELS), conv_std, 0.0),
        "conv1_b": draw_w(5, (LAYERS, CHANNELS), 0.3, 0.0),
        "temb_w": draw_w(6, (LAYERS, TEMB_DIM, CHANNELS), TEMB_DIM ** -0.5, 0.0),
        "temb_b": draw_w(7, (LAYERS, CHANNELS), 0.3, 0.0),
        "gn2_scale": draw_w(8, (LAYERS, CHANNELS), 0.3, 1.0),
        "gn2_shift": draw_w(9, (LAYERS, CHANNELS), 0.3, 0.0),
        "conv2_w": draw_w(10, (LAYERS, 3, 3, CHANNELS, CHANNELS), conv_std, 0.0),
        "conv2_b": draw_w(11, (LAYERS, CHANNELS), 0.3, 0.0),
        "down_w": draw_w(12, (3, 3, CHANNELS, CHANNELS), (9 * CHANNELS) ** -0.5, 0.0),
        "down_b": draw_w(13, (CHANNELS,), 0.3, 0.0),
    }


def conv_same(inputs, kernel, bias_c, stride):
    out_f32 = lax.conv_general_dilated(inputs[None].astype(jnp.float32), kernel.astype(jnp.float32), (stride, stride), ((1, 1), (1, 1)), dimension_numbers=("NHWC", "HWIO", "NHWC"))
    return (out_f32[0] + bias_c.astype(jnp.float32)).astype(jnp.bfloat16)


def norm_silu(values, gain_c, shift_c):
    grouped = values.reshape(values.shape[0] * values.shape[1], GROUPS, CHANNELS // GROUPS)
    grp_mean = jnp.mean(grouped, axis=(0, 2), keepdims=True)
    grp_var = jnp.mean(jnp.square(grouped - grp_mean), axis=(0, 2), keepdims=True)
    normed = ((grouped - grp_mean) * lax.rsqrt(grp_var + GN_EPS)).reshape(values.shape)
    normed = normed * gain_c.astype(jnp.float32) + shift_c.astype(jnp.float32)
    return jax.nn.silu(normed).astype(jnp.bfloat16)


def reference(latent, time_emb, w_in, b_in, gn1_scale, gn1_shift, conv1_w, conv1_b, temb_w, temb_b, gn2_scale, gn2_shift, conv2_w, conv2_b, down_w, down_b):
    layer_params = (gn1_scale, gn1_shift, conv1_w, conv1_b, temb_w, temb_b, gn2_scale, gn2_shift, conv2_w, conv2_b)

    def one_sample(sample):
        latent_s, temb_s = sample
        first_out = conv_same(latent_s, w_in, b_in, 1)
        emb_act = jax.nn.silu(temb_s.astype(jnp.float32)).astype(jnp.bfloat16)

        def layer_step(hidden, params):
            norm_g1, norm_b1, conv_w1, conv_b1, proj_w, proj_b, norm_g2, norm_b2, conv_w2, conv_b2 = params
            branch = conv_same(norm_silu(hidden.astype(jnp.float32), norm_g1, norm_b1), conv_w1, conv_b1, 1)
            emb_proj = jnp.dot(emb_act.astype(jnp.float32), proj_w.astype(jnp.float32)) + proj_b.astype(jnp.float32)
            mixed_in = branch.astype(jnp.float32) + emb_proj
            branch = conv_same(norm_silu(mixed_in, norm_g2, norm_b2), conv_w2, conv_b2, 1)
            hidden = (hidden.astype(jnp.float32) + branch.astype(jnp.float32)).astype(jnp.bfloat16)
            return hidden, hidden

        last_out, per_layer = lax.scan(layer_step, first_out, layer_params)
        return first_out, per_layer, conv_same(last_out, down_w, down_b, 2)

    firsts, layers_out, down_outs = lax.map(one_sample, (latent, time_emb))
    return firsts, layers_out[:, 0], layers_out[:, 1], down_outs
```

```python
import functools

import jax
import jax.numpy as jnp
from jax import lax
from jax.experimental import pallas as pl
from jax.experimental.pallas import tpu as pltpu
from jax.sharding import PartitionSpec as P

F32, BF = jnp.float32, jnp.bfloat16
GN_GROUPS, GN_EPS = 32, 1e-5
NS, ROWS, ROW, LANE, MAIN = 16, 8, 64, 128, 256
NP = ROWS * ROW
CH = 320
CP = CH + ROW
KP = 4 * MAIN
REST = 3 * MAIN
SPARE = 3 * CH
OFF = 8
MESH = pl.DeviceIdType.MESH


def span(i, n=ROW, base=0):
    return slice(base + i * n, base + (i + 1) * n)


def low_half():
    return lax.broadcasted_iota(jnp.int32, (ROW, LANE), 1) < ROW


def widen(p):
    return jnp.concatenate([p, p[..., MAIN:]], -1)


def keep_if(flag, x):
    return jnp.where(jnp.full(x.shape, flag, jnp.int32) > 0, x, 0.0)


def store_rest(L, o, r0, r1, r2):
    low = low_half()
    L[span(o), REST:REST + LANE] = jnp.where(low, r0, r1).astype(BF)
    L[span(o), REST + LANE:] = jnp.where(low, r2, 1.0).astype(BF)


def prep_gen(x_of_row, nrows, a, b, L):
    ha, hb = a * 0.5, b * 0.5
    rest = []
    for r in range(nrows + 2):
        x, flag = x_of_row(r)
        h = x.astype(F32) * ha + hb
        n = h + h * jnp.tanh(h)
        if flag is not None:
            n = keep_if(flag, n)
        main = n[:, :MAIN].astype(BF)
        rest.append(n[:, MAIN:])
        for dy in range(3):
            if 0 <= r - dy < nrows:
                L[span(r - dy), span(dy, MAIN)] = main
        if r >= 2:
            store_rest(L, r - 2, *rest[r - 2:])
        yield


def conv_row(Y, o, zero):
    sub = lax.broadcasted_iota(jnp.int32, (8, LANE), 0)
    top, bot = sub == 0, sub == 7

    def here(k):
        return Y[k, span(o, base=OFF), :]

    def left(k):
        v = Y[k, pl.ds(zero + (OFF - 1 + o * ROW), ROW), :]
        return jnp.concatenate([jnp.where(top, 0.0, v[:8]), v[8:]], 0)

    def right(k):
        v = Y[k, pl.ds(zero + (OFF + 1 + o * ROW), ROW), :]
        return jnp.concatenate([v[:-8], jnp.where(bot, 0.0, v[-8:])], 0)

    out = [left(k) + here(k + 2) + right(k + 4) for k in range(2)]
    mix = jnp.where(low_half(), left(6), here(6))
    return out + [mix + pltpu.roll(mix, ROW, 1) + right(7)]


def dot_chunk(L, W, Y, rows, n):
    r = jnp.dot(L[rows, :], W[:, span(n, 2 * MAIN)], preferred_element_type=F32)
    for k in range(4):
        Y[4 * n + k, OFF + rows.start:OFF + rows.stop, :] = r[:, span(k, LANE)]


def weave(chunks, gens):
    live = list(gens)
    steps = 0
    for c in chunks:
        c()
        steps += 1
        for _ in range(6):
            for g in list(live):
                if next(g, StopIteration) is StopIteration:
                    live.remove(g)
    for g in live:
        for _ in g:
            pass


def lane_left(x, k):
    return pltpu.roll(x, CP - k, 1)


def affine(tots, gain, shift, embs, sp):
    z = [jnp.zeros((4 - len(tots), CP), F32)] * (len(tots) < 4)
    s = jnp.concatenate([jnp.concatenate([t[k:k + 1] for k in range(3)], 1) for t in tots] + z, 0)
    q = jnp.concatenate([jnp.concatenate([t[k + 3:k + 4] for k in range(3)], 1) for t in tots] + z, 0)
    e = jnp.concatenate(list(embs) + z, 0)
    npos = float(sp * NP)
    x = jnp.concatenate([s + npos * e, q + e * (2.0 * s + npos * e)], 0)
    lane = lax.broadcasted_iota(jnp.int32, (8, CP), 1)
    w2 = x + lane_left(x, 1)
    w4 = w2 + lane_left(w2, 2)
    w8 = w4 + lane_left(w4, 4)
    w10 = w8 + lane_left(w2, 8)
    size = CH // GN_GROUPS
    y = jnp.where((lane % size == 0) & (lane < CH), w10, 0.0)
    r2 = y + pltpu.roll(y, 1, 1)
    r4 = r2 + pltpu.roll(r2, 2, 1)
    r8 = r4 + pltpu.roll(r4, 4, 1)
    r = r8 + pltpu.roll(r2, 8, 1)
    r = jnp.where(lane >= CH, pltpu.roll(r, ROW, 1), r) * (1.0 / (npos * size))
    mean, msq = r[:4], r[4:]
    a = gain * lax.rsqrt(msq - mean * mean + GN_EPS)
    return a, shift + a * (e - mean)


def stats_tile(acc, acq):
    parts = [x.sum(0, keepdims=True) for x in acc + acq]
    return jnp.concatenate(parts + [jnp.zeros((2, LANE), F32)], 0)


def add_stats(acc, acq, new):
    for k, x in enumerate(new):
        v = x.astype(F32).reshape(8, 8, LANE)
        acc[k] = acc[k] + v.sum(0)
        acq[k] = acq[k] + (v * v).sum(0)


def no_stats():
    return [jnp.zeros((8, LANE), F32) for _ in range(3)]


def weight_copies(src, W, WR, sem_main, sem_rest):
    for dy in range(3):
        for dx in range(3):
            cols = span(dx, MAIN)
            pltpu.make_async_copy(src.at[dy, dx, :MAIN, :MAIN], W.at[span(dy, MAIN), cols], sem_main).start()
            pltpu.make_async_copy(src.at[dy, dx, MAIN:, :MAIN], W.at[span(dy, base=REST), cols], sem_main).start()
            pltpu.make_async_copy(src.at[dy, dx, :, MAIN:], WR.at[dy * 3 + dx], sem_rest).start()


def weight_finish(W, WR, bias, sem_main, sem_rest):
    main = W.at[:SPARE, :REST]
    pltpu.make_async_copy(main, main, sem_main).wait()
    pltpu.make_async_copy(WR, WR, sem_rest).wait()
    for dy in range(3):
        for part, rows in ((slice(0, MAIN), span(dy, MAIN)), (slice(MAIN, CH), span(dy, base=REST))):
            w0, w1, w2 = (WR[dy * 3 + dx, part, :] for dx in range(3))
            W[rows, REST:REST + LANE] = jnp.concatenate([w0, w1], 1)
            W[rows, REST + LANE:] = jnp.concatenate([w2, w2], 1)
    b = widen(bias.astype(F32))
    gap = jnp.zeros((1, MAIN), F32)
    rest = jnp.where(low_half()[:1], 0.0, b[:, MAIN:])
    row = jnp.concatenate([gap, b[:, :MAIN], gap, rest, gap[:, :LANE]], 1)
    first = lax.broadcasted_iota(jnp.int32, (ROW, KP), 0) == 0
    W[SPARE:, :] = jnp.where(first, row, 0.0).astype(BF)


def mega(sp, q, qx, edges, win, temb, tb, g1, s1, g2, s2, b1, b2, tw, w1, w2, hand, hand0, halo, abo,
         H, U, H2, HS, W, WR, TW, L0, L1, Y0, Y1, ST, RS, AB, EMB, GAIN, HT, HB, HX, LQ,
         wm_sem, wr_sem, tw_sem, q_send, q_recv, st_send, st_recv, up_send, dn_send, x_send, ht_recv, hb_recv, hx_recv, out_sem, fin_sem):
    me, dp = lax.axis_index("sp"), lax.axis_index("dp")
    has_up, has_dn = (me > 0).astype(jnp.int32), (me < sp - 1).astype(jnp.int32)
    held = (H, U, H2, U)

    get_tw = pltpu.make_async_copy(tw, TW, tw_sem)
    get_tw.start()
    for j, src in enumerate((w1.at[0], w2.at[0], w1.at[1])):
        weight_copies(src, W.at[j], WR.at[j], wm_sem.at[j], wr_sem.at[j])

    barrier = pltpu.get_barrier_semaphore()
    for k in range(1, sp):
        pl.semaphore_signal(barrier, inc=1, device_id=(dp, lax.rem(me + k, sp)), device_id_type=MESH)
    pl.semaphore_wait(barrier, sp - 1)

    def remote(src, dst, ssem, rsem, dev):
        return pltpu.make_async_remote_copy(src_ref=src, dst_ref=dst, send_sem=ssem, recv_sem=rsem, device_id=(dp, dev), device_id_type=MESH)

    q_dn = remote(edges.at[0], LQ.at[0], q_send.at[0], q_recv.at[0], me + 1)
    q_up = remote(edges.at[1], LQ.at[1], q_send.at[1], q_recv.at[1], me - 1)

    def if_up(f):
        pl.when(me > 0)(f)

    def if_dn(f):
        pl.when(me < sp - 1)(f)

    if_dn(q_dn.start)
    if_up(q_up.start)

    def up_copy(slot, s):
        return remote(held[slot].at[s, :ROW], HB.at[slot, s], up_send.at[slot, s], hb_recv.at[slot, s], me - 1)

    def dn_copy(slot, s):
        return remote(held[slot].at[s, NP - ROW:], HT.at[slot, s], dn_send.at[slot, s], ht_recv.at[slot, s], me + 1)

    def dx_copy(s):
        return remote(U.at[s, NP - 2 * ROW:NP - ROW], HX.at[s], x_send.at[s], hx_recv.at[s], me + 1)

    def out_copy(slot, s):
        src, dst = ((HS, hand0), None, (H2, hand.at[0]), (U, hand.at[1]))[slot]
        return pltpu.make_async_copy(src.at[s], dst.at[s], out_sem.at[slot, s])

    def send(slot, s):
        for k in range(1, sp):
            remote(ST.at[slot, s], RS.at[slot, s, k - 1], st_send.at[slot, s], st_recv.at[slot, s], lax.rem(me + k, sp)).start()
        if slot != 1:
            out_copy(slot, s).start()
        if_up(lambda: up_copy(slot, s).start())

        def down():
            dn_copy(slot, s).start()
            if slot == 3:
                dx_copy(s).start()
        if_dn(down)

    def wait_stats(slot, s):
        pltpu.make_async_copy(RS.at[slot, s], RS.at[slot, s], st_recv.at[slot, s]).wait()

    def wait_halo(slot, s):
        if_up(lambda: remote(H.at[s, :ROW], HT.at[slot, s], dn_send.at[slot, s], ht_recv.at[slot, s], me).wait_recv())
        if_dn(lambda: remote(H.at[s, :ROW], HB.at[slot, s], up_send.at[slot, s], hb_recv.at[slot, s], me).wait_recv())

    def wait_sent(slot, s):
        if_up(lambda: up_copy(slot, s).wait_send())
        if_dn(lambda: dn_copy(slot, s).wait_send())

    for k, (ref, l) in enumerate(((g1, 0), (g2, 0), (g1, 1), (g2, 1), (s1, 0), (s2, 0), (s1, 1), (s2, 1))):
        GAIN[k:k + 1, :] = widen(ref[l:l + 1, :].astype(F32))
    get_tw.wait()
    x = temb[...].astype(F32)
    act = (x * jax.nn.sigmoid(x)).astype(BF)
    for l in range(2):
        pr = lax.dot_general(act, TW[l], (((1,), (1,)), ((), ())), preferred_element_type=F32)
        EMB[2 * l] = jnp.zeros((NS, CP), F32)
        EMB[2 * l + 1] = widen(pr + tb[l:l + 1, :].astype(F32))

    if_up(q_dn.wait_recv)
    if_dn(q_up.wait_recv)
    lane16 = lax.broadcasted_iota(jnp.int32, (NS, LANE), 1) < ROW

    def first(s):
        e0 = qx[s, :, :LANE].astype(F32)
        e1 = qx[s, :, NP:].astype(F32)
        e0 = jnp.where(lane16, keep_if(has_up, LQ[0, s].astype(F32)), e0).astype(BF)
        e1 = jnp.where(lane16, e1, keep_if(has_dn, LQ[1, s].astype(F32))).astype(BF)
        lhs = jnp.concatenate([
            jnp.concatenate([e0, qx[s, :, LANE:NP]], 1), q[s],
            jnp.concatenate([qx[s, :, LANE:NP], e1], 1)], 0)
        r = lax.dot_general(lhs, win[...], (((0,), (0,)), ((), ())), preferred_element_type=F32)
        acc, acq = no_stats(), no_stats()
        for o in range(ROWS):
            x = r[span(o), :].astype(BF)
            H[s, span(o), :] = x
            HS[s, span(o), :] = x[:, :CH]
            add_stats(acc, acq, [x[:, span(k, LANE)] for k in range(3)])
        ST[0, s] = stats_tile(acc, acq)

    def first_pair(i, carry):
        @pl.when(i > 0)
        def _():
            send(0, 2 * i - 2)
            send(0, 2 * i - 1)
        first(2 * i)
        first(2 * i + 1)
        return carry

    lax.fori_loop(0, NS // 2, first_pair, 0)
    for j in range(3):
        weight_finish(W.at[j], WR.at[j], (b1, b2)[j % 2][j // 2:j // 2 + 1, :], wm_sem.at[j], wr_sem.at[j])
    send(0, NS - 2)
    send(0, NS - 1)

    def total(slot, s):
        t = ST[slot, s]
        for k in range(sp - 1):
            t = t + RS[slot, s, k]
        return t

    def scales(slot, ss):
        a, b = affine([total(slot, s) for s in ss], GAIN[pl.ds(slot, 1)], GAIN[pl.ds(slot + 4, 1)],
                      [EMB[slot, pl.ds(s, 1)] for s in ss], sp)

        def store(dst):
            for k, s in enumerate(ss):
                dst[0, pl.ds(s, 1)] = a[k:k + 1]
                dst[1, pl.ds(s, 1)] = b[k:k + 1]
        return store

    def prep_of(slot, s, L, a, b):
        def row(r):
            if r == 0:
                return HT[slot, s], has_up
            if r == ROWS + 1:
                return HB[slot, s], has_dn
            return held[slot][s, span(r - 1), :], None
        return prep_gen(row, ROWS, a, b, L)

    def epi_gen(j, s, Y, zero):
        acc, acq = no_stats(), no_stats()
        for o in range(ROWS):
            new = [x.astype(BF) for x in conv_row(Y, o, zero)]
            for k in range(3):
                if j == 1:
                    new[k] = (new[k].astype(F32) + H[s, span(o), span(k, LANE)].astype(F32)).astype(BF)
                held[j + 1][s, span(o), span(k, LANE)] = new[k]
            add_stats(acc, acq, new)
            yield
        ST[j + 1, s] = stats_tile(acc, acq)

    def coeffs(s):
        return AB[0, pl.ds(s, 1)], AB[1, pl.ds(s, 1)]

    def half(j, t, Lc, Ln, Yc, Yp, zero):
        nxt = jnp.minimum(t + 1, NS - 1)
        chunks = [functools.partial(dot_chunk, Lc, W.at[j], Yc, slice(0, NP), n) for n in range(2)]
        weave(chunks, (prep_of(j, nxt, Ln, *coeffs(nxt)), epi_gen(j, lax.rem(t + NS - 1, NS), Yp, zero)))

    for s in range(4):
        wait_stats(0, s)
    scales(0, range(4))(AB)
    wait_halo(0, 0)
    for j in range(3):
        if j == 2:
            def sent(s, carry):
                wait_sent(1, s)
                return carry
            lax.fori_loop(0, NS, sent, 0)
        for _ in prep_of(j, 0, L0, *coeffs(0)):
            pass
        if j > 0:
            send(j, NS - 1)

        def body(i, carry, j=j):
            t = 2 * i
            zero = jnp.minimum(i, 0) * 8
            ns = [j * NS + t + k for k in (4, 5)]
            slot = ns[0] // NS
            ss = [lax.rem(n, NS) for n in ns]
            for s in ss:
                pl.when(slot < 3)(functools.partial(wait_stats, slot, s))
            for n in (j * NS + t + 1, j * NS + t + 2):
                wait_halo(n // NS, lax.rem(n, NS))

            @pl.when(i > 0)
            def _():
                send(j + 1, t - 2)

            @pl.when(i > 1)
            def _():
                send(j + 1, t - 3)
            store = scales(jnp.minimum(slot, 2), ss)
            half(j, t, L0, L1, Y0, Y1, zero)
            half(j, t + 1, L1, L0, Y1, Y0, zero)
            store(AB)
            return carry

        lax.fori_loop(0, NS // 2, body, 0)
        send(j + 1, NS - 3)
        send(j + 1, NS - 2)
        for _ in epi_gen(j, NS - 1, Y1, jnp.minimum(me, 0) * 8):
            pass

    send(3, NS - 1)

    def drain(s, carry):
        wait_stats(3, s)
        for slot in range(4):
            pltpu.make_async_copy(RS.at[slot, s], RS.at[slot, s], st_send.at[slot, s]).wait()
            if slot != 1:
                out_copy(slot, s).wait()
                wait_sent(slot, s)
        pl.when(s > 0)(lambda: wait_halo(3, s))
        if_up(lambda: dx_copy(s).wait_recv())
        if_dn(lambda: dx_copy(s).wait_send())
        return carry

    lax.fori_loop(0, NS, drain, 0)
    if_dn(q_dn.wait_send)
    if_up(q_up.wait_send)
    fins = [pltpu.make_async_copy(r, halo.at[k], fin_sem.at[k]) for k, r in enumerate((HT.at[2], HT.at[3], HX, HB.at[3]))]
    for f in fins:
        f.start()
    for k in range(4):
        scales(3, range(4 * k, 4 * k + 4))(abo)
    for f in fins:
        f.wait()


def tail(hand, hand0, halo, ab, b2, bd, w2, dw, h0o, h1o, h2o, do,
         H, U, HA, P0, X2, W, WR, L0, L1, Y0, Y1, O1, O2, OD, DS, in_sem, ha_sem, p_sem, wm_sem, wr_sem, o_sem, od_sem):
    me, sp = lax.axis_index("sp"), lax.axis_size("sp")
    has_up, has_dn = (me > 0).astype(jnp.int32), (me < sp - 1).astype(jnp.int32)
    get_halo = pltpu.make_async_copy(halo, HA, ha_sem)
    get_halo.start()

    def get(k, s):
        return pltpu.make_async_copy(hand.at[k, s], (H, U)[k].at[s], in_sem.at[k, s])

    def take0(s):
        return pltpu.make_async_copy(hand0.at[s], P0.at[s], p_sem.at[s])

    for k in (1, 0):
        get(k, 0).start()
    for j, src in enumerate((w2.at[1], dw)):
        weight_copies(src, W.at[j], WR.at[j], wm_sem.at[j], wr_sem.at[j])

    def fetch(s, carry):
        for k in (1, 0):
            get(k, s).start()
        return carry

    lax.fori_loop(1, NS, fetch, 0)

    def fetch0(s, carry):
        take0(s).start()
        return carry

    lax.fori_loop(0, NS, fetch0, 0)

    def ready(s):
        for k in (1, 0):
            get(k, s).wait()

    def prep_of(s, L):
        def row(r):
            if r < 2:
                return HA[2 - r, s], has_up
            if r == ROWS + 2:
                return HA[3, s], has_dn
            return U[s, span(r - 2), :], None
        return prep_gen(row, ROWS + 1, ab[0, pl.ds(s, 1)], ab[1, pl.ds(s, 1)], L)

    def epi_gen(s, Y, zero):
        for o in range(ROWS + 1):
            t = conv_row(Y, o, zero)
            for k in range(3):
                cols = span(k, LANE)
                old = HA[0, s, :, cols] if o == 0 else H[s, span(o - 1), cols]
                new = old.astype(F32) + t[k].astype(BF).astype(F32)
                new = (keep_if(has_up, new) if o == 0 else new).astype(BF)
                X2[s, span(o), cols] = new
                if o > 0:
                    n = min(LANE, CH - k * LANE)
                    cols = slice(k * LANE, k * LANE + n)
                    O1[s, span(o - 1), cols] = old[:, :n]
                    O2[s, span(o - 1), cols] = new[:, :n]
            yield

    def put(k, s):
        src, dst = ((P0, h0o), (O1, h1o), (O2, h2o))[k]
        return pltpu.make_async_copy(src.at[s], dst.at[s], o_sem.at[k, s])

    def half(t, Lc, Ln, Yc, Yp, zero):
        chunks = [functools.partial(dot_chunk, Lc, W.at[0], Yc, slice(0, NP + ROW), n) for n in range(2)]
        weave(chunks, (prep_of(jnp.minimum(t + 1, NS - 1), Ln), epi_gen(lax.rem(t + NS - 1, NS), Yp, zero)))

    get_halo.wait()
    ready(0)
    for _ in prep_of(0, L0):
        pass
    for j in range(2):
        weight_finish(W.at[j], WR.at[j], (b2[1:2, :], bd[...])[j], wm_sem.at[j], wr_sem.at[j])

    def body(i, carry):
        t = 2 * i
        zero = jnp.minimum(i, 0) * 8
        ready(t + 1)
        pl.when(t + 2 < NS)(lambda: ready(t + 2))
        for n in (t, t + 1):
            take0(n).wait()
            put(0, n).start()
        for n in (t - 3, t - 2):
            @pl.when(n >= 0)
            def _(n=n):
                put(1, n).start()
                put(2, n).start()
        half(t, L0, L1, Y0, Y1, zero)
        half(t + 1, L1, L0, Y1, Y0, zero)
        return carry

    lax.fori_loop(0, NS // 2, body, 0)
    still = jnp.minimum(me, 0) * 8
    for _ in epi_gen(NS - 1, Y1, still):
        pass
    for s in range(NS - 3, NS):
        put(1, s).start()
        put(2, s).start()

    def dprep(s, L):
        for o in range(4):
            xs = [X2[s, span(2 * o + dy), :] for dy in range(3)]
            for dy in range(3):
                L[span(o), span(dy, MAIN)] = xs[dy][:, :MAIN]
            store_rest(L, o, *(x[:, MAIN:].astype(F32) for x in xs))

    def depi(s, Y, zero):
        for o in range(4):
            d = conv_row(Y, o, zero)
            for k in range(3):
                DS[o, k] = d[k]
            parts = [DS[o, k, pl.ds(0, ROW // 2, stride=2), :] for k in range(3)]
            OD[s, span(o, ROW // 2), :] = jnp.concatenate(parts, 1)[:, :CH].astype(BF)

    def dhalf(t, Lc, Ln, Yc, Yp, zero):
        for n in range(2):
            dot_chunk(Lc, W.at[1], Yc, slice(0, NP // 2), n)
        dprep(jnp.minimum(t + 1, NS - 1), Ln)
        depi(lax.rem(t + NS - 1, NS), Yp, zero)

    dprep(0, L0)

    def dbody(i, carry):
        t = 2 * i
        zero = jnp.minimum(i, 0) * 8
        dhalf(t, L0, L1, Y0, Y1, zero)
        dhalf(t + 1, L1, L0, Y1, Y0, zero)
        return carry

    lax.fori_loop(0, NS // 2, dbody, 0)
    depi(NS - 1, Y1, still)
    dout = pltpu.make_async_copy(OD, do, od_sem)
    dout.start()

    def drain(s, carry):
        for k in range(3):
            put(k, s).wait()
        return carry

    lax.fori_loop(0, NS, drain, 0)
    dout.wait()


def solution(mesh):
    sp = mesh.shape["sp"]

    def program(latent, time_emb, w_in, b_in, gn1_scale, gn1_shift, conv1_w, conv1_b, temb_w, temb_b, gn2_scale, gn2_shift, conv2_w, conv2_b, down_w, down_b):
        none = (0, 0)
        lat = jnp.pad(latent.transpose(0, 3, 1, 2), (none, none, none, (1, 1)))
        q = jnp.stack([lat[..., d:d + ROW] for d in range(3)], 1).reshape(NS, 12, NP)
        q = jnp.pad(q, (none, (0, 4), none), constant_values=1)
        qx = jnp.pad(q, (none, none, (ROW, ROW)))
        edges = jnp.stack([jnp.pad(q[..., NP - ROW:], (none, none, (0, ROW))), jnp.pad(q[..., :ROW], (none, none, (ROW, 0)))])
        spare = jnp.zeros((3, 4, CH), BF).at[1, 0].set(b_in)
        win = widen(jnp.concatenate([w_in.reshape(3, 12, CH), spare], 1).reshape(3 * NS, CH))

        dma, vm = pltpu.SemaphoreType.DMA, pltpu.VMEM
        any_, vms = pl.BlockSpec(memory_space=pl.ANY), pl.BlockSpec(memory_space=pltpu.VMEM)
        params = functools.partial(pltpu.CompilerParams, vmem_limit_bytes=66_000_000)

        def big(n=NP, c=CP):
            return vm((NS, n, c), BF)

        def bufs(m):
            return [vm((m, KP), BF)] * 2 + [vm((8, m + 2 * OFF, LANE), F32)] * 2

        def out(*shape):
            return jax.ShapeDtypeStruct(shape, BF)

        hand, hand0, halo, ab = pl.pallas_call(
            functools.partial(mega, sp),
            out_shape=(out(2, NS, NP, CP), out(NS, NP, CH), out(4, NS, ROW, CP), jax.ShapeDtypeStruct((2, NS, CP), F32)),
            in_specs=[vms, vms, any_] + [vms] * 9 + [any_] * 3, out_specs=(any_, any_, any_, vms),
            scratch_shapes=[big(), big(), big(), big(NP, CH), vm((3, KP, KP), BF), vm((3, 9, CH, ROW), BF), vm((2, CH, temb_w.shape[1]), BF)] + bufs(NP)
            + [vm((4, NS, 8, LANE), F32), vm((4, NS, sp - 1, 8, LANE), F32), vm((2, NS, CP), F32), vm((4, NS, CP), F32), vm((8, CP), F32),
               vm((4, NS, ROW, CP), BF), vm((4, NS, ROW, CP), BF), big(ROW), vm((2, NS, NS, LANE), BF),
               dma((3,)), dma((3,)), dma, dma((2,)), dma((2,)), dma((4, NS)), dma((4, NS)), dma((4, NS)), dma((4, NS)), dma((NS,)),
               dma((4, NS)), dma((4, NS)), dma((NS,)), dma((4, NS)), dma((4,))],
            compiler_params=params(collective_id=0, has_side_effects=True), name="mega",
        )(q, qx, edges, win, time_emb, temb_b, gn1_scale, gn1_shift, gn2_scale, gn2_shift, conv1_b, conv2_b, temb_w.transpose(0, 2, 1), conv1_w, conv2_w)
        outs = pl.pallas_call(
            tail,
            out_shape=(out(NS, NP, CH),) * 3 + (out(NS, NP // 4, CH),),
            in_specs=[any_] * 3 + [vms] * 3 + [any_] * 2, out_specs=(any_,) * 4,
            scratch_shapes=[big(), big(), vm((4, NS, ROW, CP), BF), big(NP, CH), big(NP + ROW), vm((2, KP, KP), BF), vm((2, 9, CH, ROW), BF)] + bufs(NP + ROW)
            + [big(NP, CH), big(NP, CH), big(NP // 4, CH), vm((4, 3, ROW, LANE), F32),
               dma((2, NS)), dma, dma((NS,)), dma((2,)), dma((2,)), dma((3, NS)), dma],
            compiler_params=params(), name="tail",
        )(hand, hand0, halo, ab, conv2_b, down_b.reshape(1, CH), conv2_w, down_w)
        return tuple(o.reshape(NS, n, m, CH) for o, n, m in zip(outs, (ROWS,) * 3 + (ROWS // 2,), (ROW,) * 3 + (ROW // 2,)))

    band = P("dp", "sp", None, None)
    return jax.shard_map(program, mesh=mesh, in_specs=(band, P("dp", None)) + (P(),) * 14, out_specs=(band,) * 4, check_vma=False)
```

```python
import functools

import jax
import jax.numpy as jnp
from jax import lax
from jax.experimental import pallas as pl
from jax.experimental.pallas import tpu as pltpu
from jax.sharding import PartitionSpec as P

F32, BF = jnp.float32, jnp.bfloat16
GN_GROUPS, GN_EPS = 32, 1e-5
NS, ROWS, ROW, LANE, MAIN = 16, 8, 64, 128, 256
NP = ROWS * ROW
CH = 320
CP = CH + ROW
KP = 4 * MAIN
REST = 3 * MAIN
SPARE = 3 * CH
OFF = 8
GSIZE = CH // GN_GROUPS
PK = ROW + NS
MESH = pl.DeviceIdType.MESH
DUO, TRI, QUAD = range(2), range(3), range(4)
SLOTS = len(QUAD)
NIL = 0.0
ACC32 = dict(preferred_element_type=F32)
ROWS_DOT, COLS_DOT = ((((k,), (k,)), ((), ())) for k in DUO)


def nil(i):
    return jnp.minimum(i, 0) * OFF


def span(i, n=ROW, base=0):
    return slice(base + i * n, base + (i + 1) * n)


def low_half():
    return lax.broadcasted_iota(jnp.int32, (ROW, LANE), 1) < ROW


def widen(p):
    return jnp.concatenate([p, p[..., MAIN:]], -1)


def keep_if(flag, x):
    return jnp.where(jnp.full(x.shape, flag, jnp.int32) > 0, x, NIL)


def store_rest(L, o, r0, r1, r2):
    low = low_half()
    L[span(o), REST:REST + LANE] = jnp.where(low, r0, r1).astype(BF)
    L[span(o), REST + LANE:] = jnp.where(low, r2, 1.0).astype(BF)


def prep_gen(x_of_row, nrows, a, b, L):
    ha, hb = a * 0.5, b * 0.5
    rest = []
    for r in range(nrows + 2):
        x, flag = x_of_row(r)
        h = x.astype(F32) * ha + hb
        n = h + h * jnp.tanh(h)
        if flag is not None:
            n = keep_if(flag, n)
        main = n[:, :MAIN].astype(BF)
        rest.append(n[:, MAIN:])
        for dy in TRI:
            if 0 <= r - dy < nrows:
                L[span(r - dy), span(dy, MAIN)] = main
        if r >= 2:
            store_rest(L, r - 2, *rest[r - 2:])
        yield


def conv_row(Y, o, zero):
    sub = lax.broadcasted_iota(jnp.int32, (OFF, LANE), 0)
    top, bot = sub == 0, sub == 7

    def here(k):
        return Y[k, span(o, base=OFF), :]

    def left(k):
        v = Y[k, pl.ds(zero + (OFF - 1 + o * ROW), ROW), :]
        return jnp.concatenate([jnp.where(top, 0.0, v[:OFF]), v[OFF:]], 0)

    def right(k):
        v = Y[k, pl.ds(zero + (OFF + 1 + o * ROW), ROW), :]
        return jnp.concatenate([v[:-OFF], jnp.where(bot, 0.0, v[-OFF:])], 0)

    out = [left(k) + here(k + 2) + right(k + 4) for k in DUO]
    mix = jnp.where(low_half(), left(6), here(6))
    return out + [mix + pltpu.roll(mix, ROW, 1) + right(7)]


def dot_chunk(L, W, Y, rows, n):
    r = jnp.dot(L[rows, :], W[:, span(n, 2 * MAIN)], **ACC32)
    for k in QUAD:
        Y[4 * n + k, OFF + rows.start:OFF + rows.stop, :] = r[:, span(k, LANE)]


def weave(chunks, gens):
    live = list(gens)
    steps = 0
    for c in chunks:
        c()
        steps += 1
        for _ in range(6):
            for g in list(live):
                if next(g, StopIteration) is StopIteration:
                    live.remove(g)
    for g in live:
        for _ in g:
            pass


def lane_left(x, k):
    return pltpu.roll(x, CP - k, 1)


def starts(k):
    lane = lax.broadcasted_iota(jnp.int32, (OFF, LANE), 1) + k * LANE
    return (lane % GSIZE == 0) & (lane < CH)


def stacked(rows):
    fill = [jnp.zeros((4 - len(rows), rows[0].shape[1]), F32)] * (len(rows) < 4)
    return jnp.concatenate(list(rows) + fill, 0)


def compact(tiles, embs):
    s = stacked([jnp.concatenate([t[k:k + 1] for k in TRI], 1) for t in tiles])
    q = stacked([jnp.concatenate([t[k + 3:k + 4] for k in TRI], 1) for t in tiles])
    e = stacked(embs)
    x = jnp.concatenate([s + float(NP) * e, q + e * (2.0 * s + float(NP) * e)], 0)
    w2 = x + lane_left(x, 1)
    w4 = w2 + lane_left(w2, 2)
    w8 = w4 + lane_left(w4, 4)
    w10 = w8 + lane_left(w2, 8)
    c = sum(jnp.where(starts(k), w10[:, span(k, LANE)], NIL) for k in TRI)
    return [jnp.concatenate([c[k:k + 1], c[k + 4:k + 5]], 0) for k in range(len(tiles))]


def affine(tots, gain, shift, embs, count):
    x = jnp.concatenate([stacked([t[k:k + 1] for t in tots]) for k in DUO], 0)
    y = jnp.concatenate([jnp.where(starts(k), x, NIL) for k in TRI], 1)
    r2 = y + pltpu.roll(y, 1, 1)
    r4 = r2 + pltpu.roll(r2, 2, 1)
    r8 = r4 + pltpu.roll(r4, 4, 1)
    r = r8 + pltpu.roll(r2, 8, 1)
    lane = lax.broadcasted_iota(jnp.int32, (OFF, CP), 1)
    r = jnp.where(lane >= CH, pltpu.roll(r, ROW, 1), r) * (1.0 / count)
    mean, msq = r[:4], r[4:]
    a = gain * lax.rsqrt(msq - mean * mean + GN_EPS)
    return a, shift + a * (stacked(embs) - mean)


def pack_row(dst, x):
    dst[:ROW, :] = jnp.concatenate(x[:2], 1)
    half = ROW // 2
    p = jnp.where(low_half()[:half], x[2][:half].astype(F32), x[2][half:].astype(F32))
    dst[ROW:, :] = jnp.concatenate([p[:NS], p[NS:]], 1).astype(BF)


def unpack_row(src):
    p = src[ROW:, :].astype(F32)
    p = jnp.concatenate([p[:, :LANE], p[:, LANE:]], 0)
    swap, low = pltpu.roll(p, ROW, 1), low_half()[:ROW // 2]
    rest = jnp.concatenate([jnp.where(low, p, swap), jnp.where(low, swap, p)], 0)
    return jnp.concatenate([src[:ROW, :].astype(F32), rest], 1)


def stats_tile(acc, acq):
    parts = [x.sum(0, keepdims=True) for x in acc + acq]
    return jnp.concatenate(parts + [jnp.zeros((2, LANE), F32)], 0)


def add_stats(acc, acq, new):
    for k, x in enumerate(new):
        v = x.astype(F32).reshape(OFF, OFF, LANE)
        acc[k] = acc[k] + v.sum(0)
        acq[k] = acq[k] + (v * v).sum(0)


def no_stats():
    return [jnp.zeros((OFF, LANE), F32) for _ in TRI]


def weight_copies(src, W, WR, sem_main, sem_rest):
    for dy in TRI:
        for dx in TRI:
            cols = span(dx, MAIN)
            pltpu.make_async_copy(src.at[dy, dx, :MAIN, :MAIN], W.at[span(dy, MAIN), cols], sem_main).start()
            pltpu.make_async_copy(src.at[dy, dx, MAIN:, :MAIN], W.at[span(dy, base=REST), cols], sem_main).start()
            pltpu.make_async_copy(src.at[dy, dx, :, MAIN:], WR.at[dy * 3 + dx], sem_rest).start()


def weight_finish(W, WR, bias, sem_main, sem_rest):
    main = W.at[:SPARE, :REST]
    pltpu.make_async_copy(main, main, sem_main).wait()
    pltpu.make_async_copy(WR, WR, sem_rest).wait()
    for dy in TRI:
        for part, rows in ((slice(0, MAIN), span(dy, MAIN)), (slice(MAIN, CH), span(dy, base=REST))):
            w0, w1, w2 = (WR[dy * 3 + dx, part, :] for dx in TRI)
            W[rows, REST:REST + LANE] = jnp.concatenate([w0, w1], 1)
            W[rows, REST + LANE:] = jnp.concatenate([w2, w2], 1)
    b = widen(bias.astype(F32))
    gap = jnp.zeros((1, MAIN), F32)
    rest = jnp.where(low_half()[:1], 0.0, b[:, MAIN:])
    row = jnp.concatenate([gap, b[:, :MAIN], gap, rest, gap[:, :LANE]], 1)
    first = lax.broadcasted_iota(jnp.int32, (ROW, KP), 0) == 0
    W[SPARE:, :] = jnp.where(first, row, NIL).astype(BF)


def mega(sp, q, wi, bi, temb, tb, g1, s1, g2, s2, b1, b2, tw, w1, w2, hand, hand0, halo, abo,
         H, U, H2, HS, W, WR, TW, WI, L0, L1, Y0, Y1, ST, SG, RS, AB, EMB, GAIN, HT, HB, HX, PT, PB, PX, LQ,
         wm_sem, wr_sem, tw_sem, q_send, q_recv, st_send, st_recv, up_send, dn_send, x_send, ht_recv, hb_recv, hx_recv, out_sem, fin_sem):
    me, dp = lax.axis_index("sp"), lax.axis_index("dp")
    has_up, has_dn = (me > 0).astype(jnp.int32), (me < sp - 1).astype(jnp.int32)
    held = (H, U, H2, U)
    last = NS - 1

    get_tw = pltpu.make_async_copy(tw, TW, tw_sem)
    get_tw.start()
    for j, src in enumerate((w1.at[0], w2.at[0], w1.at[1])):
        weight_copies(src, W.at[j], WR.at[j], wm_sem.at[j], wr_sem.at[j])

    barrier = pltpu.get_barrier_semaphore()
    for k in range(1, sp):
        pl.semaphore_signal(barrier, inc=1, device_id=(dp, lax.rem(me + k, sp)), device_id_type=MESH)
    pl.semaphore_wait(barrier, sp - 1)

    def remote(src, dst, ssem, rsem, dev):
        return pltpu.make_async_remote_copy(src_ref=src, dst_ref=dst, send_sem=ssem, recv_sem=rsem, device_id=(dp, dev), device_id_type=MESH)

    def if_up(f):
        pl.when(me > 0)(f)

    def if_dn(f):
        pl.when(me < sp - 1)(f)

    q_dn = remote(q.at[:, :, NP - LANE:], LQ.at[0], q_send.at[0], q_recv.at[0], me + 1)
    q_up = remote(q.at[:, :, :LANE], LQ.at[1], q_send.at[1], q_recv.at[1], me - 1)
    if_dn(q_dn.start)
    if_up(q_up.start)

    def up_copy(slot, s):
        return remote(PT.at[slot - 1, s], HB.at[slot, s], up_send.at[slot, s], hb_recv.at[slot, s], me - 1)

    def dn_copy(slot, s):
        return remote(PB.at[slot - 1, s], HT.at[slot, s], dn_send.at[slot, s], ht_recv.at[slot, s], me + 1)

    def dx_copy(s):
        return remote(PX.at[s], HX.at[s], x_send.at[s], hx_recv.at[s], me + 1)

    def out_copy(slot, s):
        src, dst = ((HS, hand0), None, (H2, hand.at[0]), (U, hand.at[1]))[slot]
        return pltpu.make_async_copy(src.at[s], dst.at[s], out_sem.at[slot, s])

    def send_sums(slot, s):
        for k in range(1, sp):
            remote(SG.at[slot, s], RS.at[slot, s, k - 1], st_send.at[slot, s], st_recv.at[slot, s], lax.rem(me + k, sp)).start()

    def send_rows(slot, s):
        if slot != 1:
            out_copy(slot, s).start()
        if slot == 0:
            return
        if_up(lambda: up_copy(slot, s).start())

        def down():
            dn_copy(slot, s).start()
            if slot == 3:
                dx_copy(s).start()
        if_dn(down)

    def wait_sums(slot, s):
        pltpu.make_async_copy(RS.at[slot, s], RS.at[slot, s], st_recv.at[slot, s]).wait()

    def wait_rows(slot, s):
        if_up(lambda: remote(PB.at[0, s], HT.at[slot, s], dn_send.at[slot, s], ht_recv.at[slot, s], me).wait_recv())
        if_dn(lambda: remote(PT.at[0, s], HB.at[slot, s], up_send.at[slot, s], hb_recv.at[slot, s], me).wait_recv())

    def squeeze(slot, ss):
        rows = compact([ST[slot, s] for s in ss], [EMB[slot, pl.ds(s, 1)] for s in ss])

        def store():
            for r, s in zip(rows, ss):
                SG[slot, s] = r
        return store

    for k, (ref, l) in enumerate(((g1, 0), (g2, 0), (g1, 1), (g2, 1), (s1, 0), (s2, 0), (s1, 1), (s2, 1))):
        GAIN[k:k + 1, :] = widen(ref[l:l + 1, :].astype(F32))
    WI[...] = jnp.zeros_like(WI)
    for dy in TRI:
        for dx in TRI:
            WI[span(4 * dy + dx, 4), :] = widen(wi[dy, dx].astype(F32))
    WI[NS + 12:NS + 13, :] = widen(bi[...].astype(F32))
    get_tw.wait()
    x = temb[...].astype(F32)
    act = (x * jax.nn.sigmoid(x)).astype(BF)
    for l in DUO:
        pr = lax.dot_general(act, TW[l], COLS_DOT, **ACC32)
        EMB[2 * l] = jnp.zeros((NS, CP), F32)
        EMB[2 * l + 1] = widen(pr + tb[l:l + 1, :].astype(F32))

    if_up(q_dn.wait_recv)
    if_dn(q_up.wait_recv)

    def first(s):
        above, below = keep_if(has_up, LQ[0, s].astype(F32)), keep_if(has_dn, LQ[1, s].astype(F32))
        ext = jnp.concatenate([above, q[s].astype(F32), below], 1)
        mid = pltpu.roll(ext, ext.shape[1] - ROW, 1)
        wide = NP + LANE
        lhs = jnp.concatenate([ext[:, :wide], mid[:, :wide], ext[:, LANE:]], 0).astype(BF)
        r = lax.dot_general(lhs, WI[...].astype(BF), ROWS_DOT, **ACC32)
        acc, acq = no_stats(), no_stats()
        for o in range(ROWS + 2):
            x = r[span(o), :].astype(BF)
            parts = [x[:, span(k, LANE)] for k in TRI]
            if o == 0:
                pack_row(HT.at[0, s], parts)
            elif o > ROWS:
                pack_row(HB.at[0, s], parts)
            else:
                H[s, span(o - 1), :] = x
                HS[s, span(o - 1), :] = x[:, :CH]
                add_stats(acc, acq, parts)
        ST[0, s] = stats_tile(acc, acq)

    def first_pair(i, carry):
        t = 2 * i
        for n in (t - 2, t - 1):
            pl.when(i > 0)(functools.partial(send_rows, 0, n))
            pl.when(i > 1)(functools.partial(send_sums, 0, n - 2))
        store = squeeze(0, [lax.rem(n + NS, NS) for n in (t - 2, t - 1)])
        first(t)
        first(t + 1)
        store()
        return carry

    lax.fori_loop(0, NS // 2, first_pair, 0)
    squeeze(0, (last - 1, last))()
    for j in TRI:
        weight_finish(W.at[j], WR.at[j], (b1, b2)[j % 2][j // 2:j // 2 + 1, :], wm_sem.at[j], wr_sem.at[j])
    for s in range(NS - 4, NS):
        send_sums(0, s)
    for s in (last - 1, last):
        send_rows(0, s)

    def scales(slot, ss):
        tots = []
        for s in ss:
            tots.append(SG[slot, s])
            for k in range(sp - 1):
                tots[-1] = tots[-1] + RS[slot, s, k]
        a, b = affine(tots, GAIN[pl.ds(slot, 1)], GAIN[pl.ds(slot + 4, 1)],
                      [EMB[slot, pl.ds(s, 1)] for s in ss], float(sp * NP * GSIZE))

        def store(dst):
            for k, s in enumerate(ss):
                dst[0, pl.ds(s, 1)] = a[k:k + 1]
                dst[1, pl.ds(s, 1)] = b[k:k + 1]
        return store

    def prep_of(slot, s, L, a, b):
        def row(r):
            if r == 0:
                return unpack_row(HT.at[slot, s]), has_up
            if r == ROWS + 1:
                return unpack_row(HB.at[slot, s]), has_dn
            return held[slot][s, span(r - 1), :], None
        return prep_gen(row, ROWS, a, b, L)

    def epi_gen(j, s, Y, zero):
        acc, acq = no_stats(), no_stats()
        edge = {0: PT.at[j, s], ROWS - 1: PB.at[j, s]}
        if j == 2:
            edge[ROWS - 2] = PX.at[s]
        for o in range(ROWS):
            new = [x.astype(BF) for x in conv_row(Y, o, zero)]
            for k in TRI:
                if j == 1:
                    new[k] = (new[k].astype(F32) + H[s, span(o), span(k, LANE)].astype(F32)).astype(BF)
                held[j + 1][s, span(o), span(k, LANE)] = new[k]
            if o in edge:
                pack_row(edge[o], new)
            add_stats(acc, acq, new)
            yield
        ST[j + 1, s] = stats_tile(acc, acq)

    def coeffs(s):
        return AB[0, pl.ds(s, 1)], AB[1, pl.ds(s, 1)]

    def half(j, t, Lc, Ln, Yc, Yp, zero):
        nxt = jnp.minimum(t + 1, last)
        chunks = [functools.partial(dot_chunk, Lc, W.at[j], Yc, slice(0, NP), n) for n in DUO]
        weave(chunks, (prep_of(j, nxt, Ln, *coeffs(nxt)), epi_gen(j, lax.rem(t + last, NS), Yp, zero)))

    for s in QUAD:
        wait_sums(0, s)
    scales(0, QUAD)(AB)
    still = nil(me)
    for _ in prep_of(0, 0, L0, *coeffs(0)):
        pass
    for j in TRI:
        def body(i, carry, j=j):
            t = 2 * i
            zero = nil(i)
            ns = [j * NS + t + k for k in (4, 5)]
            slot = ns[0] // NS
            ss = [lax.rem(n, NS) for n in ns]
            for s in ss:
                if j < 2:
                    wait_sums(slot, s)
                else:
                    pl.when(slot < 3)(functools.partial(wait_sums, slot, s))
            for k in (1, 2):
                if j > 0:
                    wait_rows((j * NS + t + k) // NS, lax.rem(t + k, NS))
                elif k == 2:
                    pl.when(t + k == NS)(lambda: wait_rows(1, 0))
            for n, m in ((t - 2, 0), (t - 3, 1)):
                pl.when(i > m)(functools.partial(send_rows, j + 1, n))
                pl.when(i > m + 1)(functools.partial(send_sums, j + 1, n - 2))
            store = scales(jnp.minimum(slot, 2), ss)
            store_sums = squeeze(j + 1, [lax.rem(t + NS - k, NS) for k in (3, 2)])
            half(j, t, L0, L1, Y0, Y1, zero)
            half(j, t + 1, L1, L0, Y1, Y0, zero)
            store(AB)
            store_sums()
            return carry

        lax.fori_loop(0, NS // 2, body, 0)
        for s in (last - 2, last - 1):
            send_rows(j + 1, s)
            send_sums(j + 1, s - 2)
        squeeze(j + 1, (last - 2, last - 1))()
        for _ in epi_gen(j, last, Y1, still):
            pass
        if j < 2:
            for _ in prep_of(j + 1, 0, L0, *coeffs(0)):
                pass
        squeeze(j + 1, (last,))()
        for s in range(last - 2, NS):
            send_sums(j + 1, s)
        send_rows(j + 1, last)

    def drain(s, carry):
        wait_sums(3, s)
        for slot in QUAD:
            pltpu.make_async_copy(RS.at[slot, s], RS.at[slot, s], st_send.at[slot, s]).wait()
            if slot != 1:
                out_copy(slot, s).wait()
            if slot > 0:
                if_up(lambda slot=slot: up_copy(slot, s).wait_send())
                if_dn(lambda slot=slot: dn_copy(slot, s).wait_send())
        pl.when(s > 0)(lambda: wait_rows(3, s))
        if_up(lambda: dx_copy(s).wait_recv())
        if_dn(lambda: dx_copy(s).wait_send())
        return carry

    lax.fori_loop(0, NS, drain, 0)
    if_dn(q_dn.wait_send)
    if_up(q_up.wait_send)
    fins = [pltpu.make_async_copy(r, halo.at[k], fin_sem.at[k]) for k, r in enumerate((HT.at[2], HT.at[3], HX, HB.at[3]))]
    for f in fins:
        f.start()
    for k in QUAD:
        scales(3, range(4 * k, 4 * k + 4))(abo)
    for f in fins:
        f.wait()


def tail(hand, hand0, halo, ab, b2, bd, w2, dw, h0o, h1o, h2o, do,
         H, U, HA, P0, X2, W, WR, L0, L1, Y0, Y1, O1, O2, OD, DS, in_sem, ha_sem, p_sem, wm_sem, wr_sem, o_sem, od_sem):
    me, sp = lax.axis_index("sp"), lax.axis_size("sp")
    has_up, has_dn = (me > 0).astype(jnp.int32), (me < sp - 1).astype(jnp.int32)

    def gets(s):
        return ([pltpu.make_async_copy(hand.at[k, s], (H, U)[k].at[s], in_sem.at[k, s]) for k in (1, 0)]
                + [pltpu.make_async_copy(halo.at[k, s], HA.at[k, s], ha_sem.at[k, s]) for k in QUAD])

    def take0(s):
        return pltpu.make_async_copy(hand0.at[s], P0.at[s], p_sem.at[s])

    def fetch(s, carry):
        for c in gets(s):
            c.start()
        return carry

    def ready(s):
        for c in gets(s):
            c.wait()

    fetch(0, 0)
    weight_copies(w2.at[1], W.at[0], WR.at[0], wm_sem.at[0], wr_sem.at[0])
    lax.fori_loop(1, 4, fetch, 0)

    def prep_of(s, L):
        def row(r):
            if r < 2:
                return unpack_row(HA.at[2 - r, s]), has_up
            if r == ROWS + 2:
                return unpack_row(HA.at[3, s]), has_dn
            return U[s, span(r - 2), :], None
        return prep_gen(row, ROWS + 1, ab[0, pl.ds(s, 1)], ab[1, pl.ds(s, 1)], L)

    def epi_gen(s, Y, zero):
        for o in range(ROWS + 1):
            t = conv_row(Y, o, zero)
            edge = unpack_row(HA.at[0, s]) if o == 0 else None
            for k in TRI:
                cols = span(k, LANE)
                old = edge[:, cols] if o == 0 else H[s, span(o - 1), cols]
                new = old.astype(F32) + t[k].astype(BF).astype(F32)
                new = (keep_if(has_up, new) if o == 0 else new).astype(BF)
                X2[s, span(o), cols] = new
                if o > 0:
                    n = min(LANE, CH - k * LANE)
                    cols = slice(k * LANE, k * LANE + n)
                    O1[s, span(o - 1), cols] = old[:, :n]
                    O2[s, span(o - 1), cols] = new[:, :n]
            yield

    def put(k, s):
        src, dst = ((P0, h0o), (O1, h1o), (O2, h2o))[k]
        return pltpu.make_async_copy(src.at[s], dst.at[s], o_sem.at[k, s])

    def half(t, Lc, Ln, Yc, Yp, zero):
        chunks = [functools.partial(dot_chunk, Lc, W.at[0], Yc, slice(0, NP + ROW), n) for n in DUO]
        weave(chunks, (prep_of(jnp.minimum(t + 1, NS - 1), Ln), epi_gen(lax.rem(t + NS - 1, NS), Yp, zero)))

    ready(0)
    for _ in prep_of(0, L0):
        pass
    weight_finish(W.at[0], WR.at[0], b2[1:2, :], wm_sem.at[0], wr_sem.at[0])
    weight_copies(dw, W.at[1], WR.at[1], wm_sem.at[1], wr_sem.at[1])

    def body(i, carry):
        t = 2 * i
        zero = nil(i)
        ready(t + 1)
        pl.when(t + 2 < NS)(lambda: ready(t + 2))
        for n in (t, t + 1):
            take0(n).start()
            pl.when(t + 4 < NS)(functools.partial(fetch, n + 4, None))

        @pl.when(i > 0)
        def _():
            for n in (t - 2, t - 1):
                take0(n).wait()
                put(0, n).start()
        for n in (t - 3, t - 2):
            @pl.when(n >= 0)
            def _(n=n):
                put(1, n).start()
                put(2, n).start()
        half(t, L0, L1, Y0, Y1, zero)
        half(t + 1, L1, L0, Y1, Y0, zero)
        return carry

    lax.fori_loop(0, NS // 2, body, 0)
    still = nil(me)
    for _ in epi_gen(NS - 1, Y1, still):
        pass
    for s in range(NS - 3, NS):
        put(1, s).start()
        put(2, s).start()
    for s in (NS - 2, NS - 1):
        take0(s).wait()
        put(0, s).start()
    weight_finish(W.at[1], WR.at[1], bd[...].reshape(1, CH), wm_sem.at[1], wr_sem.at[1])

    def dprep(s, L):
        for o in QUAD:
            xs = [X2[s, span(2 * o + dy), :] for dy in TRI]
            for dy in TRI:
                L[span(o), span(dy, MAIN)] = xs[dy][:, :MAIN]
            store_rest(L, o, *(x[:, MAIN:].astype(F32) for x in xs))

    def depi(s, Y, zero):
        for o in QUAD:
            d = conv_row(Y, o, zero)
            for k in TRI:
                DS[o, k] = d[k]
            parts = [DS[o, k, pl.ds(0, ROW // 2, stride=2), :] for k in TRI]
            OD[s, span(o, ROW // 2), :] = jnp.concatenate(parts, 1)[:, :CH].astype(BF)

    def dhalf(t, Lc, Ln, Yc, Yp, zero):
        for n in DUO:
            dot_chunk(Lc, W.at[1], Yc, slice(0, NP // 2), n)
        dprep(jnp.minimum(t + 1, NS - 1), Ln)
        depi(lax.rem(t + NS - 1, NS), Yp, zero)

    dprep(0, L0)

    def dbody(i, carry):
        t = 2 * i
        zero = nil(i)
        dhalf(t, L0, L1, Y0, Y1, zero)
        dhalf(t + 1, L1, L0, Y1, Y0, zero)
        return carry

    lax.fori_loop(0, NS // 2, dbody, 0)
    depi(NS - 1, Y1, still)
    dout = pltpu.make_async_copy(OD, do, od_sem)
    dout.start()

    def drain(s, carry):
        for k in TRI:
            put(k, s).wait()
        return carry

    lax.fori_loop(0, NS, drain, 0)
    dout.wait()


def solution(mesh):
    sp = mesh.shape["sp"]

    def program(latent, time_emb, w_in, b_in, gn1_scale, gn1_shift, conv1_w, conv1_b, temb_w, temb_b, gn2_scale, gn2_shift, conv2_w, conv2_b, down_w, down_b):
        none = (0, 0)
        lat = jnp.pad(latent.transpose(0, 3, 1, 2), (none, none, none, (1, 1)))
        q = jnp.stack([lat[..., d:d + ROW] for d in TRI], 1).reshape(NS, 12, NP)
        q = jnp.pad(q, (none, (0, 4), none), constant_values=1)

        dma, vm = pltpu.SemaphoreType.DMA, pltpu.VMEM
        any_, vms = pl.BlockSpec(memory_space=pl.ANY), pl.BlockSpec(memory_space=pltpu.VMEM)
        params = functools.partial(pltpu.CompilerParams, vmem_limit_bytes=66_000_000)

        def big(n=NP, c=CP):
            return vm((NS, n, c), BF)

        def edge(n):
            return vm((n, NS, PK, MAIN), BF)

        def bufs(m):
            return [vm((m, KP), BF)] * 2 + [vm((8, m + 2 * OFF, LANE), F32)] * 2

        def out(*shape):
            return jax.ShapeDtypeStruct(shape, BF)

        hand, hand0, halo, ab = pl.pallas_call(
            functools.partial(mega, sp),
            out_shape=(out(2, NS, NP, CP), out(NS, NP, CH), out(SLOTS, NS, PK, MAIN), jax.ShapeDtypeStruct((2, NS, CP), F32)),
            in_specs=[vms] * 11 + [any_] * 3, out_specs=(any_, any_, any_, vms),
            scratch_shapes=[big(), big(), big(), big(NP, CH), vm((3, KP, KP), BF), vm((3, 9, CH, ROW), BF), vm((2, CH, temb_w.shape[1]), BF), vm((3 * NS, CP), F32)] + bufs(NP)
            + [vm((SLOTS, NS, OFF, LANE), F32), vm((SLOTS, NS, 2, LANE), F32), vm((SLOTS, NS, sp - 1, 2, LANE), F32), vm((2, NS, CP), F32), vm((SLOTS, NS, CP), F32), vm((OFF, CP), F32),
               edge(4), edge(4), big(PK, MAIN), edge(3), edge(3), big(PK, MAIN), vm((2, NS, NS, LANE), BF),
               dma((3,)), dma((3,)), dma, dma((2,)), dma((2,)), dma((SLOTS, NS)), dma((SLOTS, NS)), dma((SLOTS, NS)), dma((SLOTS, NS)), dma((NS,)),
               dma((SLOTS, NS)), dma((SLOTS, NS)), dma((NS,)), dma((SLOTS, NS)), dma((4,))],
            compiler_params=params(collective_id=0, has_side_effects=True), name="mega",
        )(q, w_in, b_in.reshape(1, CH), time_emb, temb_b, gn1_scale, gn1_shift, gn2_scale, gn2_shift, conv1_b, conv2_b, temb_w.transpose(0, 2, 1), conv1_w, conv2_w)
        outs = pl.pallas_call(
            tail,
            out_shape=(out(NS, NP, CH),) * 3 + (out(NS, NP // 4, CH),),
            in_specs=[any_] * 3 + [vms] * 3 + [any_] * 2, out_specs=(any_,) * 4,
            scratch_shapes=[big(), big(), edge(4), big(NP, CH), big(NP + ROW), vm((2, KP, KP), BF), vm((2, 9, CH, ROW), BF)] + bufs(NP + ROW)
            + [big(NP, CH), big(NP, CH), big(NP // 4, CH), vm((4, 3, ROW, LANE), F32),
               dma((2, NS)), dma((SLOTS, NS)), dma((NS,)), dma((2,)), dma((2,)), dma((3, NS)), dma],
            compiler_params=params(), name="tail",
        )(hand, hand0, halo, ab, conv2_b, down_b.reshape(1, CH), conv2_w, down_w)
        return tuple(o.reshape(NS, n, m, CH) for o, n, m in zip(outs, [ROWS] * len(TRI) + [ROWS // 2], [ROW] * len(TRI) + [ROW // 2]))

    band = P("dp", "sp", None, None)
    return jax.shard_map(program, mesh=mesh, in_specs=(band, P("dp", None)) + (P(),) * 14, out_specs=(band,) * 4, check_vma=False)
```

```python
import functools

import jax
import jax.numpy as jnp
from jax import lax
from jax.experimental import pallas as pl
from jax.experimental.pallas import tpu as pltpu
from jax.sharding import PartitionSpec as P

F32, BF = jnp.float32, jnp.bfloat16
GN_GROUPS, GN_EPS = 32, 1e-5
NS, ROWS, ROW, LANE, MAIN = 16, 8, 64, 128, 256
NP = ROWS * ROW
CH = 320
CP = CH + ROW
KP = 4 * MAIN
REST = 3 * MAIN
SPARE = 3 * CH
OFF = 8
GSIZE = CH // GN_GROUPS
PK = ROW + NS
MESH = pl.DeviceIdType.MESH
DUO, TRI, QUAD = range(2), range(3), range(4)
SLOTS = len(QUAD)
NIL = 0.0
SHARE = (1, 2, 3, 3)
ACC32 = dict(preferred_element_type=F32)
ROWS_DOT, COLS_DOT = ((((k,), (k,)), ((), ())) for k in DUO)


def nil(i):
    return jnp.minimum(i, 0) * OFF


def span(i, n=ROW, base=0):
    return slice(base + i * n, base + (i + 1) * n)


def low_half():
    return lax.broadcasted_iota(jnp.int32, (ROW, LANE), 1) < ROW


def widen(p):
    return jnp.concatenate([p, p[..., MAIN:]], -1)


def keep_if(flag, x):
    return jnp.where(jnp.full(x.shape, flag, jnp.int32) > 0, x, NIL)


def store_rest(L, o, r0, r1, r2):
    low = low_half()
    L[span(o), REST:REST + LANE] = jnp.where(low, r0, r1).astype(BF)
    L[span(o), REST + LANE:] = jnp.where(low, r2, 1.0).astype(BF)


def prep_gen(x_of_row, nrows, a, b, L):
    ha, hb = a * 0.5, b * 0.5
    rest = []
    for r in range(nrows + 2):
        x, flag = x_of_row(r)
        h = x.astype(F32) * ha + hb
        n = h + h * jnp.tanh(h)
        if flag is not None:
            n = keep_if(flag, n)
        main = n[:, :MAIN].astype(BF)
        rest.append(n[:, MAIN:])
        for dy in TRI:
            if 0 <= r - dy < nrows:
                L[span(r - dy), span(dy, MAIN)] = main
        if r >= 2:
            store_rest(L, r - 2, *rest[r - 2:])
        yield main


def conv_row(Y, o, zero):
    sub = lax.broadcasted_iota(jnp.int32, (OFF, LANE), 0)
    top, bot = sub == 0, sub == 7

    def here(k):
        return Y[k, span(o, base=OFF), :]

    def left(k):
        v = Y[k, pl.ds(zero + (OFF - 1 + o * ROW), ROW), :]
        return jnp.concatenate([jnp.where(top, 0.0, v[:OFF]), v[OFF:]], 0)

    def right(k):
        v = Y[k, pl.ds(zero + (OFF + 1 + o * ROW), ROW), :]
        return jnp.concatenate([v[:-OFF], jnp.where(bot, 0.0, v[-OFF:])], 0)

    out = [left(k) + here(k + 2) + right(k + 4) for k in DUO]
    mix = jnp.where(low_half(), left(6), here(6))
    return out + [mix + pltpu.roll(mix, ROW, 1) + right(7)]


def dot_chunk(L, W, Y, rows, n):
    r = jnp.dot(L[rows, :], W[:, span(n, MAIN)], **ACC32)
    for k in DUO:
        Y[2 * n + k, OFF + rows.start:OFF + rows.stop, :] = r[:, span(k, LANE)]


def weave(L, W, Y, m, prep, epi, share):
    work = [prep] * (m // ROW + 2) + [epi] * (m // ROW)
    done = 0
    for n in QUAD:
        dot_chunk(L, W, Y, slice(0, m), n)
        upto = len(work) * share[n] // share[-1]
        for g in work[done:upto]:
            mark = next(g)
        done = upto
        if n < len(QUAD) - 1:
            L[:NS, KP - NS:] = jnp.where(mark[:NS, LANE - NS:LANE].astype(F32) > NIL, 1.0, NIL).astype(BF)
    for g in (prep, epi):
        for _ in g:
            pass


def lane_left(x, k):
    return pltpu.roll(x, CP - k, 1)


def starts(k):
    lane = lax.broadcasted_iota(jnp.int32, (OFF, LANE), 1) + k * LANE
    return (lane % GSIZE == 0) & (lane < CH)


def stacked(rows):
    fill = [jnp.zeros((4 - len(rows), rows[0].shape[1]), F32)] * (len(rows) < 4)
    return jnp.concatenate(list(rows) + fill, 0)


def compact(tiles, embs):
    s = stacked([jnp.concatenate([t[k:k + 1] for k in TRI], 1) for t in tiles])
    q = stacked([jnp.concatenate([t[k + 3:k + 4] for k in TRI], 1) for t in tiles])
    e = stacked(embs)
    x = jnp.concatenate([s + float(NP) * e, q + e * (2.0 * s + float(NP) * e)], 0)
    w2 = x + lane_left(x, 1)
    w4 = w2 + lane_left(w2, 2)
    w8 = w4 + lane_left(w4, 4)
    w10 = w8 + lane_left(w2, 8)
    c = sum(jnp.where(starts(k), w10[:, span(k, LANE)], NIL) for k in TRI)
    return [jnp.concatenate([c[k:k + 1], c[k + 4:k + 5]], 0) for k in range(len(tiles))]


def affine(tots, gains, shifts, embs, count):
    x = jnp.concatenate([stacked([t[k:k + 1] for t in tots]) for k in DUO], 0)
    y = jnp.concatenate([jnp.where(starts(k), x, NIL) for k in TRI], 1)
    r2 = y + pltpu.roll(y, 1, 1)
    r4 = r2 + pltpu.roll(r2, 2, 1)
    r8 = r4 + pltpu.roll(r4, 4, 1)
    r = r8 + pltpu.roll(r2, 8, 1)
    lane = lax.broadcasted_iota(jnp.int32, (OFF, CP), 1)
    r = jnp.where(lane >= CH, pltpu.roll(r, ROW, 1), r) * (1.0 / count)
    mean, msq = r[:4], r[4:]
    a = stacked(gains) * lax.rsqrt(msq - mean * mean + GN_EPS)
    return a, stacked(shifts) + a * (stacked(embs) - mean)


def pack_row(dst, x):
    dst[:ROW, :] = jnp.concatenate(x[:2], 1)
    half = ROW // 2
    p = jnp.where(low_half()[:half], x[2][:half].astype(F32), x[2][half:].astype(F32))
    dst[ROW:, :] = jnp.concatenate([p[:NS], p[NS:]], 1).astype(BF)


def unpack_row(src):
    p = src[ROW:, :].astype(F32)
    p = jnp.concatenate([p[:, :LANE], p[:, LANE:]], 0)
    swap, low = pltpu.roll(p, ROW, 1), low_half()[:ROW // 2]
    rest = jnp.concatenate([jnp.where(low, p, swap), jnp.where(low, swap, p)], 0)
    return jnp.concatenate([src[:ROW, :].astype(F32), rest], 1)


def stats_tile(acc, acq):
    parts = [x.sum(0, keepdims=True) for x in acc + acq]
    return jnp.concatenate(parts + [jnp.zeros((2, LANE), F32)], 0)


def add_stats(acc, acq, new):
    for k, x in enumerate(new):
        v = x.astype(F32).reshape(OFF, OFF, LANE)
        acc[k] = acc[k] + v.sum(0)
        acq[k] = acq[k] + (v * v).sum(0)


def no_stats():
    return [jnp.zeros((OFF, LANE), F32) for _ in TRI]


def weight_copies(src, W, WR, sem_main, sem_rest):
    for dy in TRI:
        for dx in TRI:
            cols = span(dx, MAIN)
            pltpu.make_async_copy(src.at[dy, dx, :MAIN, :MAIN], W.at[span(dy, MAIN), cols], sem_main).start()
            pltpu.make_async_copy(src.at[dy, dx, MAIN:, :MAIN], W.at[span(dy, base=REST), cols], sem_main).start()
            pltpu.make_async_copy(src.at[dy, dx, :, MAIN:], WR.at[dy * 3 + dx], sem_rest).start()


def weight_finish(W, WR, bias, sem_main, sem_rest):
    main = W.at[:SPARE, :REST]
    pltpu.make_async_copy(main, main, sem_main).wait()
    pltpu.make_async_copy(WR, WR, sem_rest).wait()
    for dy in TRI:
        for part, rows in ((slice(0, MAIN), span(dy, MAIN)), (slice(MAIN, CH), span(dy, base=REST))):
            w0, w1, w2 = (WR[dy * 3 + dx, part, :] for dx in TRI)
            W[rows, REST:REST + LANE] = jnp.concatenate([w0, w1], 1)
            W[rows, REST + LANE:] = jnp.concatenate([w2, w2], 1)
    b = widen(bias.astype(F32))
    gap = jnp.zeros((1, MAIN), F32)
    rest = jnp.where(low_half()[:1], 0.0, b[:, MAIN:])
    row = jnp.concatenate([gap, b[:, :MAIN], gap, rest, gap[:, :LANE]], 1)
    first = lax.broadcasted_iota(jnp.int32, (ROW, KP), 0) == 0
    W[SPARE:, :] = jnp.where(first, row, NIL).astype(BF)


def mega(sp, q, wi, bi, temb, tb, g1, s1, g2, s2, b1, b2, tw, w1, w2, hand, hand0, halo, abo,
         H, U, H2, HS, W, WR, TW, WI, L0, L1, Y0, Y1, ST, STC, SG, RS, AB, EMB, GAIN, HT, HB, HX, PT, PB, PX, LQ,
         wm_sem, wr_sem, tw_sem, q_send, q_recv, st_send, st_recv, up_send, dn_send, x_send, ht_recv, hb_recv, hx_recv, out_sem, fin_sem):
    me, dp = lax.axis_index("sp"), lax.axis_index("dp")
    has_up, has_dn = (me > 0).astype(jnp.int32), (me < sp - 1).astype(jnp.int32)
    held = (H, U, H2, U)
    last = NS - 1

    get_tw = pltpu.make_async_copy(tw, TW, tw_sem)
    get_tw.start()
    for j, src in enumerate((w1.at[0], w2.at[0], w1.at[1])):
        weight_copies(src, W.at[j], WR.at[j], wm_sem.at[j], wr_sem.at[j])

    barrier = pltpu.get_barrier_semaphore()
    for k in range(1, sp):
        pl.semaphore_signal(barrier, inc=1, device_id=(dp, lax.rem(me + k, sp)), device_id_type=MESH)
    pl.semaphore_wait(barrier, sp - 1)

    def remote(src, dst, ssem, rsem, dev):
        return pltpu.make_async_remote_copy(src_ref=src, dst_ref=dst, send_sem=ssem, recv_sem=rsem, device_id=(dp, dev), device_id_type=MESH)

    def if_up(f):
        pl.when(me > 0)(f)

    def if_dn(f):
        pl.when(me < sp - 1)(f)

    q_dn = remote(q.at[:, :, NP - LANE:], LQ.at[0], q_send.at[0], q_recv.at[0], me + 1)
    q_up = remote(q.at[:, :, :LANE], LQ.at[1], q_send.at[1], q_recv.at[1], me - 1)
    if_dn(q_dn.start)
    if_up(q_up.start)

    def up_copy(slot, s):
        return remote(PT.at[slot - 1, s], HB.at[slot, s], up_send.at[slot, s], hb_recv.at[slot, s], me - 1)

    def dn_copy(slot, s):
        return remote(PB.at[slot - 1, s], HT.at[slot, s], dn_send.at[slot, s], ht_recv.at[slot, s], me + 1)

    def dx_copy(s):
        return remote(PX.at[s], HX.at[s], x_send.at[s], hx_recv.at[s], me + 1)

    def out_copy(slot, s):
        src, dst = ((HS, hand0), None, (H2, hand.at[0]), (U, hand.at[1]))[slot]
        return pltpu.make_async_copy(src.at[s], dst.at[s], out_sem.at[slot, s])

    def send_sums(slot, s):
        for k in range(1, sp):
            remote(SG.at[slot, s], RS.at[slot, s, k - 1], st_send.at[slot, s], st_recv.at[slot, s], lax.rem(me + k, sp)).start()

    def send_rows(slot, s):
        if slot != 1:
            out_copy(slot, s).start()
        if slot == 0:
            return
        if_up(lambda: up_copy(slot, s).start())

        def down():
            dn_copy(slot, s).start()
            if slot == 3:
                dx_copy(s).start()
        if_dn(down)

    def wait_sums(slot, s):
        pltpu.make_async_copy(RS.at[slot, s], RS.at[slot, s], st_recv.at[slot, s]).wait()

    def wait_rows(slot, s):
        if_up(lambda: remote(PB.at[0, s], HT.at[slot, s], dn_send.at[slot, s], ht_recv.at[slot, s], me).wait_recv())
        if_dn(lambda: remote(PT.at[0, s], HB.at[slot, s], up_send.at[slot, s], hb_recv.at[slot, s], me).wait_recv())

    def squeeze(slot, ss, tiles):
        for r, s in zip(compact(tiles, [EMB[slot, pl.ds(s, 1)] for s in ss]), ss):
            SG[slot, s] = r

    for k, (ref, l) in enumerate(((g1, 0), (g2, 0), (g1, 1), (g2, 1), (s1, 0), (s2, 0), (s1, 1), (s2, 1))):
        GAIN[k:k + 1, :] = widen(ref[l:l + 1, :].astype(F32))
    WI[...] = jnp.zeros_like(WI)
    for dy in TRI:
        for dx in TRI:
            WI[span(4 * dy + dx, 4), :] = widen(wi[dy, dx].astype(F32))
    WI[NS + 12:NS + 13, :] = widen(bi[...].reshape(1, CH).astype(F32))
    get_tw.wait()
    x = temb[...].astype(F32)
    act = (x * jax.nn.sigmoid(x)).astype(BF)
    for l in DUO:
        pr = lax.dot_general(act, TW[l], COLS_DOT, **ACC32)
        EMB[2 * l] = jnp.zeros((NS, CP), F32)
        EMB[2 * l + 1] = widen(pr + tb[l:l + 1, :].astype(F32))

    if_up(q_dn.wait_recv)
    if_dn(q_up.wait_recv)

    def first(s):
        above, below = keep_if(has_up, LQ[0, s].astype(F32)), keep_if(has_dn, LQ[1, s].astype(F32))
        ext = jnp.concatenate([above, q[s].astype(F32), below], 1)
        mid = pltpu.roll(ext, ext.shape[1] - ROW, 1)
        wide = NP + LANE
        lhs = jnp.concatenate([ext[:, :wide], mid[:, :wide], ext[:, LANE:]], 0).astype(BF)
        r = lax.dot_general(lhs, WI[...].astype(BF), ROWS_DOT, **ACC32)
        acc, acq = no_stats(), no_stats()
        for o in range(ROWS + 2):
            x = r[span(o), :].astype(BF)
            parts = [x[:, span(k, LANE)] for k in TRI]
            if o == 0:
                pack_row(HT.at[0, s], parts)
            elif o > ROWS:
                pack_row(HB.at[0, s], parts)
            else:
                H[s, span(o - 1), :] = x
                HS[s, span(o - 1), :] = x[:, :CH]
                add_stats(acc, acq, parts)
        ST[s] = stats_tile(acc, acq)

    def first_pair(i, carry):
        t = 2 * i
        for n in (t - 2, t - 1):
            pl.when(i > 0)(functools.partial(send_rows, 0, n))
            pl.when(i > 1)(functools.partial(send_sums, 0, n - 2))
        ss = [lax.rem(n + NS, NS) for n in (t - 2, t - 1)]
        tiles = [ST[s] for s in ss]
        first(t)
        first(t + 1)
        squeeze(0, ss, tiles)
        return carry

    lax.fori_loop(0, NS // 2, first_pair, 0)
    squeeze(0, (last - 1, last), (ST[last - 1], ST[last]))
    for j in TRI:
        weight_finish(W.at[j], WR.at[j], (b1, b2)[j % 2][j // 2:j // 2 + 1, :], wm_sem.at[j], wr_sem.at[j])
    for s in range(NS - 4, NS):
        send_sums(0, s)
    for s in (last - 1, last):
        send_rows(0, s)

    def scales(slots, ss):
        tots = []
        for slot, s in zip(slots, ss):
            tots.append(SG[slot, s])
            for k in range(sp - 1):
                tots[-1] = tots[-1] + RS[slot, s, k]
        return affine(tots, [GAIN[pl.ds(k, 1)] for k in slots], [GAIN[pl.ds(k + SLOTS, 1)] for k in slots],
                      [EMB[k, pl.ds(s, 1)] for k, s in zip(slots, ss)], float(sp * NP * GSIZE))

    def prep_of(slot, s, L, a, b):
        def row(r):
            if r == 0:
                return unpack_row(HT.at[slot, s]), has_up
            if r == ROWS + 1:
                return unpack_row(HB.at[slot, s]), has_dn
            return held[slot][s, span(r - 1), :], None
        return prep_gen(row, ROWS, a, b, L)

    def epi_gen(j, s, Y, zero, tiles):
        acc, acq = no_stats(), no_stats()
        edge = {0: PT.at[j, s], ROWS - 1: PB.at[j, s]}
        if j == 2:
            edge[ROWS - 2] = PX.at[s]
        for o in range(ROWS):
            new = [x.astype(BF) for x in conv_row(Y, o, zero)]
            mark = new[2]
            for k in TRI:
                if j == 1:
                    new[k] = (new[k].astype(F32) + H[s, span(o), span(k, LANE)].astype(F32)).astype(BF)
                held[j + 1][s, span(o), span(k, LANE)] = new[k]
            if o in edge:
                pack_row(edge[o], new)
            add_stats(acc, acq, new)
            if o == ROWS - 1:
                tiles.append(stats_tile(acc, acq))
            yield mark

    for Y in (Y0, Y1):
        Y[...] = jnp.zeros_like(Y)
    for s in TRI:
        wait_sums(0, s)
    for c, v in enumerate(scales((0,) * 3, TRI)):
        AB[c] = v[:3]
    still = nil(me)
    ahead = len(QUAD)
    for _ in prep_of(0, 0, L0, AB[0, :1], AB[1, :1]):
        pass
    for j in TRI:
        def body(i, carry, j=j):
            t = ahead * i
            zero = nil(i)
            ns = [jnp.minimum(j * NS + t + 3 + k, 3 * NS - 1) for k in QUAD]
            for k, n in enumerate(ns):
                go = functools.partial(wait_sums, n // NS, lax.rem(n, NS))
                if j < 2:
                    go()
                else:
                    pl.when(t + 3 + k < NS)(go)
            for k in QUAD:
                if j > 0:
                    wait_rows((j * NS + t + k + 1) // NS, lax.rem(t + k + 1, NS))
                elif k == ahead - 1:
                    pl.when(t + ahead == NS)(lambda: wait_rows(1, 0))
            for k in QUAD:
                pl.when(t + k > ahead)(functools.partial(send_rows, j + 1, t + k - 5))
                pl.when(t + k > ahead + 1)(functools.partial(send_sums, j + 1, t + k - 6))
            a, b = scales([n // NS for n in ns], [lax.rem(n, NS) for n in ns])
            co = [(AB[0, k:k + 1], AB[1, k:k + 1]) for k in (1, 2)] + [(a[k:k + 1], b[k:k + 1]) for k in DUO]
            tiles = [STC[...]]
            for u in QUAD:
                nxt = jnp.minimum(t + u + 1, last)
                if u % 2:
                    Lc, Ln, Yc, Yp = L1, L0, Y1, Y0
                else:
                    Lc, Ln, Yc, Yp = L0, L1, Y0, Y1
                weave(Lc, W.at[j], Yc, NP, prep_of(j, nxt, Ln, *co[u]), epi_gen(j, lax.rem(t + u + last, NS), Yp, zero, tiles), SHARE)
            AB[0], AB[1] = a[1:], b[1:]
            STC[...] = tiles.pop()
            squeeze(j + 1, [lax.rem(t + last - 1 + k, NS) for k in QUAD], tiles)
            return carry

        lax.fori_loop(0, NS // ahead, body, 0)
        for k in QUAD:
            send_rows(j + 1, last - ahead + k)
            send_sums(j + 1, last - ahead - 1 + k)
        tiles = [STC[...]]
        for _ in epi_gen(j, last, Y1, still, tiles):
            pass
        if j < 2:
            for _ in prep_of(j + 1, 0, L0, AB[0, :1], AB[1, :1]):
                pass
        squeeze(j + 1, (last - 1, last), tiles)
        send_sums(j + 1, last - 1)
        send_sums(j + 1, last)
        send_rows(j + 1, last)

    def drain(s, carry):
        wait_sums(3, s)
        for slot in QUAD:
            pltpu.make_async_copy(RS.at[slot, s], RS.at[slot, s], st_send.at[slot, s]).wait()
            if slot != 1:
                out_copy(slot, s).wait()
            if slot > 0:
                if_up(lambda slot=slot: up_copy(slot, s).wait_send())
                if_dn(lambda slot=slot: dn_copy(slot, s).wait_send())
        pl.when(s > 0)(lambda: wait_rows(3, s))
        if_up(lambda: dx_copy(s).wait_recv())
        if_dn(lambda: dx_copy(s).wait_send())
        return carry

    lax.fori_loop(0, NS, drain, 0)
    if_dn(q_dn.wait_send)
    if_up(q_up.wait_send)
    fins = [pltpu.make_async_copy(r, halo.at[k], fin_sem.at[k]) for k, r in enumerate((HT.at[2], HT.at[3], HX, HB.at[3]))]
    for f in fins:
        f.start()
    for k in QUAD:
        for c, v in enumerate(scales((3,) * ahead, range(ahead * k, ahead * k + ahead))):
            abo[c, span(k, ahead)] = v
    for f in fins:
        f.wait()


def tail(hand, hand0, halo, ab, b2, bd, w2, dw, h0o, h1o, h2o, do,
         H, U, HA, P0, X2, W, WR, L0, L1, Y0, Y1, O1, O2, OD, DS, in_sem, ha_sem, p_sem, wm_sem, wr_sem, o_sem, od_sem):
    me, sp = lax.axis_index("sp"), lax.axis_size("sp")
    has_up, has_dn = (me > 0).astype(jnp.int32), (me < sp - 1).astype(jnp.int32)

    def gets(s):
        return ([pltpu.make_async_copy(hand.at[k, s], (H, U)[k].at[s], in_sem.at[k, s]) for k in (1, 0)]
                + [pltpu.make_async_copy(halo.at[k, s], HA.at[k, s], ha_sem.at[k, s]) for k in QUAD])

    def take0(s):
        return pltpu.make_async_copy(hand0.at[s], P0.at[s], p_sem.at[s])

    def fetch(s, carry):
        for c in gets(s):
            c.start()
        return carry

    def ready(s):
        for c in gets(s):
            c.wait()

    fetch(0, 0)
    weight_copies(w2.at[1], W.at[0], WR.at[0], wm_sem.at[0], wr_sem.at[0])
    lax.fori_loop(1, len(QUAD) + 1, fetch, 0)

    def prep_of(s, L):
        def row(r):
            if r < 2:
                return unpack_row(HA.at[2 - r, s]), has_up
            if r == ROWS + 2:
                return unpack_row(HA.at[3, s]), has_dn
            return U[s, span(r - 2), :], None
        return prep_gen(row, ROWS + 1, ab[0, pl.ds(s, 1)], ab[1, pl.ds(s, 1)], L)

    def epi_gen(s, Y, zero):
        for o in range(ROWS + 1):
            t = [x.astype(BF) for x in conv_row(Y, o, zero)]
            edge = unpack_row(HA.at[0, s]) if o == 0 else None
            for k in TRI:
                cols = span(k, LANE)
                old = edge[:, cols] if o == 0 else H[s, span(o - 1), cols]
                new = old.astype(F32) + t[k].astype(F32)
                new = (keep_if(has_up, new) if o == 0 else new).astype(BF)
                X2[s, span(o), cols] = new
                if o > 0:
                    n = min(LANE, CH - k * LANE)
                    cols = slice(k * LANE, k * LANE + n)
                    O1[s, span(o - 1), cols] = old[:, :n]
                    O2[s, span(o - 1), cols] = new[:, :n]
            yield t[2]

    def put(k, s):
        src, dst = ((P0, h0o), (O1, h1o), (O2, h2o))[k]
        return pltpu.make_async_copy(src.at[s], dst.at[s], o_sem.at[k, s])

    ready(0)
    for _ in prep_of(0, L0):
        pass
    weight_finish(W.at[0], WR.at[0], b2[1:2, :], wm_sem.at[0], wr_sem.at[0])
    weight_copies(dw, W.at[1], WR.at[1], wm_sem.at[1], wr_sem.at[1])

    for Y in (Y0, Y1):
        Y[...] = jnp.zeros_like(Y)
    ahead = len(QUAD)

    def body(i, carry):
        t = ahead * i
        zero = nil(i)
        for k in QUAD:
            pl.when(t + k + 1 < NS)(functools.partial(ready, t + k + 1))
            pl.when(t + k + ahead + 1 < NS)(functools.partial(fetch, t + k + ahead + 1, None))
            take0(t + k).start()

        @pl.when(i > 0)
        def _():
            for k in QUAD:
                take0(t - ahead + k).wait()
                put(0, t - ahead + k).start()

        for k in QUAD:
            @pl.when(t + k > ahead)
            def _(n=t + k - 5):
                put(1, n).start()
                put(2, n).start()
        for u in QUAD:
            if u % 2:
                Lc, Ln, Yc, Yp = L1, L0, Y1, Y0
            else:
                Lc, Ln, Yc, Yp = L0, L1, Y0, Y1
            weave(Lc, W.at[0], Yc, NP + ROW, prep_of(jnp.minimum(t + u + 1, NS - 1), Ln), epi_gen(lax.rem(t + u + NS - 1, NS), Yp, zero), SHARE)
        return carry

    lax.fori_loop(0, NS // ahead, body, 0)
    still = nil(me)
    for _ in epi_gen(NS - 1, Y1, still):
        pass
    for s in range(NS - ahead - 1, NS):
        put(1, s).start()
        put(2, s).start()
    for s in range(NS - ahead, NS):
        take0(s).wait()
        put(0, s).start()
    weight_finish(W.at[1], WR.at[1], bd[...].reshape(1, CH), wm_sem.at[1], wr_sem.at[1])

    def dprep(s, L):
        for o in QUAD:
            xs = [X2[s, span(2 * o + dy), :] for dy in TRI]
            for dy in TRI:
                L[span(o), span(dy, MAIN)] = xs[dy][:, :MAIN]
            store_rest(L, o, *(x[:, MAIN:].astype(F32) for x in xs))

    def depi(s, Y, zero):
        for o in QUAD:
            d = conv_row(Y, o, zero)
            for k in TRI:
                DS[o, k] = d[k]
            parts = [DS[o, k, pl.ds(0, ROW // 2, stride=2), :] for k in TRI]
            OD[s, span(o, ROW // 2), :] = jnp.concatenate(parts, 1)[:, :CH].astype(BF)

    def dhalf(t, Lc, Ln, Yc, Yp, zero):
        for n in QUAD:
            dot_chunk(Lc, W.at[1], Yc, slice(0, NP // 2), n)
        dprep(jnp.minimum(t + 1, NS - 1), Ln)
        depi(lax.rem(t + NS - 1, NS), Yp, zero)

    dprep(0, L0)

    def dbody(i, carry):
        t = 2 * i
        zero = nil(i)
        dhalf(t, L0, L1, Y0, Y1, zero)
        dhalf(t + 1, L1, L0, Y1, Y0, zero)
        return carry

    lax.fori_loop(0, NS // 2, dbody, 0)
    depi(NS - 1, Y1, still)
    dout = pltpu.make_async_copy(OD, do, od_sem)
    dout.start()

    def drain(s, carry):
        for k in TRI:
            put(k, s).wait()
        return carry

    lax.fori_loop(0, NS, drain, 0)
    dout.wait()


def solution(mesh):
    sp = mesh.shape["sp"]

    def program(latent, time_emb, w_in, b_in, gn1_scale, gn1_shift, conv1_w, conv1_b, temb_w, temb_b, gn2_scale, gn2_shift, conv2_w, conv2_b, down_w, down_b):
        none = (0, 0)
        lat = jnp.pad(latent.transpose(0, 3, 1, 2), (none, none, none, (1, 1)))
        q = jnp.stack([lat[..., d:d + ROW] for d in TRI], 1).reshape(NS, 12, NP)
        q = jnp.pad(q, (none, (0, 4), none), constant_values=1)

        dma, vm = pltpu.SemaphoreType.DMA, pltpu.VMEM
        any_, vms = pl.BlockSpec(memory_space=pl.ANY), pl.BlockSpec(memory_space=pltpu.VMEM)
        params = functools.partial(pltpu.CompilerParams, vmem_limit_bytes=66_000_000)

        def big(n=NP, c=CP):
            return vm((NS, n, c), BF)

        def edge(n):
            return vm((n, NS, PK, MAIN), BF)

        def bufs(m):
            return [vm((m, KP), BF)] * 2 + [vm((8, m + 2 * OFF, LANE), F32)] * 2

        def out(*shape):
            return jax.ShapeDtypeStruct(shape, BF)

        hand, hand0, halo, ab = pl.pallas_call(
            functools.partial(mega, sp),
            out_shape=(out(2, NS, NP, CP), out(NS, NP, CH), out(SLOTS, NS, PK, MAIN), jax.ShapeDtypeStruct((2, NS, CP), F32)),
            in_specs=[vms] * 11 + [any_] * 3, out_specs=(any_, any_, any_, vms),
            scratch_shapes=[big(), big(), big(), big(NP, CH), vm((3, KP, KP), BF), vm((3, 9, CH, ROW), BF), vm((2, CH, temb_w.shape[1]), BF), vm((3 * NS, CP), F32)] + bufs(NP)
            + [vm((NS, OFF, LANE), F32), vm((OFF, LANE), F32), vm((SLOTS, NS, 2, LANE), F32), vm((SLOTS, NS, sp - 1, 2, LANE), F32), vm((2, 3, CP), F32), vm((SLOTS, NS, CP), F32), vm((OFF, CP), F32),
               edge(4), edge(4), big(PK, MAIN), edge(3), edge(3), big(PK, MAIN), vm((2, NS, NS, LANE), BF),
               dma((3,)), dma((3,)), dma, dma((2,)), dma((2,)), dma((SLOTS, NS)), dma((SLOTS, NS)), dma((SLOTS, NS)), dma((SLOTS, NS)), dma((NS,)),
               dma((SLOTS, NS)), dma((SLOTS, NS)), dma((NS,)), dma((SLOTS, NS)), dma((4,))],
            compiler_params=params(collective_id=0, has_side_effects=True), name="mega",
        )(q, w_in, b_in, time_emb, temb_b, gn1_scale, gn1_shift, gn2_scale, gn2_shift, conv1_b, conv2_b, temb_w.transpose(0, 2, 1), conv1_w, conv2_w)
        outs = pl.pallas_call(
            tail,
            out_shape=(out(NS, NP, CH),) * 3 + (out(NS, NP // 4, CH),),
            in_specs=[any_] * 3 + [vms] * 3 + [any_] * 2, out_specs=(any_,) * 4,
            scratch_shapes=[big(), big(), edge(4), big(NP, CH), big(NP + ROW), vm((2, KP, KP), BF), vm((2, 9, CH, ROW), BF)] + bufs(NP + ROW)
            + [big(NP, CH), big(NP, CH), big(NP // 4, CH), vm((4, 3, ROW, LANE), F32),
               dma((2, NS)), dma((SLOTS, NS)), dma((NS,)), dma((2,)), dma((2,)), dma((3, NS)), dma],
            compiler_params=params(), name="tail",
        )(hand, hand0, halo, ab, conv2_b, down_b, conv2_w, down_w)
        return tuple(o.reshape(NS, n, m, CH) for o, n, m in zip(outs, [ROWS] * len(TRI) + [ROWS // 2], [ROW] * len(TRI) + [ROW // 2]))

    band = P("dp", "sp", None, None)
    return jax.shard_map(program, mesh=mesh, in_specs=(band, P("dp", None)) + (P(),) * 14, out_specs=(band,) * 4, check_vma=False)
```

```python
import functools

import jax
import jax.numpy as jnp
from jax import lax
from jax.experimental import pallas as pl
from jax.experimental.pallas import tpu as pltpu
from jax.sharding import PartitionSpec as P

F32, BF = jnp.float32, jnp.bfloat16
GN_GROUPS, GN_EPS = 32, 1e-5
NS, ROWS, ROW, LANE, MAIN = 16, 8, 64, 128, 256
NP = ROWS * ROW
CH = 320
CP = CH + ROW
KP = 4 * MAIN
REST = 3 * MAIN
SPARE = 3 * CH
OFF = 8
GSIZE = CH // GN_GROUPS
PK = ROW + NS
MESH = pl.DeviceIdType.MESH
DUO, TRI, QUAD = range(2), range(3), range(4)
SLOTS = len(QUAD)
NIL = 0.0


def groups(n, step):
    cuts = [0, *range(n, NS, step), NS]
    return [(a, b - a) for a, b in zip(cuts, cuts[1:])]


SUMS, EDGES = groups(2, SLOTS), groups(3, SLOTS)
SHARE = (1, 2, 3, 3)
ACC32 = dict(preferred_element_type=F32)
ROWS_DOT, COLS_DOT = ((((k,), (k,)), ((), ())) for k in DUO)


def nil(i):
    return jnp.minimum(i, 0) * OFF


def span(i, n=ROW, base=0):
    return slice(base + i * n, base + (i + 1) * n)


def low_half():
    return lax.broadcasted_iota(jnp.int32, (ROW, LANE), 1) < ROW


def widen(p):
    return jnp.concatenate([p, p[..., MAIN:]], -1)


def keep_if(flag, x):
    return jnp.where(jnp.full(x.shape, flag, jnp.int32) > 0, x, NIL)


def store_rest(L, o, r0, r1, r2):
    low = low_half()
    L[span(o), REST:REST + LANE] = jnp.where(low, r0, r1).astype(BF)
    L[span(o), REST + LANE:] = jnp.where(low, r2, 1.0).astype(BF)


def prep_gen(x_of_row, nrows, a, b, L):
    ha, hb = a * 0.5, b * 0.5
    rest = []
    for r in range(nrows + 2):
        x, flag = x_of_row(r)
        h = x.astype(F32) * ha + hb
        n = h + h * jnp.tanh(h)
        if flag is not None:
            n = keep_if(flag, n)
        main = n[:, :MAIN].astype(BF)
        rest.append(n[:, MAIN:])
        for dy in TRI:
            if 0 <= r - dy < nrows:
                L[span(r - dy), span(dy, MAIN)] = main
        if r >= 2:
            store_rest(L, r - 2, *rest[r - 2:])
        yield main


def conv_row(Y, o, zero):
    sub = lax.broadcasted_iota(jnp.int32, (OFF, LANE), 0)
    top, bot = sub == 0, sub == 7

    def here(k):
        return Y[k, span(o, base=OFF), :]

    def left(k):
        v = Y[k, pl.ds(zero + (OFF - 1 + o * ROW), ROW), :]
        return jnp.concatenate([jnp.where(top, 0.0, v[:OFF]), v[OFF:]], 0)

    def right(k):
        v = Y[k, pl.ds(zero + (OFF + 1 + o * ROW), ROW), :]
        return jnp.concatenate([v[:-OFF], jnp.where(bot, 0.0, v[-OFF:])], 0)

    out = [left(k) + here(k + 2) + right(k + 4) for k in DUO]
    mix = jnp.where(low_half(), left(6), here(6))
    return out + [mix + pltpu.roll(mix, ROW, 1) + right(7)]


def dot_chunk(L, W, Y, rows, n):
    r = jnp.dot(L[rows, :], W[:, span(n, MAIN)], **ACC32)
    for k in DUO:
        Y[2 * n + k, OFF + rows.start:OFF + rows.stop, :] = r[:, span(k, LANE)]


def weave(L, W, Y, m, prep, epi, share):
    work = [prep] * (m // ROW + 2) + [epi] * (m // ROW)
    done = 0
    for n in QUAD:
        dot_chunk(L, W, Y, slice(0, m), n)
        upto = len(work) * share[n] // share[-1]
        for g in work[done:upto]:
            mark = next(g)
        done = upto
        if n < len(QUAD) - 1:
            L[:NS, KP - NS:] = jnp.where(mark[:NS, LANE - NS:LANE].astype(F32) > NIL, 1.0, NIL).astype(BF)
    for g in (prep, epi):
        for _ in g:
            pass


def lane_left(x, k):
    return pltpu.roll(x, CP - k, 1)


def starts(k):
    lane = lax.broadcasted_iota(jnp.int32, (OFF, LANE), 1) + k * LANE
    return (lane % GSIZE == 0) & (lane < CH)


def stacked(rows):
    fill = [jnp.zeros((4 - len(rows), rows[0].shape[1]), F32)] * (len(rows) < 4)
    return jnp.concatenate(list(rows) + fill, 0)


def compact(tiles, embs):
    s = stacked([jnp.concatenate([t[k:k + 1] for k in TRI], 1) for t in tiles])
    q = stacked([jnp.concatenate([t[k + 3:k + 4] for k in TRI], 1) for t in tiles])
    e = stacked(embs)
    x = jnp.concatenate([s + float(NP) * e, q + e * (2.0 * s + float(NP) * e)], 0)
    w2 = x + lane_left(x, 1)
    w4 = w2 + lane_left(w2, 2)
    w8 = w4 + lane_left(w4, 4)
    w10 = w8 + lane_left(w2, 8)
    c = sum(jnp.where(starts(k), w10[:, span(k, LANE)], NIL) for k in TRI)
    return [jnp.concatenate([c[k:k + 1], c[k + 4:k + 5]], 0) for k in range(len(tiles))]


def affine(tots, gains, shifts, embs, count):
    x = jnp.concatenate([stacked([t[k:k + 1] for t in tots]) for k in DUO], 0)
    y = jnp.concatenate([jnp.where(starts(k), x, NIL) for k in TRI], 1)
    r2 = y + pltpu.roll(y, 1, 1)
    r4 = r2 + pltpu.roll(r2, 2, 1)
    r8 = r4 + pltpu.roll(r4, 4, 1)
    r = r8 + pltpu.roll(r2, 8, 1)
    lane = lax.broadcasted_iota(jnp.int32, (OFF, CP), 1)
    r = jnp.where(lane >= CH, pltpu.roll(r, ROW, 1), r) * (1.0 / count)
    mean, msq = r[:4], r[4:]
    a = stacked(gains) * lax.rsqrt(msq - mean * mean + GN_EPS)
    return a, stacked(shifts) + a * (stacked(embs) - mean)


def pack_row(dst, x):
    dst[:ROW, :] = jnp.concatenate(x[:2], 1)
    half = ROW // 2
    p = jnp.where(low_half()[:half], x[2][:half].astype(F32), x[2][half:].astype(F32))
    dst[ROW:, :] = jnp.concatenate([p[:NS], p[NS:]], 1).astype(BF)


def unpack_row(src):
    p = src[ROW:, :].astype(F32)
    p = jnp.concatenate([p[:, :LANE], p[:, LANE:]], 0)
    swap, low = pltpu.roll(p, ROW, 1), low_half()[:ROW // 2]
    rest = jnp.concatenate([jnp.where(low, p, swap), jnp.where(low, swap, p)], 0)
    return jnp.concatenate([src[:ROW, :].astype(F32), rest], 1)


def stats_tile(acc, acq):
    parts = [x.sum(0, keepdims=True) for x in acc + acq]
    return jnp.concatenate(parts + [jnp.zeros((2, LANE), F32)], 0)


def add_stats(acc, acq, new):
    for k, x in enumerate(new):
        v = x.astype(F32).reshape(OFF, OFF, LANE)
        acc[k] = acc[k] + v.sum(0)
        acq[k] = acq[k] + (v * v).sum(0)


def no_stats():
    return [jnp.zeros((OFF, LANE), F32) for _ in TRI]


def weight_copies(src, W, WR, sem_main, sem_rest):
    for dy in TRI:
        for dx in TRI:
            cols = span(dx, MAIN)
            pltpu.make_async_copy(src.at[dy, dx, :MAIN, :MAIN], W.at[span(dy, MAIN), cols], sem_main).start()
            pltpu.make_async_copy(src.at[dy, dx, MAIN:, :MAIN], W.at[span(dy, base=REST), cols], sem_main).start()
            pltpu.make_async_copy(src.at[dy, dx, :, MAIN:], WR.at[dy * 3 + dx], sem_rest).start()


def weight_finish(bias, W, WR, sem_main, sem_rest):
    main = W.at[:SPARE, :REST]
    pltpu.make_async_copy(main, main, sem_main).wait()
    pltpu.make_async_copy(WR, WR, sem_rest).wait()
    for dy in TRI:
        for part, rows in ((slice(0, MAIN), span(dy, MAIN)), (slice(MAIN, CH), span(dy, base=REST))):
            w0, w1, w2 = (WR[dy * 3 + dx, part, :] for dx in TRI)
            W[rows, REST:REST + LANE] = jnp.concatenate([w0, w1], 1)
            W[rows, REST + LANE:] = jnp.concatenate([w2, w2], 1)
    b = widen(bias.astype(F32))
    gap = jnp.zeros((1, MAIN), F32)
    rest = jnp.where(low_half()[:1], 0.0, b[:, MAIN:])
    row = jnp.concatenate([gap, b[:, :MAIN], gap, rest, gap[:, :LANE]], 1)
    first = lax.broadcasted_iota(jnp.int32, (ROW, KP), 0) == 0
    W[SPARE:, :] = jnp.where(first, row, NIL).astype(BF)


def mega(sp, q, wi, bi, temb, tb, g1, s1, g2, s2, b1, b2, tw, w1, w2, hand, hand0, halo, abo,
         H, U, H2, HS, W, WR, TW, WI, L0, L1, Y0, Y1, ST, STC, SG, RS, AB, EMB, GAIN, HT, HB, HX, PT, PB, PX, LQ,
         wm_sem, wr_sem, tw_sem, q_send, q_recv, st_send, st_recv, up_send, dn_send, x_send, ht_recv, hb_recv, hx_recv, out_sem, fin_sem):
    me, dp = lax.axis_index("sp"), lax.axis_index("dp")
    has_up, has_dn = (me > 0).astype(jnp.int32), (me < sp - 1).astype(jnp.int32)
    held = (H, U, H2, U)
    last = NS - 1

    get_tw = pltpu.make_async_copy(tw, TW, tw_sem)
    get_tw.start()
    for j, src in enumerate((w1.at[0], w2.at[0], w1.at[1])):
        weight_copies(src, W.at[j], WR.at[j], wm_sem.at[j], wr_sem.at[j])

    barrier = pltpu.get_barrier_semaphore()
    for k in range(1, sp):
        pl.semaphore_signal(barrier, inc=1, device_id=(dp, lax.rem(me + k, sp)), device_id_type=MESH)
    pl.semaphore_wait(barrier, sp - 1)

    def remote(src, dst, ssem, rsem, dev):
        return pltpu.make_async_remote_copy(src_ref=src, dst_ref=dst, send_sem=ssem, recv_sem=rsem, device_id=(dp, dev), device_id_type=MESH)

    def if_up(f):
        pl.when(me > 0)(f)

    def if_dn(f):
        pl.when(me < sp - 1)(f)

    q_dn = remote(q.at[:, :, NP - LANE:], LQ.at[0], q_send.at[0], q_recv.at[0], me + 1)
    q_up = remote(q.at[:, :, :LANE], LQ.at[1], q_send.at[1], q_recv.at[1], me - 1)
    if_dn(q_dn.start)
    if_up(q_up.start)

    def rows_copies(slot, g, lo, n):
        ss = pl.ds(lo, n)
        up = remote(PT.at[slot - 1, ss], HB.at[slot, ss], up_send.at[slot, g], hb_recv.at[slot, g], me - 1)
        down = [remote(PB.at[slot - 1, ss], HT.at[slot, ss], dn_send.at[slot, g], ht_recv.at[slot, g], me + 1)]
        if slot == 3:
            down.append(remote(PX.at[ss], HX.at[ss], x_send.at[g], hx_recv.at[g], me + 1))
        return up, down

    def out_copy(slot, g, lo, n):
        src, dst = ((HS, hand0), None, (H2, hand.at[0]), (U, hand.at[1]))[slot]
        ss = pl.ds(lo, n)
        return pltpu.make_async_copy(src.at[ss], dst.at[ss], out_sem.at[slot, g])

    def send_sums(slot, g, lo, n):
        ss = pl.ds(lo, n)
        for k in range(1, sp):
            remote(SG.at[slot, ss], RS.at[slot, k - 1, ss], st_send.at[slot, g], st_recv.at[slot, g], lax.rem(me + k, sp)).start()

    def send_rows(slot, g, lo, n):
        if slot != 1:
            out_copy(slot, g, lo, n).start()
        if slot > 0:
            up, down = rows_copies(slot, g, lo, n)
            if_up(up.start)
            if_dn(lambda: [c.start() for c in down] and None)

    def sums_bytes(slot, n, sem, g):
        both = RS.at[slot, :, :n]
        return pltpu.make_async_copy(both, both, sem.at[slot, g])

    def wait_sums(slot, g, n):
        sums_bytes(slot, n, st_recv, g).wait()

    def wait_rows(slot, g, n):
        ss = pl.ds(0, n)
        if_up(lambda: remote(PB.at[0, ss], HT.at[slot, ss], dn_send.at[slot, g], ht_recv.at[slot, g], me).wait_recv())
        if_dn(lambda: remote(PT.at[0, ss], HB.at[slot, ss], up_send.at[slot, g], hb_recv.at[slot, g], me).wait_recv())

    def squeeze(slot, ss, tiles):
        for r, s in zip(compact(tiles, [EMB[slot, pl.ds(s, 1)] for s in ss]), ss):
            SG[slot, s] = r

    for k, (ref, l) in enumerate((ref, l) for pair in ((g1, g2), (s1, s2)) for l in DUO for ref in pair):
        GAIN[k:k + 1, :] = widen(ref[l:l + 1, :].astype(F32))
    WI[...] = jnp.zeros_like(WI)
    for dy in TRI:
        for dx in TRI:
            WI[span(4 * dy + dx, 4), :] = widen(wi[dy, dx].astype(F32))
    WI[NS + 12:NS + 13, :] = widen(bi[...].reshape(1, CH).astype(F32))
    get_tw.wait()
    x = temb[...].astype(F32)
    act = (x * jax.nn.sigmoid(x)).astype(BF)
    for l in DUO:
        pr = lax.dot_general(act, TW[l], COLS_DOT, **ACC32)
        EMB[2 * l] = jnp.zeros((NS, CP), F32)
        EMB[2 * l + 1] = widen(pr + tb[l:l + 1, :].astype(F32))

    if_up(q_dn.wait_recv)
    if_dn(q_up.wait_recv)

    def first(s):
        above, below = keep_if(has_up, LQ[0, s].astype(F32)), keep_if(has_dn, LQ[1, s].astype(F32))
        ext = jnp.concatenate([above, q[s].astype(F32), below], 1)
        mid = pltpu.roll(ext, ext.shape[1] - ROW, 1)
        wide = NP + LANE
        lhs = jnp.concatenate([ext[:, :wide], mid[:, :wide], ext[:, LANE:]], 0).astype(BF)
        r = lax.dot_general(lhs, WI[...].astype(BF), ROWS_DOT, **ACC32)
        acc, acq = no_stats(), no_stats()
        for o in range(ROWS + 2):
            x = r[span(o), :].astype(BF)
            parts = [x[:, span(k, LANE)] for k in TRI]
            if o == 0:
                pack_row(HT.at[0, s], parts)
            elif o > ROWS:
                pack_row(HB.at[0, s], parts)
            else:
                H[s, span(o - 1), :] = x
                HS[s, span(o - 1), :] = x[:, :CH]
                add_stats(acc, acq, parts)
        ST[s] = stats_tile(acc, acq)

    def first_pair(i, carry):
        t = 2 * i
        for g in TRI:
            for parts, send in ((EDGES, send_rows), (SUMS, send_sums)):
                pl.when(i == 2 * g + 2)(functools.partial(send, 0, g, *parts[g]))
        ss = [lax.rem(n + NS, NS) for n in (t - 2, t - 1)]
        tiles = [ST[s] for s in ss]
        first(t)
        first(t + 1)
        squeeze(0, ss, tiles)
        return carry

    lax.fori_loop(0, NS // 2, first_pair, 0)
    squeeze(0, (last - 1, last), (ST[last - 1], ST[last]))
    for j in TRI:
        weight_finish((b1, b2)[j % 2][j // 2:j // 2 + 1, :], W.at[j], WR.at[j], wm_sem.at[j], wr_sem.at[j])
    for g in (3, 4):
        send_sums(0, g, *SUMS[g])
        send_rows(0, g, *EDGES[g])

    def scales(slots, ss):
        tots = []
        for slot, s in zip(slots, ss):
            tots.append(SG[slot, s])
            for k in range(sp - 1):
                tots[-1] = tots[-1] + RS[slot, k, s]
        return affine(tots, [GAIN[pl.ds(k, 1)] for k in slots], [GAIN[pl.ds(k + SLOTS, 1)] for k in slots],
                      [EMB[k, pl.ds(s, 1)] for k, s in zip(slots, ss)], float(sp * NP * GSIZE))

    def prep_of(slot, s, L, a, b):
        def row(r):
            if r == 0:
                return unpack_row(HT.at[slot, s]), has_up
            if r == ROWS + 1:
                return unpack_row(HB.at[slot, s]), has_dn
            return held[slot][s, span(r - 1), :], None
        return prep_gen(row, ROWS, a, b, L)

    def epi_gen(j, s, Y, zero, tiles):
        acc, acq = no_stats(), no_stats()
        edge = {0: PT.at[j, s], ROWS - 1: PB.at[j, s]}
        if j == 2:
            edge[ROWS - 2] = PX.at[s]
        for o in range(ROWS):
            new = [x.astype(BF) for x in conv_row(Y, o, zero)]
            mark = new[2]
            for k in TRI:
                if j == 1:
                    new[k] = (new[k].astype(F32) + H[s, span(o), span(k, LANE)].astype(F32)).astype(BF)
                held[j + 1][s, span(o), span(k, LANE)] = new[k]
            if o in edge:
                pack_row(edge[o], new)
            add_stats(acc, acq, new)
            if o == ROWS - 1:
                tiles.append(stats_tile(acc, acq))
            yield mark

    for Y in (Y0, Y1):
        Y[...] = jnp.zeros_like(Y)
    for g in DUO:
        wait_sums(0, g, SUMS[g][1])
    for c, v in enumerate(scales((0,) * 3, TRI)):
        AB[c] = v[:3]
    still = nil(me)
    ahead = len(QUAD)
    for _ in prep_of(0, 0, L0, AB[0, :1], AB[1, :1]):
        pass
    for j in TRI:
        def body(i, carry, j=j):
            t = ahead * i
            zero = nil(i)
            ns = [jnp.minimum(j * NS + t + 3 + k, 3 * NS - 1) for k in QUAD]
            turn = ahead - 1
            for g in TRI:
                pl.when(i == g)(functools.partial(wait_sums, j, g + 2, SUMS[g + 2][1]))
            for g in DUO:
                if j < 2:
                    pl.when(i == turn)(functools.partial(wait_sums, j + 1, g, SUMS[g][1]))
            if j > 0:
                pl.when(i < turn)(lambda: wait_rows(j, i + 1, ahead))
                pl.when(i == turn)(lambda: wait_rows(j, ahead, 1))
            pl.when(i == turn)(lambda: wait_rows(j + 1, 0, EDGES[0][1]))
            for parts, send in ((EDGES, send_rows), (SUMS, send_sums)):
                for g in TRI:
                    pl.when(i == g + 1)(functools.partial(send, j + 1, g, *parts[g]))
            a, b = scales([n // NS for n in ns], [lax.rem(n, NS) for n in ns])
            co = [(AB[0, k:k + 1], AB[1, k:k + 1]) for k in (1, 2)] + [(a[k:k + 1], b[k:k + 1]) for k in DUO]
            tiles = [STC[...]]
            for u in QUAD:
                nxt = jnp.minimum(t + u + 1, last)
                if u % 2:
                    Lc, Ln, Yc, Yp = L1, L0, Y1, Y0
                else:
                    Lc, Ln, Yc, Yp = L0, L1, Y0, Y1
                weave(Lc, W.at[j], Yc, NP, prep_of(j, nxt, Ln, *co[u]), epi_gen(j, lax.rem(t + u + last, NS), Yp, zero, tiles), SHARE)
            AB[0], AB[1] = a[1:], b[1:]
            STC[...] = tiles.pop()
            squeeze(j + 1, [lax.rem(t + last - 1 + k, NS) for k in QUAD], tiles)
            return carry

        lax.fori_loop(0, NS // ahead, body, 0)
        send_rows(j + 1, 3, *EDGES[3])
        send_sums(j + 1, 3, *SUMS[3])
        tiles = [STC[...]]
        for _ in epi_gen(j, last, Y1, still, tiles):
            pass
        if j < 2:
            for _ in prep_of(j + 1, 0, L0, AB[0, :1], AB[1, :1]):
                pass
        squeeze(j + 1, (last - 1, last), tiles)
        send_sums(j + 1, 4, *SUMS[4])
        send_rows(j + 1, 4, *EDGES[4])

    for g in range(len(SUMS)):
        wait_sums(3, g, SUMS[g][1])
        if g > 0:
            wait_rows(3, g, EDGES[g][1])
        for slot in QUAD:
            sums_bytes(slot, SUMS[g][1], st_send, g).wait()
            if slot != 1:
                out_copy(slot, g, *EDGES[g]).wait()
            if slot > 0:
                up, down = rows_copies(slot, g, *EDGES[g])
                if_up(up.wait_send)
                if_dn(lambda down=down: [c.wait_send() for c in down] and None)
        if_up(rows_copies(3, g, *EDGES[g])[1][1].wait_recv)
    if_dn(q_dn.wait_send)
    if_up(q_up.wait_send)
    fins = [pltpu.make_async_copy(r, halo.at[k], fin_sem.at[k]) for k, r in enumerate((HT.at[2], HT.at[3], HX, HB.at[3]))]
    for f in fins:
        f.start()
    for k in QUAD:
        for c, v in enumerate(scales((3,) * ahead, range(ahead * k, ahead * k + ahead))):
            abo[c, span(k, ahead)] = v
    for f in fins:
        f.wait()


def tail(hand, hand0, halo, ab, b2, bd, w2, dw, h0o, h1o, h2o, do,
         H, U, HA, P0, X2, W, WR, L0, L1, Y0, Y1, O1, O2, OD, DS, in_sem, ha_sem, p_sem, wm_sem, wr_sem, o_sem, od_sem):
    me, sp = lax.axis_index("sp"), lax.axis_size("sp")
    has_up, has_dn = (me > 0).astype(jnp.int32), (me < sp - 1).astype(jnp.int32)

    def gets(s):
        return ([pltpu.make_async_copy(hand.at[k, s], (H, U)[k].at[s], in_sem.at[k, s]) for k in (1, 0)]
                + [pltpu.make_async_copy(halo.at[k, s], HA.at[k, s], ha_sem.at[k, s]) for k in QUAD])

    def take0(s):
        return pltpu.make_async_copy(hand0.at[s], P0.at[s], p_sem.at[s])

    def fetch(s, carry):
        for c in gets(s):
            c.start()
        return carry

    def ready(s):
        for c in gets(s):
            c.wait()

    fetch(0, 0)
    parts = [(W.at[j], WR.at[j], wm_sem.at[j], wr_sem.at[j]) for j in DUO]
    weight_copies(w2.at[1], *parts[0])
    lax.fori_loop(1, len(QUAD) + 1, fetch, 0)

    def prep_of(s, L):
        def row(r):
            if r < 2:
                return unpack_row(HA.at[2 - r, s]), has_up
            if r == ROWS + 2:
                return unpack_row(HA.at[3, s]), has_dn
            return U[s, span(r - 2), :], None
        return prep_gen(row, ROWS + 1, ab[0, pl.ds(s, 1)], ab[1, pl.ds(s, 1)], L)

    def epi_gen(s, Y, zero):
        for o in range(ROWS + 1):
            t = [x.astype(BF) for x in conv_row(Y, o, zero)]
            edge = unpack_row(HA.at[0, s]) if o == 0 else None
            for k in TRI:
                cols = span(k, LANE)
                old = edge[:, cols] if o == 0 else H[s, span(o - 1), cols]
                new = old.astype(F32) + t[k].astype(F32)
                new = (keep_if(has_up, new) if o == 0 else new).astype(BF)
                X2[s, span(o), cols] = new
                if o > 0:
                    n = min(LANE, CH - k * LANE)
                    cols = slice(k * LANE, k * LANE + n)
                    O1[s, span(o - 1), cols] = old[:, :n]
                    O2[s, span(o - 1), cols] = new[:, :n]
            yield t[2]

    def put(k, s):
        src, dst = ((P0, h0o), (O1, h1o), (O2, h2o))[k]
        return pltpu.make_async_copy(src.at[s], dst.at[s], o_sem.at[k, s])

    ready(0)
    for _ in prep_of(0, L0):
        pass
    weight_finish(b2[1:2, :], *parts[0])
    weight_copies(dw, *parts[1])

    for Y in (Y0, Y1):
        Y[...] = jnp.zeros_like(Y)
    ahead = len(QUAD)

    def body(i, carry):
        t = ahead * i
        zero = nil(i)
        for k in QUAD:
            pl.when(t + k + 1 < NS)(functools.partial(ready, t + k + 1))
            pl.when(t + k + ahead + 1 < NS)(functools.partial(fetch, t + k + ahead + 1, None))
            take0(t + k).start()

        @pl.when(i > 0)
        def _():
            for k in QUAD:
                take0(t - ahead + k).wait()
                put(0, t - ahead + k).start()

        for k in QUAD:
            @pl.when(t + k > ahead)
            def _(n=t + k - 5):
                put(1, n).start()
                put(2, n).start()
        for u in QUAD:
            if u % 2:
                Lc, Ln, Yc, Yp = L1, L0, Y1, Y0
            else:
                Lc, Ln, Yc, Yp = L0, L1, Y0, Y1
            weave(Lc, W.at[0], Yc, NP + ROW, prep_of(jnp.minimum(t + u + 1, NS - 1), Ln), epi_gen(lax.rem(t + u + NS - 1, NS), Yp, zero), SHARE)
        return carry

    lax.fori_loop(0, NS // ahead, body, 0)
    still = nil(me)
    for _ in epi_gen(NS - 1, Y1, still):
        pass
    for s in range(NS - ahead - 1, NS):
        put(1, s).start()
        put(2, s).start()
    for s in range(NS - ahead, NS):
        take0(s).wait()
        put(0, s).start()
    weight_finish(bd[...].reshape(1, CH), *parts[1])

    def dprep(s, L):
        for o in QUAD:
            xs = [X2[s, span(2 * o + dy), :] for dy in TRI]
            for dy in TRI:
                L[span(o), span(dy, MAIN)] = xs[dy][:, :MAIN]
            store_rest(L, o, *(x[:, MAIN:].astype(F32) for x in xs))

    def depi(s, Y, zero):
        for o in QUAD:
            d = conv_row(Y, o, zero)
            for k in TRI:
                DS[o, k] = d[k]
            parts = [DS[o, k, pl.ds(0, ROW // 2, stride=2), :] for k in TRI]
            OD[s, span(o, ROW // 2), :] = jnp.concatenate(parts, 1)[:, :CH].astype(BF)

    def dhalf(t, Lc, Ln, Yc, Yp, zero):
        for n in QUAD:
            dot_chunk(Lc, W.at[1], Yc, slice(0, NP // 2), n)
        dprep(jnp.minimum(t + 1, NS - 1), Ln)
        depi(lax.rem(t + NS - 1, NS), Yp, zero)

    dprep(0, L0)

    def dbody(i, carry):
        t = 2 * i
        zero = nil(i)
        dhalf(t, L0, L1, Y0, Y1, zero)
        dhalf(t + 1, L1, L0, Y1, Y0, zero)
        return carry

    lax.fori_loop(0, NS // 2, dbody, 0)
    depi(NS - 1, Y1, still)
    dout = pltpu.make_async_copy(OD, do, od_sem)
    dout.start()

    def drain(s, carry):
        for k in TRI:
            put(k, s).wait()
        return carry

    lax.fori_loop(0, NS, drain, 0)
    dout.wait()


def solution(mesh):
    sp = mesh.shape["sp"]

    def program(latent, time_emb, w_in, b_in, gn1_scale, gn1_shift, conv1_w, conv1_b, temb_w, temb_b, gn2_scale, gn2_shift, conv2_w, conv2_b, down_w, down_b):
        none = (0, 0)
        lat = jnp.pad(latent.transpose(0, 3, 1, 2), (none, none, none, (1, 1)))
        q = jnp.stack([lat[..., d:d + ROW] for d in TRI], 1).reshape(NS, 12, NP)
        q = jnp.pad(q, (none, (0, 4), none), constant_values=1)

        dma, vm = pltpu.SemaphoreType.DMA, pltpu.VMEM
        any_, vms = pl.BlockSpec(memory_space=pl.ANY), pl.BlockSpec(memory_space=pltpu.VMEM)
        params = functools.partial(pltpu.CompilerParams, vmem_limit_bytes=66_000_000)

        def big(n=NP, c=CP):
            return vm((NS, n, c), BF)

        def edge(n):
            return vm((n, NS, PK, MAIN), BF)

        def bufs(m):
            return [vm((m, KP), BF)] * 2 + [vm((8, m + 2 * OFF, LANE), F32)] * 2

        def out(*shape):
            return jax.ShapeDtypeStruct(shape, BF)

        hand, hand0, halo, ab = pl.pallas_call(
            functools.partial(mega, sp),
            out_shape=(out(2, NS, NP, CP), out(NS, NP, CH), out(SLOTS, NS, PK, MAIN), jax.ShapeDtypeStruct((2, NS, CP), F32)),
            in_specs=[vms] * 11 + [any_] * 3, out_specs=(any_, any_, any_, vms),
            scratch_shapes=[big(), big(), big(), big(NP, CH), vm((3, KP, KP), BF), vm((3, 9, CH, ROW), BF), vm((2, CH, temb_w.shape[1]), BF), vm((3 * NS, CP), F32)] + bufs(NP)
            + [vm((NS, OFF, LANE), F32), vm((OFF, LANE), F32), vm((SLOTS, NS, 2, LANE), F32), vm((SLOTS, sp - 1, NS, 2, LANE), F32), vm((2, 3, CP), F32), vm((SLOTS, NS, CP), F32), vm((OFF, CP), F32),
               edge(4), edge(4), big(PK, MAIN), edge(3), edge(3), big(PK, MAIN), vm((2, NS, NS, LANE), BF),
               dma((3,)), dma((3,)), dma] + [dma((2,))] * 2 + [dma((SLOTS, len(SUMS)))] * SLOTS + [dma((len(SUMS),))]
            + [dma((SLOTS, len(SUMS)))] * 2 + [dma((len(SUMS),)), dma((SLOTS, len(SUMS))), dma((4,))],
            compiler_params=params(collective_id=0, has_side_effects=True), name="mega",
        )(q, w_in, b_in, time_emb, temb_b, gn1_scale, gn1_shift, gn2_scale, gn2_shift, conv1_b, conv2_b, temb_w.transpose(0, 2, 1), conv1_w, conv2_w)
        outs = pl.pallas_call(
            tail,
            out_shape=(out(NS, NP, CH),) * 3 + (out(NS, NP // 4, CH),),
            in_specs=[any_] * 3 + [vms] * 3 + [any_] * 2, out_specs=(any_,) * 4,
            scratch_shapes=[big(), big(), edge(4), big(NP, CH), big(NP + ROW), vm((2, KP, KP), BF), vm((2, 9, CH, ROW), BF)] + bufs(NP + ROW)
            + [big(NP, CH), big(NP, CH), big(NP // 4, CH), vm((4, 3, ROW, LANE), F32),
               dma((2, NS)), dma((SLOTS, NS)), dma((NS,)), dma((2,)), dma((2,)), dma((3, NS)), dma],
            compiler_params=params(), name="tail",
        )(hand, hand0, halo, ab, conv2_b, down_b, conv2_w, down_w)
        return tuple(o.reshape(NS, n, m, CH) for o, n, m in zip(outs, [ROWS] * len(TRI) + [ROWS // 2], [ROW] * len(TRI) + [ROW // 2]))

    band = P("dp", "sp", None, None)
    return jax.shard_map(program, mesh=mesh, in_specs=(band, P("dp", None)) + (P(),) * 14, out_specs=(band,) * 4, check_vma=False)
```

```python
import functools

import jax
import jax.numpy as jnp
from jax import lax
from jax.experimental import pallas as pl
from jax.experimental.pallas import tpu as pltpu
from jax.sharding import PartitionSpec as P

F32, BF = jnp.float32, jnp.bfloat16
GN_GROUPS, GN_EPS = 32, 1e-5
NS, ROWS, ROW, LANE, MAIN = 16, 8, 64, 128, 256
NP = ROWS * ROW
CH = 320
CP = CH + ROW
KP = 4 * MAIN
REST = 3 * MAIN
SPARE = 3 * CH
OFF = 8
GSIZE = CH // GN_GROUPS
PK = ROW + NS
MESH = pl.DeviceIdType.MESH
DUO, TRI, QUAD = range(2), range(3), range(4)
SLOTS = len(QUAD)
NIL = 0.0


def groups(n, step):
    cuts = [0, *range(n, NS, step), NS]
    return [(a, b - a) for a, b in zip(cuts, cuts[1:])]


SUMS, EDGES = groups(2, SLOTS), groups(3, SLOTS)
SHARE = (1, 2, 3, 3)
ACC32 = dict(preferred_element_type=F32)
ROWS_DOT, COLS_DOT = ((((k,), (k,)), ((), ())) for k in DUO)


def nil(i):
    return jnp.minimum(i, 0) * OFF


def span(i, n=ROW, base=0):
    return slice(base + i * n, base + (i + 1) * n)


def low_half():
    return lax.broadcasted_iota(jnp.int32, (ROW, LANE), 1) < ROW


def widen(p):
    return jnp.concatenate([p, p[..., MAIN:]], -1)


def keep_if(flag, x):
    return jnp.where(jnp.full(x.shape, flag, jnp.int32) > 0, x, NIL)


def store_rest(L, o, r0, r1, r2):
    low = low_half()
    L[span(o), REST:REST + LANE] = jnp.where(low, r0, r1).astype(BF)
    L[span(o), REST + LANE:] = jnp.where(low, r2, 1.0).astype(BF)


def prep_gen(x_of_row, nrows, a, b, L):
    ha, hb = a * 0.5, b * 0.5
    rest = []
    for r in range(nrows + 2):
        x, flag = x_of_row(r)
        h = x.astype(F32) * ha + hb
        n = h + h * jnp.tanh(h)
        if flag is not None:
            n = keep_if(flag, n)
        main = n[:, :MAIN].astype(BF)
        rest.append(n[:, MAIN:])
        for dy in TRI:
            if 0 <= r - dy < nrows:
                L[span(r - dy), span(dy, MAIN)] = main
        if r >= 2:
            store_rest(L, r - 2, *rest[r - 2:])
        yield main


def shifted(v, step):
    v = pltpu.roll(v.reshape(OFF, OFF, LANE), step % OFF, 1)
    sub = lax.broadcasted_iota(jnp.int32, v.shape, 1)
    gap = jnp.zeros_like(v[:1])
    if step > 0:
        v = jnp.where(sub == 0, jnp.concatenate([gap, v[:-1]], 0), v)
    else:
        v = jnp.where(sub == OFF - 1, jnp.concatenate([v[1:], gap], 0), v)
    return v.reshape(ROW, LANE)


def conv_row(Y, o, zero):
    def here(k):
        return Y[k, span(o, base=OFF), :]

    out = [shifted(here(k), 1) + here(k + 2) + shifted(here(k + 4), -1) for k in DUO]
    a = here(6)
    mix = jnp.where(low_half(), shifted(a, 1), a)
    return out + [mix + pltpu.roll(mix, ROW, 1) + shifted(here(7), -1)]


def dot_chunk(L, W, Y, rows, n):
    r = jnp.dot(L[rows, :], W[:, span(n, MAIN)], **ACC32)
    for k in DUO:
        Y[2 * n + k, OFF + rows.start:OFF + rows.stop, :] = r[:, span(k, LANE)]


def weave(L, W, Y, m, prep, epi, share):
    work = [prep] * (m // ROW + 2) + [epi] * (m // ROW)
    done = 0
    for n in QUAD:
        dot_chunk(L, W, Y, slice(0, m), n)
        upto = len(work) * share[n] // share[-1]
        for g in work[done:upto]:
            mark = next(g)
        done = upto
        if n < len(QUAD) - 1:
            L[:NS, KP - NS:] = jnp.where(mark[:NS, LANE - NS:LANE].astype(F32) > NIL, 1.0, NIL).astype(BF)
    for g in (prep, epi):
        for _ in g:
            pass


def lane_left(x, k):
    return pltpu.roll(x, CP - k, 1)


def starts(k):
    lane = lax.broadcasted_iota(jnp.int32, (OFF, LANE), 1) + k * LANE
    return (lane % GSIZE == 0) & (lane < CH)


def stacked(rows):
    fill = [jnp.zeros((4 - len(rows), rows[0].shape[1]), F32)] * (len(rows) < 4)
    return jnp.concatenate(list(rows) + fill, 0)


def compact(tiles, embs):
    s = stacked([jnp.concatenate([t[k:k + 1] for k in TRI], 1) for t in tiles])
    q = stacked([jnp.concatenate([t[k + 3:k + 4] for k in TRI], 1) for t in tiles])
    e = stacked(embs)
    x = jnp.concatenate([s + float(NP) * e, q + e * (2.0 * s + float(NP) * e)], 0)
    w2 = x + lane_left(x, 1)
    w4 = w2 + lane_left(w2, 2)
    w8 = w4 + lane_left(w4, 4)
    w10 = w8 + lane_left(w2, 8)
    c = sum(jnp.where(starts(k), w10[:, span(k, LANE)], NIL) for k in TRI)
    return [jnp.concatenate([c[k:k + 1], c[k + 4:k + 5]], 0) for k in range(len(tiles))]


def affine(tots, gains, shifts, embs, count):
    x = jnp.concatenate([stacked([t[k:k + 1] for t in tots]) for k in DUO], 0)
    y = jnp.concatenate([jnp.where(starts(k), x, NIL) for k in TRI], 1)
    r2 = y + pltpu.roll(y, 1, 1)
    r4 = r2 + pltpu.roll(r2, 2, 1)
    r8 = r4 + pltpu.roll(r4, 4, 1)
    r = r8 + pltpu.roll(r2, 8, 1)
    lane = lax.broadcasted_iota(jnp.int32, (OFF, CP), 1)
    r = jnp.where(lane >= CH, pltpu.roll(r, ROW, 1), r) * (1.0 / count)
    mean, msq = r[:4], r[4:]
    a = stacked(gains) * lax.rsqrt(msq - mean * mean + GN_EPS)
    return a, stacked(shifts) + a * (stacked(embs) - mean)


def pack_row(dst, x):
    dst[:ROW, :] = jnp.concatenate(x[:2], 1)
    half = ROW // 2
    p = jnp.where(low_half()[:half], x[2][:half].astype(F32), x[2][half:].astype(F32))
    dst[ROW:, :] = jnp.concatenate([p[:NS], p[NS:]], 1).astype(BF)


def unpack_row(src):
    p = src[ROW:, :].astype(F32)
    p = jnp.concatenate([p[:, :LANE], p[:, LANE:]], 0)
    swap, low = pltpu.roll(p, ROW, 1), low_half()[:ROW // 2]
    rest = jnp.concatenate([jnp.where(low, p, swap), jnp.where(low, swap, p)], 0)
    return jnp.concatenate([src[:ROW, :].astype(F32), rest], 1)


def stats_tile(acc, acq):
    parts = [x.sum(0, keepdims=True) for x in acc + acq]
    return jnp.concatenate(parts + [jnp.zeros((2, LANE), F32)], 0)


def add_stats(acc, acq, new):
    for k, x in enumerate(new):
        v = x.astype(F32).reshape(OFF, OFF, LANE)
        acc[k] = acc[k] + v.sum(0)
        acq[k] = acq[k] + (v * v).sum(0)


def no_stats():
    return [jnp.zeros((OFF, LANE), F32) for _ in TRI]


def weight_copies(src, W, WR, sem_main, sem_rest):
    for dy in TRI:
        for dx in TRI:
            cols = span(dx, MAIN)
            pltpu.make_async_copy(src.at[dy, dx, :MAIN, :MAIN], W.at[span(dy, MAIN), cols], sem_main).start()
            pltpu.make_async_copy(src.at[dy, dx, MAIN:, :MAIN], W.at[span(dy, base=REST), cols], sem_main).start()
            pltpu.make_async_copy(src.at[dy, dx, :, MAIN:], WR.at[dy * 3 + dx], sem_rest).start()


def weight_finish(bias, W, WR, sem_main, sem_rest):
    main = W.at[:SPARE, :REST]
    pltpu.make_async_copy(main, main, sem_main).wait()
    pltpu.make_async_copy(WR, WR, sem_rest).wait()
    for dy in TRI:
        for part, rows in ((slice(0, MAIN), span(dy, MAIN)), (slice(MAIN, CH), span(dy, base=REST))):
            w0, w1, w2 = (WR[dy * 3 + dx, part, :] for dx in TRI)
            W[rows, REST:REST + LANE] = jnp.concatenate([w0, w1], 1)
            W[rows, REST + LANE:] = jnp.concatenate([w2, w2], 1)
    b = widen(bias.astype(F32))
    gap = jnp.zeros((1, MAIN), F32)
    rest = jnp.where(low_half()[:1], 0.0, b[:, MAIN:])
    row = jnp.concatenate([gap, b[:, :MAIN], gap, rest, gap[:, :LANE]], 1)
    first = lax.broadcasted_iota(jnp.int32, (ROW, KP), 0) == 0
    W[SPARE:, :] = jnp.where(first, row, NIL).astype(BF)


def mega(sp, q, wi, bi, temb, tb, g1, s1, g2, s2, b1, b2, tw, w1, w2, hand, hand0, halo, abo,
         H, U, H2, HS, W, WR, TW, WI, L0, L1, Y0, Y1, ST, STC, SG, RS, AB, EMB, GAIN, HT, HB, HX, PT, PB, PX, LQ,
         wm_sem, wr_sem, tw_sem, q_send, q_recv, st_send, st_recv, up_send, dn_send, x_send, ht_recv, hb_recv, hx_recv, out_sem, fin_sem):
    me, dp = lax.axis_index("sp"), lax.axis_index("dp")
    has_up, has_dn = (me > 0).astype(jnp.int32), (me < sp - 1).astype(jnp.int32)
    held = (H, U, H2, U)
    last = NS - 1

    get_tw = pltpu.make_async_copy(tw, TW, tw_sem)
    get_tw.start()
    for j, src in enumerate((w1.at[0], w2.at[0], w1.at[1])):
        weight_copies(src, W.at[j], WR.at[j], wm_sem.at[j], wr_sem.at[j])

    barrier = pltpu.get_barrier_semaphore()
    for k in range(1, sp):
        pl.semaphore_signal(barrier, inc=1, device_id=(dp, lax.rem(me + k, sp)), device_id_type=MESH)
    pl.semaphore_wait(barrier, sp - 1)

    def remote(src, dst, ssem, rsem, dev):
        return pltpu.make_async_remote_copy(src_ref=src, dst_ref=dst, send_sem=ssem, recv_sem=rsem, device_id=(dp, dev), device_id_type=MESH)

    def if_up(f):
        pl.when(me > 0)(f)

    def if_dn(f):
        pl.when(me < sp - 1)(f)

    q_dn = remote(q.at[:, :, NP - LANE:], LQ.at[0], q_send.at[0], q_recv.at[0], me + 1)
    q_up = remote(q.at[:, :, :LANE], LQ.at[1], q_send.at[1], q_recv.at[1], me - 1)
    if_dn(q_dn.start)
    if_up(q_up.start)

    def rows_copies(slot, g, lo, n):
        ss = pl.ds(lo, n)
        up = remote(PT.at[slot - 1, ss], HB.at[slot, ss], up_send.at[slot, g], hb_recv.at[slot, g], me - 1)
        down = [remote(PB.at[slot - 1, ss], HT.at[slot, ss], dn_send.at[slot, g], ht_recv.at[slot, g], me + 1)]
        if slot == 3:
            down.append(remote(PX.at[ss], HX.at[ss], x_send.at[g], hx_recv.at[g], me + 1))
        return up, down

    def out_copy(slot, g, lo, n):
        src, dst = ((HS, hand0), None, (H2, hand.at[0]), (U, hand.at[1]))[slot]
        ss = pl.ds(lo, n)
        return pltpu.make_async_copy(src.at[ss], dst.at[ss], out_sem.at[slot, g])

    def send_sums(slot, g, lo, n):
        ss = pl.ds(lo, n)
        for k in range(1, sp):
            remote(SG.at[slot, ss], RS.at[slot, k - 1, ss], st_send.at[slot, g], st_recv.at[slot, g], lax.rem(me + k, sp)).start()

    def send_rows(slot, g, lo, n):
        if slot != 1:
            out_copy(slot, g, lo, n).start()
        if slot > 0:
            up, down = rows_copies(slot, g, lo, n)
            if_up(up.start)
            if_dn(lambda: [c.start() for c in down] and None)

    def sums_bytes(slot, n, sem, g):
        both = RS.at[slot, :, :n]
        return pltpu.make_async_copy(both, both, sem.at[slot, g])

    def wait_sums(slot, g, n):
        sums_bytes(slot, n, st_recv, g).wait()

    def wait_rows(slot, g, n):
        ss = pl.ds(0, n)
        if_up(lambda: remote(PB.at[0, ss], HT.at[slot, ss], dn_send.at[slot, g], ht_recv.at[slot, g], me).wait_recv())
        if_dn(lambda: remote(PT.at[0, ss], HB.at[slot, ss], up_send.at[slot, g], hb_recv.at[slot, g], me).wait_recv())

    def squeeze(slot, ss, tiles):
        for r, s in zip(compact(tiles, [EMB[slot, pl.ds(s, 1)] for s in ss]), ss):
            SG[slot, s] = r

    for k, (ref, l) in enumerate((ref, l) for pair in ((g1, g2), (s1, s2)) for l in DUO for ref in pair):
        GAIN[k:k + 1, :] = widen(ref[l:l + 1, :].astype(F32))
    WI[...] = jnp.zeros_like(WI)
    for dy in TRI:
        for dx in TRI:
            WI[span(4 * dy + dx, 4), :] = widen(wi[dy, dx].astype(F32))
    WI[NS + 12:NS + 13, :] = widen(bi[...].reshape(1, CH).astype(F32))
    get_tw.wait()
    x = temb[...].astype(F32)
    act = (x * jax.nn.sigmoid(x)).astype(BF)
    for l in DUO:
        pr = lax.dot_general(act, TW[l], COLS_DOT, **ACC32)
        EMB[2 * l] = jnp.zeros((NS, CP), F32)
        EMB[2 * l + 1] = widen(pr + tb[l:l + 1, :].astype(F32))

    if_up(q_dn.wait_recv)
    if_dn(q_up.wait_recv)

    def first(s):
        above, below = keep_if(has_up, LQ[0, s].astype(F32)), keep_if(has_dn, LQ[1, s].astype(F32))
        ext = jnp.concatenate([above, q[s].astype(F32), below], 1)
        mid = pltpu.roll(ext, ext.shape[1] - ROW, 1)
        wide = NP + LANE
        lhs = jnp.concatenate([ext[:, :wide], mid[:, :wide], ext[:, LANE:]], 0).astype(BF)
        r = lax.dot_general(lhs, WI[...].astype(BF), ROWS_DOT, **ACC32)
        acc, acq = no_stats(), no_stats()
        for o in range(ROWS + 2):
            x = r[span(o), :].astype(BF)
            parts = [x[:, span(k, LANE)] for k in TRI]
            if o == 0:
                pack_row(HT.at[0, s], parts)
            elif o > ROWS:
                pack_row(HB.at[0, s], parts)
            else:
                H[s, span(o - 1), :] = x
                HS[s, span(o - 1), :] = x[:, :CH]
                add_stats(acc, acq, parts)
        ST[s] = stats_tile(acc, acq)

    def first_pair(i, carry):
        t = 2 * i
        for g in TRI:
            for parts, send in ((EDGES, send_rows), (SUMS, send_sums)):
                pl.when(i == 2 * g + 2)(functools.partial(send, 0, g, *parts[g]))
        ss = [lax.rem(n + NS, NS) for n in (t - 2, t - 1)]
        tiles = [ST[s] for s in ss]
        first(t)
        first(t + 1)
        squeeze(0, ss, tiles)
        return carry

    lax.fori_loop(0, NS // 2, first_pair, 0)
    squeeze(0, (last - 1, last), (ST[last - 1], ST[last]))
    for j in TRI:
        weight_finish((b1, b2)[j % 2][j // 2:j // 2 + 1, :], W.at[j], WR.at[j], wm_sem.at[j], wr_sem.at[j])
    for g in (3, 4):
        send_sums(0, g, *SUMS[g])
        send_rows(0, g, *EDGES[g])

    def scales(slots, ss):
        tots = []
        for slot, s in zip(slots, ss):
            tots.append(SG[slot, s])
            for k in range(sp - 1):
                tots[-1] = tots[-1] + RS[slot, k, s]
        return affine(tots, [GAIN[pl.ds(k, 1)] for k in slots], [GAIN[pl.ds(k + SLOTS, 1)] for k in slots],
                      [EMB[k, pl.ds(s, 1)] for k, s in zip(slots, ss)], float(sp * NP * GSIZE))

    def prep_of(slot, s, L, a, b):
        def row(r):
            if r == 0:
                return unpack_row(HT.at[slot, s]), has_up
            if r == ROWS + 1:
                return unpack_row(HB.at[slot, s]), has_dn
            return held[slot][s, span(r - 1), :], None
        return prep_gen(row, ROWS, a, b, L)

    def epi_gen(j, s, Y, zero, tiles):
        acc, acq = no_stats(), no_stats()
        edge = {0: PT.at[j, s], ROWS - 1: PB.at[j, s]}
        if j == 2:
            edge[ROWS - 2] = PX.at[s]
        for o in range(ROWS):
            new = [x.astype(BF) for x in conv_row(Y, o, zero)]
            mark = new[2]
            for k in TRI:
                if j == 1:
                    new[k] = (new[k].astype(F32) + H[s, span(o), span(k, LANE)].astype(F32)).astype(BF)
                held[j + 1][s, span(o), span(k, LANE)] = new[k]
            if o in edge:
                pack_row(edge[o], new)
            add_stats(acc, acq, new)
            if o == ROWS - 1:
                tiles.append(stats_tile(acc, acq))
            yield mark

    for Y in (Y0, Y1):
        Y[...] = jnp.zeros_like(Y)
    for g in DUO:
        wait_sums(0, g, SUMS[g][1])
    for c, v in enumerate(scales((0,) * 3, TRI)):
        AB[c] = v[:3]
    still = nil(me)
    ahead = len(QUAD)
    for _ in prep_of(0, 0, L0, AB[0, :1], AB[1, :1]):
        pass
    for j in TRI:
        def body(i, carry, j=j):
            t = ahead * i
            zero = nil(i)
            ns = [jnp.minimum(j * NS + t + 3 + k, 3 * NS - 1) for k in QUAD]
            turn = ahead - 1
            for g in TRI:
                pl.when(i == g)(functools.partial(wait_sums, j, g + 2, SUMS[g + 2][1]))
            for g in DUO:
                if j < 2:
                    pl.when(i == turn)(functools.partial(wait_sums, j + 1, g, SUMS[g][1]))
            if j > 0:
                pl.when(i < turn)(lambda: wait_rows(j, i + 1, ahead))
                pl.when(i == turn)(lambda: wait_rows(j, ahead, 1))
            pl.when(i == turn)(lambda: wait_rows(j + 1, 0, EDGES[0][1]))
            for parts, send in ((EDGES, send_rows), (SUMS, send_sums)):
                for g in TRI:
                    pl.when(i == g + 1)(functools.partial(send, j + 1, g, *parts[g]))
            a, b = scales([n // NS for n in ns], [lax.rem(n, NS) for n in ns])
            co = [(AB[0, k:k + 1], AB[1, k:k + 1]) for k in (1, 2)] + [(a[k:k + 1], b[k:k + 1]) for k in DUO]
            tiles = [STC[...]]
            for u in QUAD:
                nxt = jnp.minimum(t + u + 1, last)
                if u % 2:
                    Lc, Ln, Yc, Yp = L1, L0, Y1, Y0
                else:
                    Lc, Ln, Yc, Yp = L0, L1, Y0, Y1
                weave(Lc, W.at[j], Yc, NP, prep_of(j, nxt, Ln, *co[u]), epi_gen(j, lax.rem(t + u + last, NS), Yp, zero, tiles), SHARE)
            AB[0], AB[1] = a[1:], b[1:]
            STC[...] = tiles.pop()
            squeeze(j + 1, [lax.rem(t + last - 1 + k, NS) for k in QUAD], tiles)
            return carry

        lax.fori_loop(0, NS // ahead, body, 0)
        send_rows(j + 1, 3, *EDGES[3])
        send_sums(j + 1, 3, *SUMS[3])
        tiles = [STC[...]]
        for _ in epi_gen(j, last, Y1, still, tiles):
            pass
        if j < 2:
            for _ in prep_of(j + 1, 0, L0, AB[0, :1], AB[1, :1]):
                pass
        squeeze(j + 1, (last - 1, last), tiles)
        send_sums(j + 1, 4, *SUMS[4])
        send_rows(j + 1, 4, *EDGES[4])

    for g in range(len(SUMS)):
        wait_sums(3, g, SUMS[g][1])
        if g > 0:
            wait_rows(3, g, EDGES[g][1])
        for slot in QUAD:
            sums_bytes(slot, SUMS[g][1], st_send, g).wait()
            if slot != 1:
                out_copy(slot, g, *EDGES[g]).wait()
            if slot > 0:
                up, down = rows_copies(slot, g, *EDGES[g])
                if_up(up.wait_send)
                if_dn(lambda down=down: [c.wait_send() for c in down] and None)
        if_up(rows_copies(3, g, *EDGES[g])[1][1].wait_recv)
    if_dn(q_dn.wait_send)
    if_up(q_up.wait_send)
    fins = [pltpu.make_async_copy(r, halo.at[k], fin_sem.at[k]) for k, r in enumerate((HT.at[2], HT.at[3], HX, HB.at[3]))]
    for f in fins:
        f.start()
    for k in QUAD:
        for c, v in enumerate(scales((3,) * ahead, range(ahead * k, ahead * k + ahead))):
            abo[c, span(k, ahead)] = v
    for f in fins:
        f.wait()


def tail(hand, hand0, halo, ab, b2, bd, w2, dw, h0o, h1o, h2o, do,
         H, U, HA, P0, X2, W, WR, L0, L1, Y0, Y1, O1, O2, OD, DS, in_sem, ha_sem, p_sem, wm_sem, wr_sem, o_sem, od_sem):
    me, sp = lax.axis_index("sp"), lax.axis_size("sp")
    has_up, has_dn = (me > 0).astype(jnp.int32), (me < sp - 1).astype(jnp.int32)

    def gets(s):
        return ([pltpu.make_async_copy(hand.at[k, s], (H, U)[k].at[s], in_sem.at[k, s]) for k in (1, 0)]
                + [pltpu.make_async_copy(halo.at[k, s], HA.at[k, s], ha_sem.at[k, s]) for k in QUAD])

    def take0(s):
        return pltpu.make_async_copy(hand0.at[s], P0.at[s], p_sem.at[s])

    def fetch(s, carry):
        for c in gets(s):
            c.start()
        return carry

    def ready(s):
        for c in gets(s):
            c.wait()

    fetch(0, 0)
    parts = [(W.at[j], WR.at[j], wm_sem.at[j], wr_sem.at[j]) for j in DUO]
    weight_copies(w2.at[1], *parts[0])
    lax.fori_loop(1, len(QUAD) + 1, fetch, 0)

    def prep_of(s, L):
        def row(r):
            if r < 2:
                return unpack_row(HA.at[2 - r, s]), has_up
            if r == ROWS + 2:
                return unpack_row(HA.at[3, s]), has_dn
            return U[s, span(r - 2), :], None
        return prep_gen(row, ROWS + 1, ab[0, pl.ds(s, 1)], ab[1, pl.ds(s, 1)], L)

    def epi_gen(s, Y, zero):
        for o in range(ROWS + 1):
            t = [x.astype(BF) for x in conv_row(Y, o, zero)]
            edge = unpack_row(HA.at[0, s]) if o == 0 else None
            for k in TRI:
                cols = span(k, LANE)
                old = edge[:, cols] if o == 0 else H[s, span(o - 1), cols]
                new = old.astype(F32) + t[k].astype(F32)
                new = (keep_if(has_up, new) if o == 0 else new).astype(BF)
                X2[s, span(o), cols] = new
                if o > 0:
                    n = min(LANE, CH - k * LANE)
                    cols = slice(k * LANE, k * LANE + n)
                    O1[s, span(o - 1), cols] = old[:, :n]
                    O2[s, span(o - 1), cols] = new[:, :n]
            yield t[2]

    def put(k, s):
        src, dst = ((P0, h0o), (O1, h1o), (O2, h2o))[k]
        return pltpu.make_async_copy(src.at[s], dst.at[s], o_sem.at[k, s])

    ready(0)
    for _ in prep_of(0, L0):
        pass
    weight_finish(b2[1:2, :], *parts[0])
    weight_copies(dw, *parts[1])

    for Y in (Y0, Y1):
        Y[...] = jnp.zeros_like(Y)
    ahead = len(QUAD)

    def body(i, carry):
        t = ahead * i
        zero = nil(i)
        for k in QUAD:
            pl.when(t + k + 1 < NS)(functools.partial(ready, t + k + 1))
            pl.when(t + k + ahead + 1 < NS)(functools.partial(fetch, t + k + ahead + 1, None))
            take0(t + k).start()

        @pl.when(i > 0)
        def _():
            for k in QUAD:
                take0(t - ahead + k).wait()
                put(0, t - ahead + k).start()

        for k in QUAD:
            @pl.when(t + k > ahead)
            def _(n=t + k - 5):
                put(1, n).start()
                put(2, n).start()
        for u in QUAD:
            if u % 2:
                Lc, Ln, Yc, Yp = L1, L0, Y1, Y0
            else:
                Lc, Ln, Yc, Yp = L0, L1, Y0, Y1
            weave(Lc, W.at[0], Yc, NP + ROW, prep_of(jnp.minimum(t + u + 1, NS - 1), Ln), epi_gen(lax.rem(t + u + NS - 1, NS), Yp, zero), SHARE)
        return carry

    lax.fori_loop(0, NS // ahead, body, 0)
    still = nil(me)
    for _ in epi_gen(NS - 1, Y1, still):
        pass
    for s in range(NS - ahead - 1, NS):
        put(1, s).start()
        put(2, s).start()
    for s in range(NS - ahead, NS):
        take0(s).wait()
        put(0, s).start()
    weight_finish(bd[...].reshape(1, CH), *parts[1])

    def dprep(s, L):
        for o in QUAD:
            xs = [X2[s, span(2 * o + dy), :] for dy in TRI]
            for dy in TRI:
                L[span(o), span(dy, MAIN)] = xs[dy][:, :MAIN]
            store_rest(L, o, *(x[:, MAIN:].astype(F32) for x in xs))

    def depi(s, Y, zero):
        for o in QUAD:
            d = conv_row(Y, o, zero)
            for k in TRI:
                DS[o, k] = d[k]
            parts = [DS[o, k, pl.ds(0, ROW // 2, stride=2), :] for k in TRI]
            OD[s, span(o, ROW // 2), :] = jnp.concatenate(parts, 1)[:, :CH].astype(BF)

    def dhalf(t, Lc, Ln, Yc, Yp, zero):
        for n in QUAD:
            dot_chunk(Lc, W.at[1], Yc, slice(0, NP // 2), n)
        dprep(jnp.minimum(t + 1, NS - 1), Ln)
        depi(lax.rem(t + NS - 1, NS), Yp, zero)

    dprep(0, L0)

    def dbody(i, carry):
        t = 2 * i
        zero = nil(i)
        dhalf(t, L0, L1, Y0, Y1, zero)
        dhalf(t + 1, L1, L0, Y1, Y0, zero)
        return carry

    lax.fori_loop(0, NS // 2, dbody, 0)
    depi(NS - 1, Y1, still)
    dout = pltpu.make_async_copy(OD, do, od_sem)
    dout.start()

    def drain(s, carry):
        for k in TRI:
            put(k, s).wait()
        return carry

    lax.fori_loop(0, NS, drain, 0)
    dout.wait()


def solution(mesh):
    sp = mesh.shape["sp"]

    def program(latent, time_emb, w_in, b_in, gn1_scale, gn1_shift, conv1_w, conv1_b, temb_w, temb_b, gn2_scale, gn2_shift, conv2_w, conv2_b, down_w, down_b):
        none = (0, 0)
        lat = jnp.pad(latent.transpose(0, 3, 1, 2), (none, none, none, (1, 1)))
        q = jnp.stack([lat[..., d:d + ROW] for d in TRI], 1).reshape(NS, 12, NP)
        q = jnp.pad(q, (none, (0, 4), none), constant_values=1)

        dma, vm = pltpu.SemaphoreType.DMA, pltpu.VMEM
        any_, vms = pl.BlockSpec(memory_space=pl.ANY), pl.BlockSpec(memory_space=pltpu.VMEM)
        params = functools.partial(pltpu.CompilerParams, vmem_limit_bytes=66_000_000)

        def big(n=NP, c=CP):
            return vm((NS, n, c), BF)

        def edge(n):
            return vm((n, NS, PK, MAIN), BF)

        def bufs(m):
            return [vm((m, KP), BF)] * 2 + [vm((8, m + 2 * OFF, LANE), F32)] * 2

        def out(*shape):
            return jax.ShapeDtypeStruct(shape, BF)

        hand, hand0, halo, ab = pl.pallas_call(
            functools.partial(mega, sp),
            out_shape=(out(2, NS, NP, CP), out(NS, NP, CH), out(SLOTS, NS, PK, MAIN), jax.ShapeDtypeStruct((2, NS, CP), F32)),
            in_specs=[vms] * 11 + [any_] * 3, out_specs=(any_, any_, any_, vms),
            scratch_shapes=[big(), big(), big(), big(NP, CH), vm((3, KP, KP), BF), vm((3, 9, CH, ROW), BF), vm((2, CH, temb_w.shape[1]), BF), vm((3 * NS, CP), F32)] + bufs(NP)
            + [vm((NS, OFF, LANE), F32), vm((OFF, LANE), F32), vm((SLOTS, NS, 2, LANE), F32), vm((SLOTS, sp - 1, NS, 2, LANE), F32), vm((2, 3, CP), F32), vm((SLOTS, NS, CP), F32), vm((OFF, CP), F32),
               edge(4), edge(4), big(PK, MAIN), edge(3), edge(3), big(PK, MAIN), vm((2, NS, NS, LANE), BF),
               dma((3,)), dma((3,)), dma] + [dma((2,))] * 2 + [dma((SLOTS, len(SUMS)))] * SLOTS + [dma((len(SUMS),))]
            + [dma((SLOTS, len(SUMS)))] * 2 + [dma((len(SUMS),)), dma((SLOTS, len(SUMS))), dma((4,))],
            compiler_params=params(collective_id=0, has_side_effects=True), name="mega",
        )(q, w_in, b_in, time_emb, temb_b, gn1_scale, gn1_shift, gn2_scale, gn2_shift, conv1_b, conv2_b, temb_w.transpose(0, 2, 1), conv1_w, conv2_w)
        outs = pl.pallas_call(
            tail,
            out_shape=(out(NS, NP, CH),) * 3 + (out(NS, NP // 4, CH),),
            in_specs=[any_] * 3 + [vms] * 3 + [any_] * 2, out_specs=(any_,) * 4,
            scratch_shapes=[big(), big(), edge(4), big(NP, CH), big(NP + ROW), vm((2, KP, KP), BF), vm((2, 9, CH, ROW), BF)] + bufs(NP + ROW)
            + [big(NP, CH), big(NP, CH), big(NP // 4, CH), vm((4, 3, ROW, LANE), F32),
               dma((2, NS)), dma((SLOTS, NS)), dma((NS,)), dma((2,)), dma((2,)), dma((3, NS)), dma],
            compiler_params=params(), name="tail",
        )(hand, hand0, halo, ab, conv2_b, down_b, conv2_w, down_w)
        return tuple(o.reshape(NS, n, m, CH) for o, n, m in zip(outs, [ROWS] * len(TRI) + [ROWS // 2], [ROW] * len(TRI) + [ROW // 2]))

    band = P("dp", "sp", None, None)
    return jax.shard_map(program, mesh=mesh, in_specs=(band, P("dp", None)) + (P(),) * 14, out_specs=(band,) * 4, check_vma=False)
```

```python
import functools

import jax
import jax.numpy as jnp
from jax import lax
from jax.experimental import pallas as pl
from jax.experimental.pallas import tpu as pltpu
from jax.sharding import PartitionSpec as P

F32, BF = jnp.float32, jnp.bfloat16
GN_GROUPS, GN_EPS = 32, 1e-5
NS, ROWS, ROW, LANE, MAIN = 16, 8, 64, 128, 256
NP = ROWS * ROW
CH = 320
CP = CH + ROW
KP = 4 * MAIN
REST = 3 * MAIN
SPARE = 3 * CH
OFF = 8
GSIZE = CH // GN_GROUPS
PK = ROW + NS
MESH = pl.DeviceIdType.MESH
DUO, TRI, QUAD = range(2), range(3), range(4)
SLOTS = len(QUAD)
NIL = 0.0


def groups(n, step):
    cuts = [0, *range(n, NS, step), NS]
    return [(a, b - a) for a, b in zip(cuts, cuts[1:])]


SUMS, EDGES = groups(2, SLOTS), groups(3, SLOTS)
SHARE = (1, 2, 3, 3)
ACC32 = dict(preferred_element_type=F32)
ROWS_DOT, COLS_DOT = ((((k,), (k,)), ((), ())) for k in DUO)


def nil(i):
    return jnp.minimum(i, 0) * OFF


def span(i, n=ROW, base=0):
    return slice(base + i * n, base + (i + 1) * n)


def low_half():
    return lax.broadcasted_iota(jnp.int32, (ROW, LANE), 1) < ROW


def widen(p):
    return jnp.concatenate([p, p[..., MAIN:]], -1)


def keep_if(flag, x):
    return jnp.where(jnp.full(x.shape, flag, jnp.int32) > 0, x, NIL)


def store_rest(L, o, r0, r1, r2):
    low = low_half()
    L[span(o), REST:REST + LANE] = jnp.where(low, r0, r1).astype(BF)
    L[span(o), REST + LANE:] = jnp.where(low, r2, 1.0).astype(BF)


def prep_gen(x_of_row, nrows, a, b, L):
    ha, hb = a * 0.5, b * 0.5
    rest = []
    for r in range(nrows + 2):
        x, flag = x_of_row(r)
        h = x.astype(F32) * ha + hb
        n = h + h * jnp.tanh(h)
        if flag is not None:
            n = keep_if(flag, n)
        main = n[:, :MAIN].astype(BF)
        rest.append(n[:, MAIN:])
        for dy in TRI:
            if 0 <= r - dy < nrows:
                L[span(r - dy), span(dy, MAIN)] = main
        if r >= 2:
            store_rest(L, r - 2, *rest[r - 2:])
        yield main


def shifted(v, step):
    v = pltpu.roll(v.reshape(OFF, OFF, LANE), step % OFF, 1)
    sub = lax.broadcasted_iota(jnp.int32, v.shape, 1)
    gap = jnp.zeros_like(v[:1])
    if step > 0:
        v = jnp.where(sub == 0, jnp.concatenate([gap, v[:-1]], 0), v)
    else:
        v = jnp.where(sub == OFF - 1, jnp.concatenate([v[1:], gap], 0), v)
    return v.reshape(ROW, LANE)


def conv_row(Y, o, zero):
    def here(k):
        return Y[k, span(o, base=OFF), :]

    out = [shifted(here(k), 1) + here(k + 2) + shifted(here(k + 4), -1) for k in DUO]
    a = here(6)
    mix = jnp.where(low_half(), shifted(a, 1), a)
    return out + [mix + pltpu.roll(mix, ROW, 1) + shifted(here(7), -1)]


def dot_chunk(L, W, Y, rows, n):
    r = jnp.dot(L[rows, :], W[:, span(n, MAIN)], **ACC32)
    for k in DUO:
        Y[2 * n + k, OFF + rows.start:OFF + rows.stop, :] = r[:, span(k, LANE)]


def weave(L, W, Y, m, prep, epi, share):
    work = [prep] * (m // ROW + 2) + [epi] * (m // ROW)
    done = 0
    for n in QUAD:
        dot_chunk(L, W, Y, slice(0, m), n)
        upto = len(work) * share[n] // share[-1]
        for g in work[done:upto]:
            mark = next(g)
        done = upto
        if n < len(QUAD) - 1:
            L[:NS, KP - NS:] = jnp.where(mark[:NS, LANE - NS:LANE].astype(F32) > NIL, 1.0, NIL).astype(BF)
    for g in (prep, epi):
        for _ in g:
            pass


def lane_left(x, k):
    return pltpu.roll(x, CP - k, 1)


def starts(k):
    lane = lax.broadcasted_iota(jnp.int32, (OFF, LANE), 1) + k * LANE
    return (lane % GSIZE == 0) & (lane < CH)


def stacked(rows):
    fill = [jnp.zeros((4 - len(rows), rows[0].shape[1]), F32)] * (len(rows) < 4)
    return jnp.concatenate(list(rows) + fill, 0)


def compact(tiles, embs):
    s = stacked([jnp.concatenate([t[k:k + 1] for k in TRI], 1) for t in tiles])
    q = stacked([jnp.concatenate([t[k + 3:k + 4] for k in TRI], 1) for t in tiles])
    e = stacked(embs)
    x = jnp.concatenate([s + float(NP) * e, q + e * (2.0 * s + float(NP) * e)], 0)
    w2 = x + lane_left(x, 1)
    w4 = w2 + lane_left(w2, 2)
    w8 = w4 + lane_left(w4, 4)
    w10 = w8 + lane_left(w2, 8)
    c = sum(jnp.where(starts(k), w10[:, span(k, LANE)], NIL) for k in TRI)
    return [jnp.concatenate([c[k:k + 1], c[k + 4:k + 5]], 0) for k in range(len(tiles))]


def affine(tots, gains, shifts, embs, count):
    x = jnp.concatenate([stacked([t[k:k + 1] for t in tots]) for k in DUO], 0)
    y = jnp.concatenate([jnp.where(starts(k), x, NIL) for k in TRI], 1)
    r2 = y + pltpu.roll(y, 1, 1)
    r4 = r2 + pltpu.roll(r2, 2, 1)
    r8 = r4 + pltpu.roll(r4, 4, 1)
    r = r8 + pltpu.roll(r2, 8, 1)
    lane = lax.broadcasted_iota(jnp.int32, (OFF, CP), 1)
    r = jnp.where(lane >= CH, pltpu.roll(r, ROW, 1), r) * (1.0 / count)
    mean, msq = r[:4], r[4:]
    a = stacked(gains) * lax.rsqrt(msq - mean * mean + GN_EPS)
    return a, stacked(shifts) + a * (stacked(embs) - mean)


def pack_row(dst, x):
    dst[:ROW, :] = jnp.concatenate(x[:2], 1)
    half = ROW // 2
    p = jnp.where(low_half()[:half], x[2][:half].astype(F32), x[2][half:].astype(F32))
    dst[ROW:, :] = jnp.concatenate([p[:NS], p[NS:]], 1).astype(BF)


def unpack_row(src):
    p = src[ROW:, :].astype(F32)
    p = jnp.concatenate([p[:, :LANE], p[:, LANE:]], 0)
    swap, low = pltpu.roll(p, ROW, 1), low_half()[:ROW // 2]
    rest = jnp.concatenate([jnp.where(low, p, swap), jnp.where(low, swap, p)], 0)
    return jnp.concatenate([src[:ROW, :].astype(F32), rest], 1)


def stats_tile(acc, acq):
    parts = [x.sum(0, keepdims=True) for x in acc + acq]
    return jnp.concatenate(parts + [jnp.zeros((2, LANE), F32)], 0)


def add_stats(acc, acq, new):
    for k, x in enumerate(new):
        v = x.astype(F32).reshape(OFF, OFF, LANE)
        acc[k] = acc[k] + v.sum(0)
        acq[k] = acq[k] + (v * v).sum(0)


def no_stats():
    return [jnp.zeros((OFF, LANE), F32) for _ in TRI]


def weight_copies(src, W, WR, sem_main, sem_rest):
    for dy in TRI:
        for dx in TRI:
            cols = span(dx, MAIN)
            pltpu.make_async_copy(src.at[dy, dx, :MAIN, :MAIN], W.at[span(dy, MAIN), cols], sem_main).start()
            pltpu.make_async_copy(src.at[dy, dx, MAIN:, :MAIN], W.at[span(dy, base=REST), cols], sem_main).start()
            pltpu.make_async_copy(src.at[dy, dx, :, MAIN:], WR.at[dy * 3 + dx], sem_rest).start()


def weight_finish(bias, W, WR, sem_main, sem_rest):
    main = W.at[:SPARE, :REST]
    pltpu.make_async_copy(main, main, sem_main).wait()
    pltpu.make_async_copy(WR, WR, sem_rest).wait()
    for dy in TRI:
        for part, rows in ((slice(0, MAIN), span(dy, MAIN)), (slice(MAIN, CH), span(dy, base=REST))):
            w0, w1, w2 = (WR[dy * 3 + dx, part, :] for dx in TRI)
            W[rows, REST:REST + LANE] = jnp.concatenate([w0, w1], 1)
            W[rows, REST + LANE:] = jnp.concatenate([w2, w2], 1)
    b = widen(bias.astype(F32))
    gap = jnp.zeros((1, MAIN), F32)
    rest = jnp.where(low_half()[:1], 0.0, b[:, MAIN:])
    row = jnp.concatenate([gap, b[:, :MAIN], gap, rest, gap[:, :LANE]], 1)
    first = lax.broadcasted_iota(jnp.int32, (ROW, KP), 0) == 0
    W[SPARE:, :] = jnp.where(first, row, NIL).astype(BF)


def mega(sp, q, wi, bi, temb, tb, g1, s1, g2, s2, b1, b2, tw, w1, w2, hand, halo,
         H, U, H2, HS, W, WR, TW, WI, L0, L1, Y0, Y1, ST, STC, SG, RS, AB, EMB, GAIN, HT, HB, PT, PB, LQ,
         wm_sem, wr_sem, tw_sem, q_send, q_recv, st_send, st_recv, up_send, dn_send, ht_recv, hb_recv, out_sem, fin_sem):
    me, dp = lax.axis_index("sp"), lax.axis_index("dp")
    has_up, has_dn = (me > 0).astype(jnp.int32), (me < sp - 1).astype(jnp.int32)
    held = (H, U, H2, U)
    end = SLOTS
    last = NS - 1

    get_tw = pltpu.make_async_copy(tw, TW, tw_sem)
    get_tw.start()
    for j, src in enumerate((w1.at[0], w2.at[0], w1.at[1], w2.at[1])):
        weight_copies(src, W.at[j], WR.at[j], wm_sem.at[j], wr_sem.at[j])

    barrier = pltpu.get_barrier_semaphore()
    for k in range(1, sp):
        pl.semaphore_signal(barrier, inc=1, device_id=(dp, lax.rem(me + k, sp)), device_id_type=MESH)
    pl.semaphore_wait(barrier, sp - 1)

    def remote(src, dst, ssem, rsem, dev):
        return pltpu.make_async_remote_copy(src_ref=src, dst_ref=dst, send_sem=ssem, recv_sem=rsem, device_id=(dp, dev), device_id_type=MESH)

    def if_up(f):
        pl.when(me > 0)(f)

    def if_dn(f):
        pl.when(me < sp - 1)(f)

    q_dn = remote(q.at[:, :, NP - LANE:], LQ.at[0], q_send.at[0], q_recv.at[0], me + 1)
    q_up = remote(q.at[:, :, :LANE], LQ.at[1], q_send.at[1], q_recv.at[1], me - 1)
    if_dn(q_dn.start)
    if_up(q_up.start)

    def rows_copies(slot, g, lo, n):
        ss = pl.ds(lo, n)
        down = remote(PB.at[slot - 1, ss], HT.at[slot, ss], dn_send.at[slot, g], ht_recv.at[slot, g], me + 1)
        if slot == end:
            return None, down
        return remote(PT.at[slot - 1, ss], HB.at[slot, ss], up_send.at[slot, g], hb_recv.at[slot, g], me - 1), down

    def out_copy(slot, g, lo, n):
        ss = pl.ds(lo, n)
        return pltpu.make_async_copy(HS.at[ss], hand.at[slot // 2, ss], out_sem.at[slot, g])

    def send_sums(slot, g, lo, n):
        ss = pl.ds(lo, n)
        for k in range(1, sp):
            remote(SG.at[slot, ss], RS.at[slot, k - 1, ss], st_send.at[slot, g], st_recv.at[slot, g], lax.rem(me + k, sp)).start()

    def send_rows(slot, g, lo, n):
        if slot % 2 == 0:
            out_copy(slot, g, lo, n).start()
        if slot > 0:
            up, down = rows_copies(slot, g, lo, n)
            if up is not None:
                if_up(up.start)
            if_dn(down.start)

    def sums_bytes(slot, n, sem, g):
        both = RS.at[slot, :, :n]
        return pltpu.make_async_copy(both, both, sem.at[slot, g])

    def wait_sums(slot, g, n):
        sums_bytes(slot, n, st_recv, g).wait()

    def wait_rows(slot, g, n):
        ss = pl.ds(0, n)
        if_up(lambda: remote(PB.at[0, ss], HT.at[slot, ss], dn_send.at[slot, g], ht_recv.at[slot, g], me).wait_recv())
        if slot is not end:
            if_dn(lambda: remote(PT.at[0, ss], HB.at[slot, ss], up_send.at[slot, g], hb_recv.at[slot, g], me).wait_recv())

    def squeeze(slot, ss, tiles):
        for r, s in zip(compact(tiles, [EMB[slot, pl.ds(s, 1)] for s in ss]), ss):
            SG[slot, s] = r

    for k, (ref, l) in enumerate((ref, l) for pair in ((g1, g2), (s1, s2)) for l in DUO for ref in pair):
        GAIN[k:k + 1, :] = widen(ref[l:l + 1, :].astype(F32))
    WI[...] = jnp.zeros_like(WI)
    for dy in TRI:
        for dx in TRI:
            WI[span(4 * dy + dx, 4), :] = widen(wi[dy, dx].astype(F32))
    WI[NS + 12:NS + 13, :] = widen(bi[...].reshape(1, CH).astype(F32))
    get_tw.wait()
    x = temb[...].astype(F32)
    act = (x * jax.nn.sigmoid(x)).astype(BF)
    for l in DUO:
        pr = lax.dot_general(act, TW[l], COLS_DOT, **ACC32)
        EMB[2 * l] = jnp.zeros((NS, CP), F32)
        EMB[2 * l + 1] = widen(pr + tb[l:l + 1, :].astype(F32))

    if_up(q_dn.wait_recv)
    if_dn(q_up.wait_recv)

    def first(s):
        above, below = keep_if(has_up, LQ[0, s].astype(F32)), keep_if(has_dn, LQ[1, s].astype(F32))
        ext = jnp.concatenate([above, q[s].astype(F32), below], 1)
        mid = pltpu.roll(ext, ext.shape[1] - ROW, 1)
        wide = NP + LANE
        lhs = jnp.concatenate([ext[:, :wide], mid[:, :wide], ext[:, LANE:]], 0).astype(BF)
        r = lax.dot_general(lhs, WI[...].astype(BF), ROWS_DOT, **ACC32)
        acc, acq = no_stats(), no_stats()
        for o in range(ROWS + 2):
            x = r[span(o), :].astype(BF)
            parts = [x[:, span(k, LANE)] for k in TRI]
            if o == 0:
                pack_row(HT.at[0, s], parts)
            elif o > ROWS:
                pack_row(HB.at[0, s], parts)
            else:
                H[s, span(o - 1), :] = x
                HS[s, span(o - 1), :] = x[:, :CH]
                add_stats(acc, acq, parts)
        ST[s] = stats_tile(acc, acq)

    def first_pair(i, carry):
        t = 2 * i
        for g in TRI:
            for parts, send in ((EDGES, send_rows), (SUMS, send_sums)):
                pl.when(i == 2 * g + 2)(functools.partial(send, 0, g, *parts[g]))
        ss = [lax.rem(n + NS, NS) for n in (t - 2, t - 1)]
        tiles = [ST[s] for s in ss]
        first(t)
        first(t + 1)
        squeeze(0, ss, tiles)
        return carry

    lax.fori_loop(0, NS // 2, first_pair, 0)
    squeeze(0, (last - 1, last), (ST[last - 1], ST[last]))
    for j in QUAD:
        weight_finish((b1, b2)[j % 2][j // 2:j // 2 + 1, :], W.at[j], WR.at[j], wm_sem.at[j], wr_sem.at[j])
    for g in (3, 4):
        send_sums(0, g, *SUMS[g])
        send_rows(0, g, *EDGES[g])

    def scales(slots, ss):
        tots = []
        for slot, s in zip(slots, ss):
            tots.append(SG[slot, s])
            for k in range(sp - 1):
                tots[-1] = tots[-1] + RS[slot, k, s]
        return affine(tots, [GAIN[pl.ds(k, 1)] for k in slots], [GAIN[pl.ds(k + SLOTS, 1)] for k in slots],
                      [EMB[k, pl.ds(s, 1)] for k, s in zip(slots, ss)], float(sp * NP * GSIZE))

    def prep_of(slot, s, L, a, b):
        def row(r):
            if r == 0:
                return unpack_row(HT.at[slot, s]), has_up
            if r == ROWS + 1:
                return unpack_row(HB.at[slot, s]), has_dn
            return held[slot][s, span(r - 1), :], None
        return prep_gen(row, ROWS, a, b, L)

    def epi_gen(j, s, Y, zero, tiles):
        acc, acq = no_stats(), no_stats()
        edge = {ROWS - 1: PB.at[j, s]}
        if j + 1 < end:
            edge[0] = PT.at[j, s]
        for o in range(ROWS):
            new = [x.astype(BF) for x in conv_row(Y, o, zero)]
            mark = new[2]
            for k in TRI:
                cols = span(k, LANE)
                if j % 2:
                    new[k] = (new[k].astype(F32) + held[j - 1][s, span(o), cols].astype(F32)).astype(BF)
                    cols_out = slice(k * LANE, min(k * LANE + LANE, CH))
                    HS[s, span(o), cols_out] = new[k][:, :cols_out.stop - cols_out.start]
                if j + 1 < end:
                    held[j + 1][s, span(o), cols] = new[k]
            if o in edge:
                pack_row(edge[o], new)
            if j + 1 < end:
                add_stats(acc, acq, new)
            if o == ROWS - 1:
                tiles.append(stats_tile(acc, acq))
            yield mark

    for Y in (Y0, Y1):
        Y[...] = jnp.zeros_like(Y)
    for g in DUO:
        wait_sums(0, g, SUMS[g][1])
    for c, v in enumerate(scales((0,) * 3, TRI)):
        AB[c] = v[:3]
    still = nil(me)
    for _ in prep_of(0, 0, L0, AB[0, :1], AB[1, :1]):
        pass
    for j in QUAD:
        if j % 2:
            for g in range(len(EDGES)):
                out_copy(j - 1, g, *EDGES[g]).wait()

        def body(i, carry, j=j):
            t = 2 * i
            zero = nil(i)
            turn = NS // 2 - 1
            ns = [jnp.minimum(j * NS + t + 3 + k, end * NS - 1) for k in DUO]
            for g in TRI:
                pl.when(i == 2 * g + 1)(functools.partial(wait_sums, j, g + 2, SUMS[g + 2][1]))
            for g in DUO:
                if j + 1 < end:
                    pl.when(i == turn - 1 + g)(functools.partial(wait_sums, j + 1, g, SUMS[g][1]))
            if j > 0:
                for g in TRI:
                    pl.when(i == 2 * g + 1)(functools.partial(wait_rows, j, g + 1, EDGES[g + 1][1]))
                pl.when(i == turn)(functools.partial(wait_rows, j, 4, EDGES[4][1]))
            if j + 1 < end:
                pl.when(i == turn)(functools.partial(wait_rows, j + 1, 0, EDGES[0][1]))
            for parts, send in ((EDGES, send_rows), (SUMS, send_sums))[:end - j]:
                for g in TRI:
                    pl.when(i == 2 * g + 2)(functools.partial(send, j + 1, g, *parts[g]))
            new = scales([n // NS for n in ns], [lax.rem(n, NS) for n in ns])
            co = [(AB[0, k:k + 1], AB[1, k:k + 1]) for k in (1, 2)]
            tiles = [STC[...]]
            for u, (Lc, Ln, Yc, Yp) in enumerate(((L0, L1, Y0, Y1), (L1, L0, Y1, Y0))):
                nxt = jnp.minimum(t + u + 1, last)
                weave(Lc, W.at[j], Yc, NP, prep_of(j, nxt, Ln, *co[u]), epi_gen(j, lax.rem(t + u + last, NS), Yp, zero, tiles), SHARE)
            for c in DUO:
                AB[c] = jnp.concatenate([co[1][c], new[c][:2]], 0)
            if j + 1 == end:
                return carry
            STC[...] = tiles.pop()
            squeeze(j + 1, [lax.rem(t + last - 1 + k, NS) for k in DUO], tiles)
            return carry

        lax.fori_loop(0, NS // 2, body, 0)
        send_rows(j + 1, 3, *EDGES[3])
        if j + 1 < end:
            send_sums(j + 1, 3, *SUMS[3])
        tiles = [STC[...]]
        for _ in epi_gen(j, last, Y1, still, tiles):
            pass
        if j + 1 < end:
            for _ in prep_of(j + 1, 0, L0, AB[0, :1], AB[1, :1]):
                pass
            squeeze(j + 1, (last - 1, last), tiles)
            send_sums(j + 1, 4, *SUMS[4])
        send_rows(j + 1, 4, *EDGES[4])

    for g in range(len(SUMS)):
        wait_rows(end, g, EDGES[g][1])
        out_copy(end, g, *EDGES[g]).wait()
        for slot in QUAD:
            sums_bytes(slot, SUMS[g][1], st_send, g).wait()
            up, down = rows_copies(slot + 1, g, *EDGES[g])
            if up is not None:
                if_up(up.wait_send)
            if_dn(down.wait_send)
    if_dn(q_dn.wait_send)
    if_up(q_up.wait_send)
    fin = pltpu.make_async_copy(HT.at[end], halo, fin_sem)
    fin.start()
    fin.wait()


def tail(hand, halo, bd, dw, h0o, h1o, h2o, do, P0, P1, P2, HA, W, WR, L0, L1, Y0, Y1, OD, DS, in_sem, ha_sem, wm_sem, wr_sem, o_sem, od_sem):
    me = lax.axis_index("sp")
    has_up = (me > 0).astype(jnp.int32)
    held, outs = (P0, P1, P2), (h0o, h1o, h2o)
    ahead = len(QUAD)

    def take(k, s):
        return pltpu.make_async_copy(hand.at[k, s], held[k].at[s], in_sem.at[k, s])

    def put(k, s):
        return pltpu.make_async_copy(held[k].at[s], outs[k].at[s], o_sem.at[k, s])

    def fetch(s):
        for k in (2, 0, 1):
            take(k, s).start()

    get_halo = pltpu.make_async_copy(halo, HA, ha_sem)
    take(2, 0).start()
    get_halo.start()
    weight_copies(dw, W, WR, wm_sem, wr_sem)
    for k in DUO:
        take(k, 0).start()
    for s in range(1, ahead):
        fetch(s)
    for Y in (Y0, Y1):
        Y[...] = jnp.zeros_like(Y)
    get_halo.wait()
    take(2, 0).wait()
    still = nil(me)

    def row_of(s, r):
        if r == 0:
            return keep_if(has_up, unpack_row(HA.at[s]))
        return widen(P2[s, span(r - 1), :].astype(F32))

    def dprep(s, L):
        for o in QUAD:
            xs = [row_of(s, 2 * o + dy) for dy in TRI]
            for dy in TRI:
                L[span(o), span(dy, MAIN)] = xs[dy][:, :MAIN].astype(BF)
            store_rest(L, o, *(x[:, MAIN:] for x in xs))

    def depi(s, Y, zero):
        for o in QUAD:
            d = conv_row(Y, o, zero)
            for k in TRI:
                DS[o, k] = d[k]
            parts = [DS[o, k, pl.ds(0, ROW // 2, stride=2), :] for k in TRI]
            OD[s, span(o, ROW // 2), :] = jnp.concatenate(parts, 1)[:, :CH].astype(BF)

    def dhalf(t, Lc, Ln, Yc, Yp, zero):
        for n in QUAD:
            dot_chunk(Lc, W, Yc, slice(0, NP // 2), n)
        dprep(jnp.minimum(t + 1, NS - 1), Ln)
        depi(lax.rem(t + NS - 1, NS), Yp, zero)

    dprep(0, L0)
    weight_finish(bd[...].reshape(1, CH), W, WR, wm_sem, wr_sem)

    def dbody(i, carry):
        t = 2 * i
        zero = nil(i)
        for s in (t, t + 1):
            pl.when(s + ahead < NS)(functools.partial(fetch, s + ahead))
            pl.when(s + 1 < NS)(lambda s=s: take(2, s + 1).wait())
            put(2, s).start()
            for k in DUO:
                take(k, s).wait()
                put(k, s).start()
        dhalf(t, L0, L1, Y0, Y1, zero)
        dhalf(t + 1, L1, L0, Y1, Y0, zero)
        return carry

    lax.fori_loop(0, NS // 2, dbody, 0)
    depi(NS - 1, Y1, still)
    dout = pltpu.make_async_copy(OD, do, od_sem)
    dout.start()

    def drain(s, carry):
        for k in TRI:
            put(k, s).wait()
        return carry

    lax.fori_loop(0, NS, drain, 0)
    dout.wait()


def solution(mesh):
    sp = mesh.shape["sp"]

    def program(latent, time_emb, w_in, b_in, gn1_scale, gn1_shift, conv1_w, conv1_b, temb_w, temb_b, gn2_scale, gn2_shift, conv2_w, conv2_b, down_w, down_b):
        none = (0, 0)
        lat = jnp.pad(latent.transpose(0, 3, 1, 2), (none, none, none, (1, 1)))
        q = jnp.stack([lat[..., d:d + ROW] for d in TRI], 1).reshape(NS, 12, NP)
        q = jnp.pad(q, (none, (0, 4), none), constant_values=1)

        dma, vm = pltpu.SemaphoreType.DMA, pltpu.VMEM
        any_, vms = pl.BlockSpec(memory_space=pl.ANY), pl.BlockSpec(memory_space=pltpu.VMEM)
        params = functools.partial(pltpu.CompilerParams, vmem_limit_bytes=66_000_000)

        def big(n=NP, c=CP):
            return vm((NS, n, c), BF)

        def edge(n):
            return vm((n, NS, PK, MAIN), BF)

        def bufs(m):
            return [vm((m, KP), BF)] * 2 + [vm((8, m + 2 * OFF, LANE), F32)] * 2

        def out(*shape):
            return jax.ShapeDtypeStruct(shape, BF)

        hand, halo = pl.pallas_call(
            functools.partial(mega, sp),
            out_shape=(out(3, NS, NP, CH), out(NS, PK, MAIN)),
            in_specs=[vms] * 11 + [any_] * 3, out_specs=(any_, any_),
            scratch_shapes=[big(), big(), big(), big(NP, CH), vm((SLOTS, KP, KP), BF), vm((SLOTS, 9, CH, ROW), BF), vm((2, CH, temb_w.shape[1]), BF), vm((3 * NS, CP), F32)] + bufs(NP)
            + [vm((NS, OFF, LANE), F32), vm((OFF, LANE), F32), vm((SLOTS, NS, 2, LANE), F32), vm((SLOTS, sp - 1, NS, 2, LANE), F32), vm((2, 3, CP), F32), vm((SLOTS, NS, CP), F32), vm((OFF, CP), F32),
               edge(SLOTS + 1), edge(SLOTS), edge(SLOTS - 1), edge(SLOTS), vm((2, NS, NS, LANE), BF),
               dma((SLOTS,)), dma((SLOTS,)), dma] + [dma((2,))] * 2 + [dma((SLOTS + 1, len(SUMS)))] * 7 + [dma],
            compiler_params=params(collective_id=0, has_side_effects=True), name="mega",
        )(q, w_in, b_in, time_emb, temb_b, gn1_scale, gn1_shift, gn2_scale, gn2_shift, conv1_b, conv2_b, temb_w.transpose(0, 2, 1), conv1_w, conv2_w)
        outs = pl.pallas_call(
            tail,
            out_shape=(out(NS, NP, CH),) * 3 + (out(NS, NP // 4, CH),),
            in_specs=[any_] * 2 + [vms, any_], out_specs=(any_,) * 4,
            scratch_shapes=[big(NP, CH)] * 3 + [big(PK, MAIN), vm((KP, KP), BF), vm((9, CH, ROW), BF)] + bufs(NP // 2)
            + [big(NP // 4, CH), vm((4, 3, ROW, LANE), F32), dma((3, NS)), dma, dma, dma, dma((3, NS)), dma],
            compiler_params=params(), name="tail",
        )(hand, halo, down_b, down_w)
        return tuple(o.reshape(NS, n, m, CH) for o, n, m in zip(outs, [ROWS] * len(TRI) + [ROWS // 2], [ROW] * len(TRI) + [ROW // 2]))

    band = P("dp", "sp", None, None)
    return jax.shard_map(program, mesh=mesh, in_specs=(band, P("dp", None)) + (P(),) * 14, out_specs=(band,) * 4, check_vma=False)
```

```python
import functools

import jax
import jax.numpy as jnp
from jax import lax
from jax.experimental import pallas as pl
from jax.experimental.pallas import tpu as pltpu
from jax.sharding import PartitionSpec as P

F32, BF = jnp.float32, jnp.bfloat16
GN_GROUPS, GN_EPS = 32, 1e-5
NS, ROWS, ROW, LANE, MAIN = 16, 8, 64, 128, 256
NP = ROWS * ROW
CH = 320
CP = CH + ROW
KP = 4 * MAIN
REST = 3 * MAIN
SPARE = 3 * CH
OFF = 8
GSIZE = CH // GN_GROUPS
PK = ROW + NS
MESH = pl.DeviceIdType.MESH
DUO, TRI, QUAD = range(2), range(3), range(4)
SLOTS = len(QUAD)
NIL = 0.0


def groups(n, step):
    cuts = [0, *range(n, NS, step), NS]
    return [(a, b - a) for a, b in zip(cuts, cuts[1:])]


SUMS, EDGES = groups(2, SLOTS), groups(3, SLOTS)
SHARE = (1, 2, 3, 3)
ACC32 = dict(preferred_element_type=F32)
ROWS_DOT, COLS_DOT = ((((k,), (k,)), ((), ())) for k in DUO)


def nil(i):
    return jnp.minimum(i, 0) * OFF


def span(i, n=ROW, base=0):
    return slice(base + i * n, base + (i + 1) * n)


def low_half():
    return lax.broadcasted_iota(jnp.int32, (ROW, LANE), 1) < ROW


def widen(p):
    return jnp.concatenate([p, p[..., MAIN:]], -1)


def keep_if(flag, x):
    return jnp.where(jnp.full(x.shape, flag, jnp.int32) > 0, x, NIL)


def store_rest(L, o, r0, r1, r2):
    low = low_half()
    L[span(o), REST:REST + LANE] = jnp.where(low, r0, r1).astype(BF)
    L[span(o), REST + LANE:] = jnp.where(low, r2, 1.0).astype(BF)


def prep_gen(x_of_row, nrows, a, b, L):
    ha, hb = a * 0.5, b * 0.5
    rest = []
    for r in range(nrows + 2):
        x, flag = x_of_row(r)
        h = x.astype(F32) * ha + hb
        n = h + h * jnp.tanh(h)
        if flag is not None:
            n = keep_if(flag, n)
        main = n[:, :MAIN].astype(BF)
        rest.append(n[:, MAIN:])
        for dy in TRI:
            if 0 <= r - dy < nrows:
                L[span(r - dy), span(dy, MAIN)] = main
        if r >= 2:
            store_rest(L, r - 2, *rest[r - 2:])
        yield main


def shifted(v, step):
    v = pltpu.roll(v.reshape(OFF, OFF, LANE), step % OFF, 1)
    sub = lax.broadcasted_iota(jnp.int32, v.shape, 1)
    gap = jnp.zeros_like(v[:1])
    if step > 0:
        v = jnp.where(sub == 0, jnp.concatenate([gap, v[:-1]], 0), v)
    else:
        v = jnp.where(sub == OFF - 1, jnp.concatenate([v[1:], gap], 0), v)
    return v.reshape(ROW, LANE)


def conv_row(Y, o, zero):
    def here(k):
        return Y[k, span(o, base=OFF), :]

    out = [shifted(here(k), 1) + here(k + 2) + shifted(here(k + 4), -1) for k in DUO]
    a = here(6)
    mix = jnp.where(low_half(), shifted(a, 1), a)
    return out + [mix + pltpu.roll(mix, ROW, 1) + shifted(here(7), -1)]


def dot_chunk(L, W, Y, rows, n):
    r = jnp.dot(L[rows, :], W[:, span(n, MAIN)], **ACC32)
    for k in DUO:
        Y[2 * n + k, OFF + rows.start:OFF + rows.stop, :] = r[:, span(k, LANE)]


def weave(L, W, Y, m, prep, epi, share):
    work = [prep] * (m // ROW + 2) + [epi] * (m // ROW)
    done = 0
    for n in QUAD:
        dot_chunk(L, W, Y, slice(0, m), n)
        upto = len(work) * share[n] // share[-1]
        for g in work[done:upto]:
            mark = next(g)
        done = upto
        if n < len(QUAD) - 1:
            L[:NS, KP - NS:] = jnp.where(mark[:NS, LANE - NS:LANE].astype(F32) > NIL, 1.0, NIL).astype(BF)
    for g in (prep, epi):
        for _ in g:
            pass


def lane_left(x, k):
    return pltpu.roll(x, CP - k, 1)


def starts(k):
    lane = lax.broadcasted_iota(jnp.int32, (OFF, LANE), 1) + k * LANE
    return (lane % GSIZE == 0) & (lane < CH)


def stacked(rows):
    fill = [jnp.zeros((4 - len(rows), rows[0].shape[1]), F32)] * (len(rows) < 4)
    return jnp.concatenate(list(rows) + fill, 0)


def compact(tiles, embs):
    s = stacked([jnp.concatenate([t[k:k + 1] for k in TRI], 1) for t in tiles])
    q = stacked([jnp.concatenate([t[k + 3:k + 4] for k in TRI], 1) for t in tiles])
    e = stacked(embs)
    x = jnp.concatenate([s + float(NP) * e, q + e * (2.0 * s + float(NP) * e)], 0)
    w2 = x + lane_left(x, 1)
    w4 = w2 + lane_left(w2, 2)
    w8 = w4 + lane_left(w4, 4)
    w10 = w8 + lane_left(w2, 8)
    c = sum(jnp.where(starts(k), w10[:, span(k, LANE)], NIL) for k in TRI)
    return [jnp.concatenate([c[k:k + 1], c[k + 4:k + 5]], 0) for k in range(len(tiles))]


def affine(tots, gains, shifts, embs, count):
    x = jnp.concatenate([stacked([t[k:k + 1] for t in tots]) for k in DUO], 0)
    y = jnp.concatenate([jnp.where(starts(k), x, NIL) for k in TRI], 1)
    r2 = y + pltpu.roll(y, 1, 1)
    r4 = r2 + pltpu.roll(r2, 2, 1)
    r8 = r4 + pltpu.roll(r4, 4, 1)
    r = r8 + pltpu.roll(r2, 8, 1)
    lane = lax.broadcasted_iota(jnp.int32, (OFF, CP), 1)
    r = jnp.where(lane >= CH, pltpu.roll(r, ROW, 1), r) * (1.0 / count)
    mean, msq = r[:4], r[4:]
    a = stacked(gains) * lax.rsqrt(msq - mean * mean + GN_EPS)
    return a, stacked(shifts) + a * (stacked(embs) - mean)


def pack_row(dst, x):
    dst[:ROW, :] = jnp.concatenate(x[:2], 1)
    half = ROW // 2
    p = jnp.where(low_half()[:half], x[2][:half].astype(F32), x[2][half:].astype(F32))
    dst[ROW:, :] = jnp.concatenate([p[:NS], p[NS:]], 1).astype(BF)


def unpack_row(src):
    p = src[ROW:, :].astype(F32)
    p = jnp.concatenate([p[:, :LANE], p[:, LANE:]], 0)
    swap, low = pltpu.roll(p, ROW, 1), low_half()[:ROW // 2]
    rest = jnp.concatenate([jnp.where(low, p, swap), jnp.where(low, swap, p)], 0)
    return jnp.concatenate([src[:ROW, :].astype(F32), rest], 1)


def stats_tile(acc, acq):
    parts = [x.sum(0, keepdims=True) for x in acc + acq]
    return jnp.concatenate(parts + [jnp.zeros((2, LANE), F32)], 0)


def add_stats(acc, acq, new):
    for k, x in enumerate(new):
        v = x.astype(F32).reshape(OFF, OFF, LANE)
        acc[k] = acc[k] + v.sum(0)
        acq[k] = acq[k] + (v * v).sum(0)


def no_stats():
    return [jnp.zeros((OFF, LANE), F32) for _ in TRI]


def weight_copies(src, W, WR, sem_main, sem_rest):
    for dy in TRI:
        for dx in TRI:
            cols = span(dx, MAIN)
            pltpu.make_async_copy(src.at[dy, dx, :MAIN, :MAIN], W.at[span(dy, MAIN), cols], sem_main).start()
            pltpu.make_async_copy(src.at[dy, dx, MAIN:, :MAIN], W.at[span(dy, base=REST), cols], sem_main).start()
            pltpu.make_async_copy(src.at[dy, dx, :, MAIN:], WR.at[dy * 3 + dx], sem_rest).start()


def weight_finish(bias, W, WR, sem_main, sem_rest):
    main = W.at[:SPARE, :REST]
    pltpu.make_async_copy(main, main, sem_main).wait()
    pltpu.make_async_copy(WR, WR, sem_rest).wait()
    for dy in TRI:
        for part, rows in ((slice(0, MAIN), span(dy, MAIN)), (slice(MAIN, CH), span(dy, base=REST))):
            w0, w1, w2 = (WR[dy * 3 + dx, part, :] for dx in TRI)
            W[rows, REST:REST + LANE] = jnp.concatenate([w0, w1], 1)
            W[rows, REST + LANE:] = jnp.concatenate([w2, w2], 1)
    b = widen(bias.astype(F32))
    gap = jnp.zeros((1, MAIN), F32)
    rest = jnp.where(low_half()[:1], 0.0, b[:, MAIN:])
    row = jnp.concatenate([gap, b[:, :MAIN], gap, rest, gap[:, :LANE]], 1)
    first = lax.broadcasted_iota(jnp.int32, (ROW, KP), 0) == 0
    W[SPARE:, :] = jnp.where(first, row, NIL).astype(BF)


def mega(sp, q, wi, bi, temb, tb, g1, s1, g2, s2, b1, b2, tw, w1, w2, hand, halo,
         H, U, H2, HS, W, WR, TW, WI, L0, L1, Y0, Y1, ST, STC, SG, RS, AB, EMB, GAIN, HT, HB, PT, PB, LQ,
         wm_sem, wr_sem, tw_sem, q_send, q_recv, st_send, st_recv, up_send, dn_send, ht_recv, hb_recv, out_sem, fin_sem):
    me, dp = lax.axis_index("sp"), lax.axis_index("dp")
    has_up, has_dn = (me > 0).astype(jnp.int32), (me < sp - 1).astype(jnp.int32)
    held = (H, U, H2, U)
    end = SLOTS
    last = NS - 1

    get_tw = pltpu.make_async_copy(tw, TW, tw_sem)
    get_tw.start()
    for j, src in enumerate((w1.at[0], w2.at[0], w1.at[1], w2.at[1])):
        weight_copies(src, W.at[j], WR.at[j], wm_sem.at[j], wr_sem.at[j])

    barrier = pltpu.get_barrier_semaphore()
    for k in range(1, sp):
        pl.semaphore_signal(barrier, inc=1, device_id=(dp, lax.rem(me + k, sp)), device_id_type=MESH)
    for k, (ref, l) in enumerate((ref, l) for pair in ((g1, g2), (s1, s2)) for l in DUO for ref in pair):
        GAIN[k:k + 1, :] = widen(ref[l:l + 1, :].astype(F32))
    WI[...] = jnp.zeros_like(WI)
    for dy in TRI:
        for dx in TRI:
            WI[span(4 * dy + dx, 4), :] = widen(wi[dy, dx].astype(F32))
    WI[NS + 12:NS + 13, :] = widen(bi[...].reshape(1, CH).astype(F32))
    get_tw.wait()
    x = temb[...].astype(F32)
    act = (x * jax.nn.sigmoid(x)).astype(BF)
    for l in DUO:
        pr = lax.dot_general(act, TW[l], COLS_DOT, **ACC32)
        EMB[2 * l] = jnp.zeros((NS, CP), F32)
        EMB[2 * l + 1] = widen(pr + tb[l:l + 1, :].astype(F32))
    for Y in (Y0, Y1):
        Y[...] = jnp.zeros_like(Y)
    pl.semaphore_wait(barrier, sp - 1)

    def remote(src, dst, ssem, rsem, dev):
        return pltpu.make_async_remote_copy(src_ref=src, dst_ref=dst, send_sem=ssem, recv_sem=rsem, device_id=(dp, dev), device_id_type=MESH)

    def if_up(f):
        pl.when(me > 0)(f)

    def if_dn(f):
        pl.when(me < sp - 1)(f)

    q_dn = remote(q.at[:, :, NP - LANE:], LQ.at[0], q_send.at[0], q_recv.at[0], me + 1)
    q_up = remote(q.at[:, :, :LANE], LQ.at[1], q_send.at[1], q_recv.at[1], me - 1)
    if_dn(q_dn.start)
    if_up(q_up.start)

    def rows_copies(slot, g, lo, n):
        ss = pl.ds(lo, n)
        down = remote(PB.at[slot - 1, ss], HT.at[slot, ss], dn_send.at[slot, g], ht_recv.at[slot, g], me + 1)
        if slot == end:
            return None, down
        return remote(PT.at[slot - 1, ss], HB.at[slot, ss], up_send.at[slot, g], hb_recv.at[slot, g], me - 1), down

    def out_copy(slot, g, lo, n):
        ss = pl.ds(lo, n)
        return pltpu.make_async_copy(HS.at[ss], hand.at[slot // 2, ss], out_sem.at[slot, g])

    def send_sums(slot, g, lo, n):
        ss = pl.ds(lo, n)
        for k in range(1, sp):
            remote(SG.at[slot, ss], RS.at[slot, k - 1, ss], st_send.at[slot, g], st_recv.at[slot, g], lax.rem(me + k, sp)).start()

    def send_rows(slot, g, lo, n):
        if slot % 2 == 0:
            out_copy(slot, g, lo, n).start()
        if slot > 0:
            up, down = rows_copies(slot, g, lo, n)
            if up is not None:
                if_up(up.start)
            if_dn(down.start)

    def sums_bytes(slot, n, sem, g):
        both = RS.at[slot, :, :n]
        return pltpu.make_async_copy(both, both, sem.at[slot, g])

    def wait_sums(slot, g, n):
        sums_bytes(slot, n, st_recv, g).wait()

    def wait_rows(slot, g, n):
        ss = pl.ds(0, n)
        if_up(lambda: remote(PB.at[0, ss], HT.at[slot, ss], dn_send.at[slot, g], ht_recv.at[slot, g], me).wait_recv())
        if slot is not end:
            if_dn(lambda: remote(PT.at[0, ss], HB.at[slot, ss], up_send.at[slot, g], hb_recv.at[slot, g], me).wait_recv())

    def squeeze(slot, ss, tiles):
        for r, s in zip(compact(tiles, [EMB[slot, pl.ds(s, 1)] for s in ss]), ss):
            SG[slot, s] = r

    for j in QUAD:
        weight_finish((b1, b2)[j % 2][j // 2:j // 2 + 1, :], W.at[j], WR.at[j], wm_sem.at[j], wr_sem.at[j])

    if_up(q_dn.wait_recv)
    if_dn(q_up.wait_recv)

    def first(s):
        above, below = keep_if(has_up, LQ[0, s].astype(F32)), keep_if(has_dn, LQ[1, s].astype(F32))
        ext = jnp.concatenate([above, q[s].astype(F32), below], 1)
        mid = pltpu.roll(ext, ext.shape[1] - ROW, 1)
        wide = NP + LANE
        lhs = jnp.concatenate([ext[:, :wide], mid[:, :wide], ext[:, LANE:]], 0).astype(BF)
        r = lax.dot_general(lhs, WI[...].astype(BF), ROWS_DOT, **ACC32)
        acc, acq = no_stats(), no_stats()
        for o in range(ROWS + 2):
            x = r[span(o), :].astype(BF)
            parts = [x[:, span(k, LANE)] for k in TRI]
            if o == 0:
                pack_row(HT.at[0, s], parts)
            elif o > ROWS:
                pack_row(HB.at[0, s], parts)
            else:
                H[s, span(o - 1), :] = x
                HS[s, span(o - 1), :] = x[:, :CH]
                add_stats(acc, acq, parts)
        ST[s] = stats_tile(acc, acq)

    def first_pair(i, carry):
        t = 2 * i
        for g in TRI:
            for parts, send in ((EDGES, send_rows), (SUMS, send_sums)):
                pl.when(i == 2 * g + 2)(functools.partial(send, 0, g, *parts[g]))
        ss = [lax.rem(n + NS, NS) for n in (t - 2, t - 1)]
        tiles = [ST[s] for s in ss]
        first(t)
        first(t + 1)
        squeeze(0, ss, tiles)
        return carry

    lax.fori_loop(0, NS // 2, first_pair, 0)
    squeeze(0, (last - 1, last), (ST[last - 1], ST[last]))
    for g in (3, 4):
        send_sums(0, g, *SUMS[g])
        send_rows(0, g, *EDGES[g])

    def scales(slots, ss):
        tots = []
        for slot, s in zip(slots, ss):
            tots.append(SG[slot, s])
            for k in range(sp - 1):
                tots[-1] = tots[-1] + RS[slot, k, s]
        return affine(tots, [GAIN[pl.ds(k, 1)] for k in slots], [GAIN[pl.ds(k + SLOTS, 1)] for k in slots],
                      [EMB[k, pl.ds(s, 1)] for k, s in zip(slots, ss)], float(sp * NP * GSIZE))

    def prep_of(slot, s, L, a, b):
        def row(r):
            if r == 0:
                return unpack_row(HT.at[slot, s]), has_up
            if r == ROWS + 1:
                return unpack_row(HB.at[slot, s]), has_dn
            return held[slot][s, span(r - 1), :], None
        return prep_gen(row, ROWS, a, b, L)

    def epi_gen(j, s, Y, zero, tiles):
        acc, acq = no_stats(), no_stats()
        edge = {ROWS - 1: PB.at[j, s]}
        if j + 1 < end:
            edge[0] = PT.at[j, s]
        for o in range(ROWS):
            new = [x.astype(BF) for x in conv_row(Y, o, zero)]
            mark = new[2]
            for k in TRI:
                cols = span(k, LANE)
                if j % 2:
                    new[k] = (new[k].astype(F32) + held[j - 1][s, span(o), cols].astype(F32)).astype(BF)
                    cols_out = slice(k * LANE, min(k * LANE + LANE, CH))
                    HS[s, span(o), cols_out] = new[k][:, :cols_out.stop - cols_out.start]
                if j + 1 < end:
                    held[j + 1][s, span(o), cols] = new[k]
            if o in edge:
                pack_row(edge[o], new)
            if j + 1 < end:
                add_stats(acc, acq, new)
            if o == ROWS - 1:
                tiles.append(stats_tile(acc, acq))
            yield mark

    for g in DUO:
        wait_sums(0, g, SUMS[g][1])
    for c, v in enumerate(scales((0,) * 3, TRI)):
        AB[c] = v[:3]
    still = nil(me)
    for _ in prep_of(0, 0, L0, AB[0, :1], AB[1, :1]):
        pass
    for j in QUAD:
        if j % 2:
            for g in range(len(EDGES)):
                out_copy(j - 1, g, *EDGES[g]).wait()

        def body(i, carry, j=j):
            t = 2 * i
            zero = nil(i)
            turn = NS // 2 - 1
            ns = [jnp.minimum(j * NS + t + 3 + k, end * NS - 1) for k in DUO]
            for g in TRI:
                pl.when(i == 2 * g + 1)(functools.partial(wait_sums, j, g + 2, SUMS[g + 2][1]))
            for g in DUO:
                if j + 1 < end:
                    pl.when(i == turn - 1 + g)(functools.partial(wait_sums, j + 1, g, SUMS[g][1]))
            if j > 0:
                for g in TRI:
                    pl.when(i == 2 * g + 1)(functools.partial(wait_rows, j, g + 1, EDGES[g + 1][1]))
                pl.when(i == turn)(functools.partial(wait_rows, j, 4, EDGES[4][1]))
            if j + 1 < end:
                pl.when(i == turn)(functools.partial(wait_rows, j + 1, 0, EDGES[0][1]))
            for parts, send in ((EDGES, send_rows), (SUMS, send_sums))[:end - j]:
                for g in TRI:
                    pl.when(i == 2 * g + 2)(functools.partial(send, j + 1, g, *parts[g]))
            new = scales([n // NS for n in ns], [lax.rem(n, NS) for n in ns])
            co = [(AB[0, k:k + 1], AB[1, k:k + 1]) for k in (1, 2)]
            tiles = [STC[...]]
            for u, (Lc, Ln, Yc, Yp) in enumerate(((L0, L1, Y0, Y1), (L1, L0, Y1, Y0))):
                nxt = jnp.minimum(t + u + 1, last)
                weave(Lc, W.at[j], Yc, NP, prep_of(j, nxt, Ln, *co[u]), epi_gen(j, lax.rem(t + u + last, NS), Yp, zero, tiles), SHARE)
            for c in DUO:
                AB[c] = jnp.concatenate([co[1][c], new[c][:2]], 0)
            if j + 1 == end:
                return carry
            STC[...] = tiles.pop()
            squeeze(j + 1, [lax.rem(t + last - 1 + k, NS) for k in DUO], tiles)
            return carry

        lax.fori_loop(0, NS // 2, body, 0)
        send_rows(j + 1, 3, *EDGES[3])
        if j + 1 < end:
            send_sums(j + 1, 3, *SUMS[3])
        tiles = [STC[...]]
        for _ in epi_gen(j, last, Y1, still, tiles):
            pass
        if j + 1 < end:
            for _ in prep_of(j + 1, 0, L0, AB[0, :1], AB[1, :1]):
                pass
            squeeze(j + 1, (last - 1, last), tiles)
            send_sums(j + 1, 4, *SUMS[4])
        send_rows(j + 1, 4, *EDGES[4])

    for g in range(len(SUMS)):
        wait_rows(end, g, EDGES[g][1])
        out_copy(end, g, *EDGES[g]).wait()
        for slot in QUAD:
            sums_bytes(slot, SUMS[g][1], st_send, g).wait()
            up, down = rows_copies(slot + 1, g, *EDGES[g])
            if up is not None:
                if_up(up.wait_send)
            if_dn(down.wait_send)
    if_dn(q_dn.wait_send)
    if_up(q_up.wait_send)
    fin = pltpu.make_async_copy(HT.at[end], halo, fin_sem)
    fin.start()
    fin.wait()


def tail(hand, halo, bd, dw, h0o, h1o, h2o, do, P0, P1, P2, HA, W, WR, L0, L1, Y0, Y1, OD, DS, in_sem, ha_sem, wm_sem, wr_sem, o_sem, od_sem):
    me = lax.axis_index("sp")
    has_up = (me > 0).astype(jnp.int32)
    held, outs = (P0, P1, P2), (h0o, h1o, h2o)
    ahead = 6

    def take(k, s):
        return pltpu.make_async_copy(hand.at[k, s], held[k].at[s], in_sem.at[k, s])

    def put(k, s):
        return pltpu.make_async_copy(held[k].at[s], outs[k].at[s], o_sem.at[k, s])

    def fetch(s):
        for k in (2, 0, 1):
            take(k, s).start()

    get_halo = pltpu.make_async_copy(halo, HA, ha_sem)
    take(2, 0).start()
    get_halo.start()
    weight_copies(dw, W, WR, wm_sem, wr_sem)
    for k in DUO:
        take(k, 0).start()
    for s in range(1, ahead):
        fetch(s)
    for Y in (Y0, Y1):
        Y[...] = jnp.zeros_like(Y)
    get_halo.wait()
    take(2, 0).wait()
    still = nil(me)

    def row_of(s, r):
        if r == 0:
            return keep_if(has_up, unpack_row(HA.at[s]))
        return widen(P2[s, span(r - 1), :].astype(F32))

    def dprep(s, L):
        for o in QUAD:
            xs = [row_of(s, 2 * o + dy) for dy in TRI]
            for dy in TRI:
                L[span(o), span(dy, MAIN)] = xs[dy][:, :MAIN].astype(BF)
            store_rest(L, o, *(x[:, MAIN:] for x in xs))

    def depi(s, Y, zero):
        for o in QUAD:
            d = conv_row(Y, o, zero)
            for k in TRI:
                DS[o, k] = d[k]
            parts = [DS[o, k, pl.ds(0, ROW // 2, stride=2), :] for k in TRI]
            OD[s, span(o, ROW // 2), :] = jnp.concatenate(parts, 1)[:, :CH].astype(BF)

    def dhalf(t, Lc, Ln, Yc, Yp, zero):
        for n in QUAD:
            dot_chunk(Lc, W, Yc, slice(0, NP // 2), n)
        dprep(jnp.minimum(t + 1, NS - 1), Ln)
        depi(lax.rem(t + NS - 1, NS), Yp, zero)

    dprep(0, L0)
    weight_finish(bd[...].reshape(1, CH), W, WR, wm_sem, wr_sem)

    def dbody(i, carry):
        t = 2 * i
        zero = nil(i)
        for s in (t, t + 1):
            pl.when(s + ahead < NS)(functools.partial(fetch, s + ahead))
            pl.when(s + 1 < NS)(lambda s=s: take(2, s + 1).wait())
            put(2, s).start()
            for k in DUO:
                take(k, s).wait()
                put(k, s).start()
        dhalf(t, L0, L1, Y0, Y1, zero)
        dhalf(t + 1, L1, L0, Y1, Y0, zero)
        return carry

    lax.fori_loop(0, NS // 2, dbody, 0)
    depi(NS - 1, Y1, still)
    dout = pltpu.make_async_copy(OD, do, od_sem)
    dout.start()

    def drain(s, carry):
        for k in TRI:
            put(k, s).wait()
        return carry

    lax.fori_loop(0, NS, drain, 0)
    dout.wait()


def solution(mesh):
    sp = mesh.shape["sp"]

    def program(latent, time_emb, w_in, b_in, gn1_scale, gn1_shift, conv1_w, conv1_b, temb_w, temb_b, gn2_scale, gn2_shift, conv2_w, conv2_b, down_w, down_b):
        none = (0, 0)
        lat = jnp.pad(latent.transpose(0, 3, 1, 2), (none, none, none, (1, 1)))
        q = jnp.stack([lat[..., d:d + ROW] for d in TRI], 1).reshape(NS, 12, NP)
        q = jnp.pad(q, (none, (0, 4), none), constant_values=1)

        dma, vm = pltpu.SemaphoreType.DMA, pltpu.VMEM
        any_, vms = pl.BlockSpec(memory_space=pl.ANY), pl.BlockSpec(memory_space=pltpu.VMEM)
        params = functools.partial(pltpu.CompilerParams, vmem_limit_bytes=66_000_000)

        def big(n=NP, c=CP):
            return vm((NS, n, c), BF)

        def edge(n):
            return vm((n, NS, PK, MAIN), BF)

        def bufs(m):
            return [vm((m, KP), BF)] * 2 + [vm((8, m + 2 * OFF, LANE), F32)] * 2

        def out(*shape):
            return jax.ShapeDtypeStruct(shape, BF)

        hand, halo = pl.pallas_call(
            functools.partial(mega, sp),
            out_shape=(out(3, NS, NP, CH), out(NS, PK, MAIN)),
            in_specs=[vms] * 11 + [any_] * 3, out_specs=(any_, any_),
            scratch_shapes=[big(), big(), big(), big(NP, CH), vm((SLOTS, KP, KP), BF), vm((SLOTS, 9, CH, ROW), BF), vm((2, CH, temb_w.shape[1]), BF), vm((3 * NS, CP), F32)] + bufs(NP)
            + [vm((NS, OFF, LANE), F32), vm((OFF, LANE), F32), vm((SLOTS, NS, 2, LANE), F32), vm((SLOTS, sp - 1, NS, 2, LANE), F32), vm((2, 3, CP), F32), vm((SLOTS, NS, CP), F32), vm((OFF, CP), F32),
               edge(SLOTS + 1), edge(SLOTS), edge(SLOTS - 1), edge(SLOTS), vm((2, NS, NS, LANE), BF),
               dma((SLOTS,)), dma((SLOTS,)), dma] + [dma((2,))] * 2 + [dma((SLOTS + 1, len(SUMS)))] * 7 + [dma],
            compiler_params=params(collective_id=0, has_side_effects=True), name="mega",
        )(q, w_in, b_in, time_emb, temb_b, gn1_scale, gn1_shift, gn2_scale, gn2_shift, conv1_b, conv2_b, temb_w.transpose(0, 2, 1), conv1_w, conv2_w)
        outs = pl.pallas_call(
            tail,
            out_shape=(out(NS, NP, CH),) * 3 + (out(NS, NP // 4, CH),),
            in_specs=[any_] * 2 + [vms, any_], out_specs=(any_,) * 4,
            scratch_shapes=[big(NP, CH)] * 3 + [big(PK, MAIN), vm((KP, KP), BF), vm((9, CH, ROW), BF)] + bufs(NP // 2)
            + [big(NP // 4, CH), vm((4, 3, ROW, LANE), F32), dma((3, NS)), dma, dma, dma, dma((3, NS)), dma],
            compiler_params=params(), name="tail",
        )(hand, halo, down_b, down_w)
        return tuple(o.reshape(NS, n, m, CH) for o, n, m in zip(outs, [ROWS] * len(TRI) + [ROWS // 2], [ROW] * len(TRI) + [ROW // 2]))

    band = P("dp", "sp", None, None)
    return jax.shard_map(program, mesh=mesh, in_specs=(band, P("dp", None)) + (P(),) * 14, out_specs=(band,) * 4, check_vma=False)
```

```python
import functools

import jax
import jax.numpy as jnp
from jax import lax
from jax.experimental import pallas as pl
from jax.experimental.pallas import tpu as pltpu
from jax.sharding import PartitionSpec as P

F32, BF = jnp.float32, jnp.bfloat16
GN_GROUPS, GN_EPS = 32, 1e-5
NS, ROWS, ROW, LANE, MAIN = 16, 8, 64, 128, 256
NP = ROWS * ROW
CH = 320
CP = CH + ROW
KP = 4 * MAIN
REST = 3 * MAIN
SPARE = 3 * CH
OFF = 8
GSIZE = CH // GN_GROUPS
PK = ROW + NS
MESH = pl.DeviceIdType.MESH
DUO, TRI, QUAD = range(2), range(3), range(4)
SLOTS = len(QUAD)
NIL = 0.0


def groups(n, step):
    cuts = [0, *range(n, NS, step), NS]
    return [(a, b - a) for a, b in zip(cuts, cuts[1:])]


SUMS, EDGES = groups(2, SLOTS), groups(3, SLOTS)
SHARE = (1, 2, 3, 3)
ACC32 = dict(preferred_element_type=F32)
ROWS_DOT, COLS_DOT = ((((k,), (k,)), ((), ())) for k in DUO)


def nil(i):
    return jnp.minimum(i, 0) * OFF


def span(i, n=ROW, base=0):
    return slice(base + i * n, base + (i + 1) * n)


def low_half():
    return lax.broadcasted_iota(jnp.int32, (ROW, LANE), 1) < ROW


def widen(p):
    return jnp.concatenate([p, p[..., MAIN:]], -1)


def keep_if(flag, x):
    return jnp.where(jnp.full(x.shape, flag, jnp.int32) > 0, x, NIL)


def store_rest(L, o, r0, r1, r2):
    low = low_half()
    L[span(o), REST:REST + LANE] = jnp.where(low, r0, r1).astype(BF)
    L[span(o), REST + LANE:] = jnp.where(low, r2, 1.0).astype(BF)


def prep_gen(x_of_row, nrows, a, b, L):
    ha, hb = a * 0.5, b * 0.5
    rest = []
    for r in range(nrows + 2):
        x, flag = x_of_row(r)
        h = x.astype(F32) * ha + hb
        n = h + h * jnp.tanh(h)
        if flag is not None:
            n = keep_if(flag, n)
        main = n[:, :MAIN].astype(BF)
        rest.append(n[:, MAIN:])
        for dy in TRI:
            if 0 <= r - dy < nrows:
                L[span(r - dy), span(dy, MAIN)] = main
        if r >= 2:
            store_rest(L, r - 2, *rest[r - 2:])
        yield main


def shifted(v, step):
    v = pltpu.roll(v.reshape(OFF, OFF, LANE), step % OFF, 1)
    sub = lax.broadcasted_iota(jnp.int32, v.shape, 1)
    gap = jnp.zeros_like(v[:1])
    if step > 0:
        v = jnp.where(sub == 0, jnp.concatenate([gap, v[:-1]], 0), v)
    else:
        v = jnp.where(sub == OFF - 1, jnp.concatenate([v[1:], gap], 0), v)
    return v.reshape(ROW, LANE)


def conv_row(Y, o, zero):
    def here(k):
        return Y[k, span(o, base=OFF), :]

    out = [shifted(here(k), 1) + here(k + 2) + shifted(here(k + 4), -1) for k in DUO]
    a = here(6)
    mix = jnp.where(low_half(), shifted(a, 1), a)
    return out + [mix + pltpu.roll(mix, ROW, 1) + shifted(here(7), -1)]


def dot_chunk(L, W, Y, rows, n):
    r = jnp.dot(L[rows, :], W[:, span(n, MAIN)], **ACC32)
    for k in DUO:
        Y[2 * n + k, OFF + rows.start:OFF + rows.stop, :] = r[:, span(k, LANE)]


def weave(L, W, Y, m, prep, epi, share):
    work = [prep] * (m // ROW + 2) + [epi] * (m // ROW)
    done = 0
    for n in QUAD:
        dot_chunk(L, W, Y, slice(0, m), n)
        upto = len(work) * share[n] // share[-1]
        for g in work[done:upto]:
            mark = next(g)
        done = upto
        if n < len(QUAD) - 1:
            L[:NS, KP - NS:] = jnp.where(mark[:NS, LANE - NS:LANE].astype(F32) > NIL, 1.0, NIL).astype(BF)
    for g in (prep, epi):
        for _ in g:
            pass


def lane_left(x, k):
    return pltpu.roll(x, CP - k, 1)


def starts(k):
    lane = lax.broadcasted_iota(jnp.int32, (OFF, LANE), 1) + k * LANE
    return (lane % GSIZE == 0) & (lane < CH)


def stacked(rows):
    fill = [jnp.zeros((4 - len(rows), rows[0].shape[1]), F32)] * (len(rows) < 4)
    return jnp.concatenate(list(rows) + fill, 0)


def compact(tiles, embs):
    s = stacked([jnp.concatenate([t[k:k + 1] for k in TRI], 1) for t in tiles])
    q = stacked([jnp.concatenate([t[k + 3:k + 4] for k in TRI], 1) for t in tiles])
    e = stacked(embs)
    x = jnp.concatenate([s + float(NP) * e, q + e * (2.0 * s + float(NP) * e)], 0)
    w2 = x + lane_left(x, 1)
    w4 = w2 + lane_left(w2, 2)
    w8 = w4 + lane_left(w4, 4)
    w10 = w8 + lane_left(w2, 8)
    c = sum(jnp.where(starts(k), w10[:, span(k, LANE)], NIL) for k in TRI)
    return [jnp.concatenate([c[k:k + 1], c[k + 4:k + 5]], 0) for k in range(len(tiles))]


def affine(tots, gains, shifts, embs, count):
    x = jnp.concatenate([stacked([t[k:k + 1] for t in tots]) for k in DUO], 0)
    y = jnp.concatenate([jnp.where(starts(k), x, NIL) for k in TRI], 1)
    r2 = y + pltpu.roll(y, 1, 1)
    r4 = r2 + pltpu.roll(r2, 2, 1)
    r8 = r4 + pltpu.roll(r4, 4, 1)
    r = r8 + pltpu.roll(r2, 8, 1)
    lane = lax.broadcasted_iota(jnp.int32, (OFF, CP), 1)
    r = jnp.where(lane >= CH, pltpu.roll(r, ROW, 1), r) * (1.0 / count)
    mean, msq = r[:4], r[4:]
    a = stacked(gains) * lax.rsqrt(msq - mean * mean + GN_EPS)
    return a, stacked(shifts) + a * (stacked(embs) - mean)


def pack_row(dst, x):
    dst[:ROW, :] = jnp.concatenate(x[:2], 1)
    half = ROW // 2
    p = jnp.where(low_half()[:half], x[2][:half].astype(F32), x[2][half:].astype(F32))
    dst[ROW:, :] = jnp.concatenate([p[:NS], p[NS:]], 1).astype(BF)


def unpack_row(src):
    p = src[ROW:, :].astype(F32)
    p = jnp.concatenate([p[:, :LANE], p[:, LANE:]], 0)
    swap, low = pltpu.roll(p, ROW, 1), low_half()[:ROW // 2]
    rest = jnp.concatenate([jnp.where(low, p, swap), jnp.where(low, swap, p)], 0)
    return jnp.concatenate([src[:ROW, :].astype(F32), rest], 1)


def stats_tile(acc, acq):
    parts = [x.sum(0, keepdims=True) for x in acc + acq]
    return jnp.concatenate(parts + [jnp.zeros((2, LANE), F32)], 0)


def add_stats(acc, acq, new):
    for k, x in enumerate(new):
        v = x.astype(F32).reshape(OFF, OFF, LANE)
        acc[k] = acc[k] + v.sum(0)
        acq[k] = acq[k] + (v * v).sum(0)


def no_stats():
    return [jnp.zeros((OFF, LANE), F32) for _ in TRI]


def weight_copies(src, W, WR, sem_main, sem_rest):
    for dy in TRI:
        for dx in TRI:
            cols = span(dx, MAIN)
            pltpu.make_async_copy(src.at[dy, dx, :MAIN, :MAIN], W.at[span(dy, MAIN), cols], sem_main).start()
            pltpu.make_async_copy(src.at[dy, dx, MAIN:, :MAIN], W.at[span(dy, base=REST), cols], sem_main).start()
            pltpu.make_async_copy(src.at[dy, dx, :, MAIN:], WR.at[dy * 3 + dx], sem_rest).start()


def weight_finish(bias, W, WR, sem_main, sem_rest):
    main = W.at[:SPARE, :REST]
    pltpu.make_async_copy(main, main, sem_main).wait()
    pltpu.make_async_copy(WR, WR, sem_rest).wait()
    for dy in TRI:
        for part, rows in ((slice(0, MAIN), span(dy, MAIN)), (slice(MAIN, CH), span(dy, base=REST))):
            w0, w1, w2 = (WR[dy * 3 + dx, part, :] for dx in TRI)
            W[rows, REST:REST + LANE] = jnp.concatenate([w0, w1], 1)
            W[rows, REST + LANE:] = jnp.concatenate([w2, w2], 1)
    b = widen(bias.astype(F32))
    gap = jnp.zeros((1, MAIN), F32)
    rest = jnp.where(low_half()[:1], 0.0, b[:, MAIN:])
    row = jnp.concatenate([gap, b[:, :MAIN], gap, rest, gap[:, :LANE]], 1)
    first = lax.broadcasted_iota(jnp.int32, (ROW, KP), 0) == 0
    W[SPARE:, :] = jnp.where(first, row, NIL).astype(BF)


def mega(sp, lat, wi, bi, temb, tb, g1, s1, g2, s2, b1, b2, tw, w1, w2, hand, halo,
         H, U, H2, HS, W, WR, TW, WI, L0, L1, Y0, Y1, ST, STC, SG, RS, AB, EMB, GAIN, HT, HB, PT, PB, LQ,
         wm_sem, wr_sem, tw_sem, q_send, q_recv, st_send, st_recv, up_send, dn_send, ht_recv, hb_recv, out_sem, fin_sem):
    me, dp = lax.axis_index("sp"), lax.axis_index("dp")
    has_up, has_dn = (me > 0).astype(jnp.int32), (me < sp - 1).astype(jnp.int32)
    held = (H, U, H2, U)
    end = SLOTS
    last = NS - 1

    get_tw = pltpu.make_async_copy(tw, TW, tw_sem)
    get_tw.start()
    for j, src in enumerate((w1.at[0], w2.at[0], w1.at[1], w2.at[1])):
        weight_copies(src, W.at[j], WR.at[j], wm_sem.at[j], wr_sem.at[j])

    barrier = pltpu.get_barrier_semaphore()
    for k in range(1, sp):
        pl.semaphore_signal(barrier, inc=1, device_id=(dp, lax.rem(me + k, sp)), device_id_type=MESH)
    for k, (ref, l) in enumerate((ref, l) for pair in ((g1, g2), (s1, s2)) for l in DUO for ref in pair):
        GAIN[k:k + 1, :] = widen(ref[l:l + 1, :].astype(F32))
    WI[...] = jnp.zeros_like(WI)
    for dy in TRI:
        for dx in TRI:
            WI[span(4 * dy + dx, 4), :] = widen(wi[dy, dx].astype(F32))
    WI[NS + 12:NS + 13, :] = widen(bi[...].reshape(1, CH).astype(F32))
    get_tw.wait()
    x = temb[...].astype(F32)
    act = (x * jax.nn.sigmoid(x)).astype(BF)
    for l in DUO:
        pr = lax.dot_general(act, TW[l], COLS_DOT, **ACC32)
        EMB[2 * l] = jnp.zeros((NS, CP), F32)
        EMB[2 * l + 1] = widen(pr + tb[l:l + 1, :].astype(F32))
    for Y in (Y0, Y1):
        Y[...] = jnp.zeros_like(Y)
    pl.semaphore_wait(barrier, sp - 1)

    def remote(src, dst, ssem, rsem, dev):
        return pltpu.make_async_remote_copy(src_ref=src, dst_ref=dst, send_sem=ssem, recv_sem=rsem, device_id=(dp, dev), device_id_type=MESH)

    def if_up(f):
        pl.when(me > 0)(f)

    def if_dn(f):
        pl.when(me < sp - 1)(f)

    q_dn = remote(lat.at[:, ROWS - 2:], LQ.at[0], q_send.at[0], q_recv.at[0], me + 1)
    q_up = remote(lat.at[:, :2], LQ.at[1], q_send.at[1], q_recv.at[1], me - 1)
    if_dn(q_dn.start)
    if_up(q_up.start)

    def rows_copies(slot, g, lo, n):
        ss = pl.ds(lo, n)
        down = remote(PB.at[slot - 1, ss], HT.at[slot, ss], dn_send.at[slot, g], ht_recv.at[slot, g], me + 1)
        if slot == end:
            return None, down
        return remote(PT.at[slot - 1, ss], HB.at[slot, ss], up_send.at[slot, g], hb_recv.at[slot, g], me - 1), down

    def out_copy(slot, g, lo, n):
        ss = pl.ds(lo, n)
        return pltpu.make_async_copy(HS.at[ss], hand.at[slot // 2, ss], out_sem.at[slot, g])

    def send_sums(slot, g, lo, n):
        ss = pl.ds(lo, n)
        for k in range(1, sp):
            remote(SG.at[slot, ss], RS.at[slot, k - 1, ss], st_send.at[slot, g], st_recv.at[slot, g], lax.rem(me + k, sp)).start()

    def send_rows(slot, g, lo, n):
        if slot % 2 == 0:
            out_copy(slot, g, lo, n).start()
        if slot > 0:
            up, down = rows_copies(slot, g, lo, n)
            if up is not None:
                if_up(up.start)
            if_dn(down.start)

    def sums_bytes(slot, n, sem, g):
        both = RS.at[slot, :, :n]
        return pltpu.make_async_copy(both, both, sem.at[slot, g])

    def wait_sums(slot, g, n):
        sums_bytes(slot, n, st_recv, g).wait()

    def wait_rows(slot, g, n):
        ss = pl.ds(0, n)
        if_up(lambda: remote(PB.at[0, ss], HT.at[slot, ss], dn_send.at[slot, g], ht_recv.at[slot, g], me).wait_recv())
        if slot is not end:
            if_dn(lambda: remote(PT.at[0, ss], HB.at[slot, ss], up_send.at[slot, g], hb_recv.at[slot, g], me).wait_recv())

    def squeeze(slot, ss, tiles):
        for r, s in zip(compact(tiles, [EMB[slot, pl.ds(s, 1)] for s in ss]), ss):
            SG[slot, s] = r

    if_up(q_dn.wait_recv)
    if_dn(q_up.wait_recv)

    def first(s):
        above, own, below = (x.astype(F32) for x in (LQ[0, s], lat[s], LQ[1, s]))
        rows = [keep_if(has_up, above[k]) for k in DUO] + [own[k] for k in range(ROWS)] + [keep_if(has_dn, below[k]) for k in DUO]
        ext = jnp.concatenate(rows, 1)
        col = lax.broadcasted_iota(jnp.int32, ext.shape, 1) % ROW
        left = jnp.where(col == 0, NIL, pltpu.roll(ext, 1, 1))
        right = jnp.where(col == ROW - 1, NIL, pltpu.roll(ext, ext.shape[1] - 1, 1))
        ext = jnp.concatenate([left, ext, right, jnp.ones_like(ext)], 0)
        mid = pltpu.roll(ext, ext.shape[1] - ROW, 1)
        wide = NP + LANE
        lhs = jnp.concatenate([ext[:, :wide], mid[:, :wide], ext[:, LANE:]], 0).astype(BF)
        r = lax.dot_general(lhs, WI[...].astype(BF), ROWS_DOT, **ACC32)
        acc, acq = no_stats(), no_stats()
        for o in range(ROWS + 2):
            x = r[span(o), :].astype(BF)
            parts = [x[:, span(k, LANE)] for k in TRI]
            if o == 0:
                pack_row(HT.at[0, s], parts)
            elif o > ROWS:
                pack_row(HB.at[0, s], parts)
            else:
                H[s, span(o - 1), :] = x
                HS[s, span(o - 1), :] = x[:, :CH]
                add_stats(acc, acq, parts)
        ST[s] = stats_tile(acc, acq)

    def first_pair(i, carry):
        t = 2 * i
        for g in TRI:
            for parts, send in ((EDGES, send_rows), (SUMS, send_sums)):
                pl.when(i == 2 * g + 2)(functools.partial(send, 0, g, *parts[g]))
        ss = [lax.rem(n + NS, NS) for n in (t - 2, t - 1)]
        tiles = [ST[s] for s in ss]
        first(t)
        first(t + 1)
        squeeze(0, ss, tiles)
        return carry

    lax.fori_loop(0, NS // 2, first_pair, 0)
    squeeze(0, (last - 1, last), (ST[last - 1], ST[last]))
    for j in QUAD:
        weight_finish((b1, b2)[j % 2][j // 2:j // 2 + 1, :], W.at[j], WR.at[j], wm_sem.at[j], wr_sem.at[j])
    for g in (3, 4):
        send_sums(0, g, *SUMS[g])
        send_rows(0, g, *EDGES[g])

    def scales(slots, ss):
        tots = []
        for slot, s in zip(slots, ss):
            tots.append(SG[slot, s])
            for k in range(sp - 1):
                tots[-1] = tots[-1] + RS[slot, k, s]
        return affine(tots, [GAIN[pl.ds(k, 1)] for k in slots], [GAIN[pl.ds(k + SLOTS, 1)] for k in slots],
                      [EMB[k, pl.ds(s, 1)] for k, s in zip(slots, ss)], float(sp * NP * GSIZE))

    def prep_of(slot, s, L, a, b):
        def row(r):
            if r == 0:
                return unpack_row(HT.at[slot, s]), has_up
            if r == ROWS + 1:
                return unpack_row(HB.at[slot, s]), has_dn
            return held[slot][s, span(r - 1), :], None
        return prep_gen(row, ROWS, a, b, L)

    def epi_gen(j, s, Y, zero, tiles):
        acc, acq = no_stats(), no_stats()
        edge = {ROWS - 1: PB.at[j, s]}
        if j + 1 < end:
            edge[0] = PT.at[j, s]
        for o in range(ROWS):
            new = [x.astype(BF) for x in conv_row(Y, o, zero)]
            mark = new[2]
            for k in TRI:
                cols = span(k, LANE)
                if j % 2:
                    new[k] = (new[k].astype(F32) + held[j - 1][s, span(o), cols].astype(F32)).astype(BF)
                    cols_out = slice(k * LANE, min(k * LANE + LANE, CH))
                    HS[s, span(o), cols_out] = new[k][:, :cols_out.stop - cols_out.start]
                if j + 1 < end:
                    held[j + 1][s, span(o), cols] = new[k]
            if o in edge:
                pack_row(edge[o], new)
            if j + 1 < end:
                add_stats(acc, acq, new)
            if o == ROWS - 1:
                tiles.append(stats_tile(acc, acq))
            yield mark

    for g in DUO:
        wait_sums(0, g, SUMS[g][1])
    for c, v in enumerate(scales((0,) * 3, TRI)):
        AB[c] = v[:3]
    still = nil(me)
    for _ in prep_of(0, 0, L0, AB[0, :1], AB[1, :1]):
        pass
    for j in QUAD:
        if j % 2:
            for g in range(len(EDGES)):
                out_copy(j - 1, g, *EDGES[g]).wait()

        def body(i, carry, j=j):
            t = 2 * i
            zero = nil(i)
            turn = NS // 2 - 1
            ns = [jnp.minimum(j * NS + t + 3 + k, end * NS - 1) for k in DUO]
            for g in TRI:
                pl.when(i == 2 * g + 1)(functools.partial(wait_sums, j, g + 2, SUMS[g + 2][1]))
            for g in DUO:
                if j + 1 < end:
                    pl.when(i == turn - 1 + g)(functools.partial(wait_sums, j + 1, g, SUMS[g][1]))
            if j > 0:
                for g in TRI:
                    pl.when(i == 2 * g + 1)(functools.partial(wait_rows, j, g + 1, EDGES[g + 1][1]))
                pl.when(i == turn)(functools.partial(wait_rows, j, 4, EDGES[4][1]))
            if j + 1 < end:
                pl.when(i == turn)(functools.partial(wait_rows, j + 1, 0, EDGES[0][1]))
            for parts, send in ((EDGES, send_rows), (SUMS, send_sums))[:end - j]:
                for g in TRI:
                    pl.when(i == 2 * g + 2)(functools.partial(send, j + 1, g, *parts[g]))
            new = scales([n // NS for n in ns], [lax.rem(n, NS) for n in ns])
            co = [(AB[0, k:k + 1], AB[1, k:k + 1]) for k in (1, 2)]
            tiles = [STC[...]]
            for u, (Lc, Ln, Yc, Yp) in enumerate(((L0, L1, Y0, Y1), (L1, L0, Y1, Y0))):
                nxt = jnp.minimum(t + u + 1, last)
                weave(Lc, W.at[j], Yc, NP, prep_of(j, nxt, Ln, *co[u]), epi_gen(j, lax.rem(t + u + last, NS), Yp, zero, tiles), SHARE)
            for c in DUO:
                AB[c] = jnp.concatenate([co[1][c], new[c][:2]], 0)
            if j + 1 == end:
                return carry
            STC[...] = tiles.pop()
            squeeze(j + 1, [lax.rem(t + last - 1 + k, NS) for k in DUO], tiles)
            return carry

        lax.fori_loop(0, NS // 2, body, 0)
        send_rows(j + 1, 3, *EDGES[3])
        if j + 1 < end:
            send_sums(j + 1, 3, *SUMS[3])
        tiles = [STC[...]]
        for _ in epi_gen(j, last, Y1, still, tiles):
            pass
        if j + 1 < end:
            for _ in prep_of(j + 1, 0, L0, AB[0, :1], AB[1, :1]):
                pass
            squeeze(j + 1, (last - 1, last), tiles)
            send_sums(j + 1, 4, *SUMS[4])
        send_rows(j + 1, 4, *EDGES[4])

    for g in range(len(SUMS)):
        wait_rows(end, g, EDGES[g][1])
        out_copy(end, g, *EDGES[g]).wait()
        for slot in QUAD:
            sums_bytes(slot, SUMS[g][1], st_send, g).wait()
            up, down = rows_copies(slot + 1, g, *EDGES[g])
            if up is not None:
                if_up(up.wait_send)
            if_dn(down.wait_send)
    if_dn(q_dn.wait_send)
    if_up(q_up.wait_send)
    fin = pltpu.make_async_copy(HT.at[end], halo, fin_sem)
    fin.start()
    fin.wait()


def tail(hand, halo, bd, dw, h0o, h1o, h2o, do, P0, P1, P2, HA, W, WR, L0, L1, Y0, Y1, OD, DS, in_sem, ha_sem, wm_sem, wr_sem, o_sem, od_sem):
    me = lax.axis_index("sp")
    has_up = (me > 0).astype(jnp.int32)
    held, outs = (P0, P1, P2), (h0o, h1o, h2o)
    ahead = 6

    def take(k, s):
        return pltpu.make_async_copy(hand.at[k, s], held[k].at[s], in_sem.at[k, s])

    def put(k, s):
        return pltpu.make_async_copy(held[k].at[s], outs[k].at[s], o_sem.at[k, s])

    def fetch(s):
        for k in (2, 0, 1):
            take(k, s).start()

    get_halo = pltpu.make_async_copy(halo, HA, ha_sem)
    take(2, 0).start()
    get_halo.start()
    weight_copies(dw, W, WR, wm_sem, wr_sem)
    for k in DUO:
        take(k, 0).start()
    for s in range(1, ahead):
        fetch(s)
    for Y in (Y0, Y1):
        Y[...] = jnp.zeros_like(Y)
    get_halo.wait()
    take(2, 0).wait()
    still = nil(me)

    def row_of(s, r):
        if r == 0:
            return keep_if(has_up, unpack_row(HA.at[s]))
        return widen(P2[s, span(r - 1), :].astype(F32))

    def dprep(s, L):
        for o in QUAD:
            xs = [row_of(s, 2 * o + dy) for dy in TRI]
            for dy in TRI:
                L[span(o), span(dy, MAIN)] = xs[dy][:, :MAIN].astype(BF)
            store_rest(L, o, *(x[:, MAIN:] for x in xs))

    def depi(s, Y, zero):
        for o in QUAD:
            d = conv_row(Y, o, zero)
            for k in TRI:
                DS[o, k] = d[k]
            parts = [DS[o, k, pl.ds(0, ROW // 2, stride=2), :] for k in TRI]
            OD[s, span(o, ROW // 2), :] = jnp.concatenate(parts, 1)[:, :CH].astype(BF)

    def dhalf(t, Lc, Ln, Yc, Yp, zero):
        for n in QUAD:
            dot_chunk(Lc, W, Yc, slice(0, NP // 2), n)
        dprep(jnp.minimum(t + 1, NS - 1), Ln)
        depi(lax.rem(t + NS - 1, NS), Yp, zero)

    dprep(0, L0)
    weight_finish(bd[...].reshape(1, CH), W, WR, wm_sem, wr_sem)

    def dbody(i, carry):
        t = 2 * i
        zero = nil(i)
        for s in (t, t + 1):
            pl.when(s + ahead < NS)(functools.partial(fetch, s + ahead))
            pl.when(s + 1 < NS)(lambda s=s: take(2, s + 1).wait())
            put(2, s).start()
            for k in DUO:
                take(k, s).wait()
                put(k, s).start()
        dhalf(t, L0, L1, Y0, Y1, zero)
        dhalf(t + 1, L1, L0, Y1, Y0, zero)
        return carry

    lax.fori_loop(0, NS // 2, dbody, 0)
    depi(NS - 1, Y1, still)
    dout = pltpu.make_async_copy(OD, do, od_sem)
    dout.start()

    def drain(s, carry):
        for k in TRI:
            put(k, s).wait()
        return carry

    lax.fori_loop(0, NS, drain, 0)
    dout.wait()


def solution(mesh):
    sp = mesh.shape["sp"]

    def program(latent, time_emb, w_in, b_in, gn1_scale, gn1_shift, conv1_w, conv1_b, temb_w, temb_b, gn2_scale, gn2_shift, conv2_w, conv2_b, down_w, down_b):
        dma, vm = pltpu.SemaphoreType.DMA, pltpu.VMEM
        any_, vms = pl.BlockSpec(memory_space=pl.ANY), pl.BlockSpec(memory_space=pltpu.VMEM)
        params = functools.partial(pltpu.CompilerParams, vmem_limit_bytes=66_000_000)

        def big(n=NP, c=CP):
            return vm((NS, n, c), BF)

        def edge(n):
            return vm((n, NS, PK, MAIN), BF)

        def bufs(m):
            return [vm((m, KP), BF)] * 2 + [vm((8, m + 2 * OFF, LANE), F32)] * 2

        def out(*shape):
            return jax.ShapeDtypeStruct(shape, BF)

        hand, halo = pl.pallas_call(
            functools.partial(mega, sp),
            out_shape=(out(3, NS, NP, CH), out(NS, PK, MAIN)),
            in_specs=[vms] * 11 + [any_] * 3, out_specs=(any_, any_),
            scratch_shapes=[big(), big(), big(), big(NP, CH), vm((SLOTS, KP, KP), BF), vm((SLOTS, 9, CH, ROW), BF), vm((2, CH, temb_w.shape[1]), BF), vm((3 * NS, CP), F32)] + bufs(NP)
            + [vm((NS, OFF, LANE), F32), vm((OFF, LANE), F32), vm((SLOTS, NS, 2, LANE), F32), vm((SLOTS, sp - 1, NS, 2, LANE), F32), vm((2, 3, CP), F32), vm((SLOTS, NS, CP), F32), vm((OFF, CP), F32),
               edge(SLOTS + 1), edge(SLOTS), edge(SLOTS - 1), edge(SLOTS), vm((2, NS, 2, 4, ROW), BF),
               dma((SLOTS,)), dma((SLOTS,)), dma] + [dma((2,))] * 2 + [dma((SLOTS + 1, len(SUMS)))] * 7 + [dma],
            compiler_params=params(collective_id=0, has_side_effects=True), name="mega",
        )(latent.transpose(0, 1, 3, 2), w_in, b_in, time_emb, temb_b, gn1_scale, gn1_shift, gn2_scale, gn2_shift, conv1_b, conv2_b, temb_w.transpose(0, 2, 1), conv1_w, conv2_w)
        outs = pl.pallas_call(
            tail,
            out_shape=(out(NS, NP, CH),) * 3 + (out(NS, NP // 4, CH),),
            in_specs=[any_] * 2 + [vms, any_], out_specs=(any_,) * 4,
            scratch_shapes=[big(NP, CH)] * 3 + [big(PK, MAIN), vm((KP, KP), BF), vm((9, CH, ROW), BF)] + bufs(NP // 2)
            + [big(NP // 4, CH), vm((4, 3, ROW, LANE), F32), dma((3, NS)), dma, dma, dma, dma((3, NS)), dma],
            compiler_params=params(), name="tail",
        )(hand, halo, down_b, down_w)
        return tuple(o.reshape(NS, n, m, CH) for o, n, m in zip(outs, [ROWS] * len(TRI) + [ROWS // 2], [ROW] * len(TRI) + [ROW // 2]))

    band = P("dp", "sp", None, None)
    return jax.shard_map(program, mesh=mesh, in_specs=(band, P("dp", None)) + (P(),) * 14, out_specs=(band,) * 4, check_vma=False)
```

```python
import functools

import jax
import jax.numpy as jnp
from jax import lax
from jax.experimental import pallas as pl
from jax.experimental.pallas import tpu as pltpu
from jax.sharding import PartitionSpec as P

F32, BF = jnp.float32, jnp.bfloat16
GN_GROUPS, GN_EPS = 32, 1e-5
NS, ROWS, ROW, LANE, MAIN = 16, 8, 64, 128, 256
NP = ROWS * ROW
CH = 320
CP = CH + ROW
KP = 4 * MAIN
REST = 3 * MAIN
SPARE = 3 * CH
OFF = 8
GSIZE = CH // GN_GROUPS
PK = ROW + NS
MESH = pl.DeviceIdType.MESH
DUO, TRI, QUAD = range(2), range(3), range(4)
SLOTS = len(QUAD)
NIL = 0.0


def groups(n, step):
    cuts = [0, *range(n, NS, step), NS]
    return [(a, b - a) for a, b in zip(cuts, cuts[1:])]


SUMS, EDGES = groups(2, SLOTS), groups(3, SLOTS)
LATE = [(0, 3), (3, 6), (9, 4), (13, 2), (15, 1)]
SHARE = (1, 2, 3, 3)
ACC32 = dict(preferred_element_type=F32)
ROWS_DOT, COLS_DOT = ((((k,), (k,)), ((), ())) for k in DUO)


def nil(i):
    return jnp.minimum(i, 0) * OFF


def span(i, n=ROW, base=0):
    return slice(base + i * n, base + (i + 1) * n)


def low_half():
    return lax.broadcasted_iota(jnp.int32, (ROW, LANE), 1) < ROW


def widen(p):
    return jnp.concatenate([p, p[..., MAIN:]], -1)


def keep_if(flag, x):
    return jnp.where(jnp.full(x.shape, flag, jnp.int32) > 0, x, NIL)


def store_rest(L, o, r0, r1, r2):
    low = low_half()
    L[span(o), REST:REST + LANE] = jnp.where(low, r0, r1).astype(BF)
    L[span(o), REST + LANE:] = jnp.where(low, r2, 1.0).astype(BF)


def prep_gen(x_of_row, nrows, a, b, L):
    ha, hb = a * 0.5, b * 0.5
    rest = []
    for r in range(nrows + 2):
        x, flag = x_of_row(r)
        h = x.astype(F32) * ha + hb
        n = h + h * jnp.tanh(h)
        if flag is not None:
            n = keep_if(flag, n)
        main = n[:, :MAIN].astype(BF)
        rest.append(n[:, MAIN:])
        for dy in TRI:
            if 0 <= r - dy < nrows:
                L[span(r - dy), span(dy, MAIN)] = main
        if r >= 2:
            store_rest(L, r - 2, *rest[r - 2:])
        yield main


def shifted(v, step):
    v = pltpu.roll(v.reshape(OFF, OFF, LANE), step % OFF, 1)
    sub = lax.broadcasted_iota(jnp.int32, v.shape, 1)
    gap = jnp.zeros_like(v[:1])
    if step > 0:
        v = jnp.where(sub == 0, jnp.concatenate([gap, v[:-1]], 0), v)
    else:
        v = jnp.where(sub == OFF - 1, jnp.concatenate([v[1:], gap], 0), v)
    return v.reshape(ROW, LANE)


def conv_row(Y, o, zero):
    def here(k):
        return Y[k, span(o, base=OFF), :]

    out = [shifted(here(k), 1) + here(k + 2) + shifted(here(k + 4), -1) for k in DUO]
    a = here(6)
    mix = jnp.where(low_half(), shifted(a, 1), a)
    return out + [mix + pltpu.roll(mix, ROW, 1) + shifted(here(7), -1)]


def dot_chunk(L, W, Y, rows, n):
    r = jnp.dot(L[rows, :], W[:, span(n, MAIN)], **ACC32)
    for k in DUO:
        Y[2 * n + k, OFF + rows.start:OFF + rows.stop, :] = r[:, span(k, LANE)]


def weave(L, W, Y, m, prep, epi, share):
    work = [prep] * (m // ROW + 2) + [epi] * (m // ROW)
    done = 0
    for n in QUAD:
        dot_chunk(L, W, Y, slice(0, m), n)
        upto = len(work) * share[n] // share[-1]
        for g in work[done:upto]:
            mark = next(g)
        done = upto
        if n < len(QUAD) - 1:
            L[:NS, KP - NS:] = jnp.where(mark[:NS, LANE - NS:LANE].astype(F32) > NIL, 1.0, NIL).astype(BF)
    for g in (prep, epi):
        for _ in g:
            pass


def lane_left(x, k):
    return pltpu.roll(x, CP - k, 1)


def starts(k):
    lane = lax.broadcasted_iota(jnp.int32, (OFF, LANE), 1) + k * LANE
    return (lane % GSIZE == 0) & (lane < CH)


def stacked(rows):
    fill = [jnp.zeros((4 - len(rows), rows[0].shape[1]), F32)] * (len(rows) < 4)
    return jnp.concatenate(list(rows) + fill, 0)


def compact(tiles, embs):
    s = stacked([jnp.concatenate([t[k:k + 1] for k in TRI], 1) for t in tiles])
    q = stacked([jnp.concatenate([t[k + 3:k + 4] for k in TRI], 1) for t in tiles])
    e = stacked(embs)
    x = jnp.concatenate([s + float(NP) * e, q + e * (2.0 * s + float(NP) * e)], 0)
    w2 = x + lane_left(x, 1)
    w4 = w2 + lane_left(w2, 2)
    w8 = w4 + lane_left(w4, 4)
    w10 = w8 + lane_left(w2, 8)
    c = sum(jnp.where(starts(k), w10[:, span(k, LANE)], NIL) for k in TRI)
    return [jnp.concatenate([c[k:k + 1], c[k + 4:k + 5]], 0) for k in range(len(tiles))]


def affine(tots, gains, shifts, embs, count):
    x = jnp.concatenate([stacked([t[k:k + 1] for t in tots]) for k in DUO], 0)
    y = jnp.concatenate([jnp.where(starts(k), x, NIL) for k in TRI], 1)
    r2 = y + pltpu.roll(y, 1, 1)
    r4 = r2 + pltpu.roll(r2, 2, 1)
    r8 = r4 + pltpu.roll(r4, 4, 1)
    r = r8 + pltpu.roll(r2, 8, 1)
    lane = lax.broadcasted_iota(jnp.int32, (OFF, CP), 1)
    r = jnp.where(lane >= CH, pltpu.roll(r, ROW, 1), r) * (1.0 / count)
    mean, msq = r[:4], r[4:]
    a = stacked(gains) * lax.rsqrt(msq - mean * mean + GN_EPS)
    return a, stacked(shifts) + a * (stacked(embs) - mean)


def pack_row(dst, x):
    dst[:ROW, :] = jnp.concatenate(x[:2], 1)
    half = ROW // 2
    p = jnp.where(low_half()[:half], x[2][:half].astype(F32), x[2][half:].astype(F32))
    dst[ROW:, :] = jnp.concatenate([p[:NS], p[NS:]], 1).astype(BF)


def unpack_row(src):
    p = src[ROW:, :].astype(F32)
    p = jnp.concatenate([p[:, :LANE], p[:, LANE:]], 0)
    swap, low = pltpu.roll(p, ROW, 1), low_half()[:ROW // 2]
    rest = jnp.concatenate([jnp.where(low, p, swap), jnp.where(low, swap, p)], 0)
    return jnp.concatenate([src[:ROW, :].astype(F32), rest], 1)


def stats_tile(acc, acq):
    parts = [x.sum(0, keepdims=True) for x in acc + acq]
    return jnp.concatenate(parts + [jnp.zeros((2, LANE), F32)], 0)


def add_stats(acc, acq, new):
    for k, x in enumerate(new):
        v = x.astype(F32).reshape(OFF, OFF, LANE)
        acc[k] = acc[k] + v.sum(0)
        acq[k] = acq[k] + (v * v).sum(0)


def no_stats():
    return [jnp.zeros((OFF, LANE), F32) for _ in TRI]


def weight_copies(src, W, WR, sem_main, sem_rest):
    for dy in TRI:
        for dx in TRI:
            cols = span(dx, MAIN)
            pltpu.make_async_copy(src.at[dy, dx, :MAIN, :MAIN], W.at[span(dy, MAIN), cols], sem_main).start()
            pltpu.make_async_copy(src.at[dy, dx, MAIN:, :MAIN], W.at[span(dy, base=REST), cols], sem_main).start()
            pltpu.make_async_copy(src.at[dy, dx, :, MAIN:], WR.at[dy * 3 + dx], sem_rest).start()


def weight_finish(bias, W, WR, sem_main, sem_rest):
    main = W.at[:SPARE, :REST]
    pltpu.make_async_copy(main, main, sem_main).wait()
    pltpu.make_async_copy(WR, WR, sem_rest).wait()
    for dy in TRI:
        for part, rows in ((slice(0, MAIN), span(dy, MAIN)), (slice(MAIN, CH), span(dy, base=REST))):
            w0, w1, w2 = (WR[dy * 3 + dx, part, :] for dx in TRI)
            W[rows, REST:REST + LANE] = jnp.concatenate([w0, w1], 1)
            W[rows, REST + LANE:] = jnp.concatenate([w2, w2], 1)
    b = widen(bias.astype(F32))
    gap = jnp.zeros((1, MAIN), F32)
    rest = jnp.where(low_half()[:1], 0.0, b[:, MAIN:])
    row = jnp.concatenate([gap, b[:, :MAIN], gap, rest, gap[:, :LANE]], 1)
    first = lax.broadcasted_iota(jnp.int32, (ROW, KP), 0) == 0
    W[SPARE:, :] = jnp.where(first, row, NIL).astype(BF)


def mega(sp, lat, wi, bi, temb, tb, g1, s1, g2, s2, b1, b2, tw, w1, w2, hand, halo,
         H, U, H2, HS, W, WR, TW, WI, L0, L1, Y0, Y1, ST, STC, SG, RS, AB, EMB, GAIN, HT, HB, PT, PB, LQ,
         wm_sem, wr_sem, tw_sem, q_send, q_recv, st_send, st_recv, up_send, dn_send, ht_recv, hb_recv, out_sem, fin_sem):
    me, dp = lax.axis_index("sp"), lax.axis_index("dp")
    has_up, has_dn = (me > 0).astype(jnp.int32), (me < sp - 1).astype(jnp.int32)
    held = (H, U, H2, U)
    end = SLOTS
    last = NS - 1

    get_tw = pltpu.make_async_copy(tw, TW, tw_sem)
    get_tw.start()
    for j, src in enumerate((w1.at[0], w2.at[0], w1.at[1], w2.at[1])):
        weight_copies(src, W.at[j], WR.at[j], wm_sem.at[j], wr_sem.at[j])

    barrier = pltpu.get_barrier_semaphore()
    for k in range(1, sp):
        pl.semaphore_signal(barrier, inc=1, device_id=(dp, lax.rem(me + k, sp)), device_id_type=MESH)
    for k, (ref, l) in enumerate((ref, l) for pair in ((g1, g2), (s1, s2)) for l in DUO for ref in pair):
        GAIN[k:k + 1, :] = widen(ref[l:l + 1, :].astype(F32))
    WI[...] = jnp.zeros_like(WI)
    for dy in TRI:
        for dx in TRI:
            WI[span(4 * dy + dx, 4), :] = widen(wi[dy, dx].astype(F32))
    WI[NS + 12:NS + 13, :] = widen(bi[...].reshape(1, CH).astype(F32))
    get_tw.wait()
    x = temb[...].astype(F32)
    act = (x * jax.nn.sigmoid(x)).astype(BF)
    for l in DUO:
        pr = lax.dot_general(act, TW[l], COLS_DOT, **ACC32)
        EMB[2 * l] = jnp.zeros((NS, CP), F32)
        EMB[2 * l + 1] = widen(pr + tb[l:l + 1, :].astype(F32))
    for Y in (Y0, Y1):
        Y[...] = jnp.zeros_like(Y)
    pl.semaphore_wait(barrier, sp - 1)

    def remote(src, dst, ssem, rsem, dev):
        return pltpu.make_async_remote_copy(src_ref=src, dst_ref=dst, send_sem=ssem, recv_sem=rsem, device_id=(dp, dev), device_id_type=MESH)

    def if_up(f):
        pl.when(me > 0)(f)

    def if_dn(f):
        pl.when(me < sp - 1)(f)

    q_dn = remote(lat.at[:, ROWS - 2:], LQ.at[0], q_send.at[0], q_recv.at[0], me + 1)
    q_up = remote(lat.at[:, :2], LQ.at[1], q_send.at[1], q_recv.at[1], me - 1)
    if_dn(q_dn.start)
    if_up(q_up.start)

    def rows_copies(slot, g, lo, n):
        ss = pl.ds(lo, n)
        down = remote(PB.at[slot - 1, ss], HT.at[slot, ss], dn_send.at[slot, g], ht_recv.at[slot, g], me + 1)
        if slot == end:
            return None, down
        return remote(PT.at[slot - 1, ss], HB.at[slot, ss], up_send.at[slot, g], hb_recv.at[slot, g], me - 1), down

    def out_copy(slot, g, lo, n):
        ss = pl.ds(lo, n)
        return pltpu.make_async_copy(HS.at[ss], hand.at[slot // 2, ss], out_sem.at[slot, g])

    def send_sums(slot, g, lo, n):
        ss = pl.ds(lo, n)
        for k in range(1, sp):
            remote(SG.at[slot, ss], RS.at[slot, k - 1, ss], st_send.at[slot, g], st_recv.at[slot, g], lax.rem(me + k, sp)).start()

    def send_rows(slot, g, lo, n):
        if slot % 2 == 0:
            out_copy(slot, g, lo, n).start()
        if slot > 0:
            up, down = rows_copies(slot, g, lo, n)
            if up is not None:
                if_up(up.start)
            if_dn(down.start)

    def sums_bytes(slot, n, sem, g):
        both = RS.at[slot, :, :n]
        return pltpu.make_async_copy(both, both, sem.at[slot, g])

    def wait_sums(slot, g, n):
        sums_bytes(slot, n, st_recv, g).wait()

    def wait_rows(slot, g, n):
        ss = pl.ds(0, n)
        if_up(lambda: remote(PB.at[0, ss], HT.at[slot, ss], dn_send.at[slot, g], ht_recv.at[slot, g], me).wait_recv())
        if slot is not end:
            if_dn(lambda: remote(PT.at[0, ss], HB.at[slot, ss], up_send.at[slot, g], hb_recv.at[slot, g], me).wait_recv())

    def squeeze(slot, ss, tiles):
        for r, s in zip(compact(tiles, [EMB[slot, pl.ds(s, 1)] for s in ss]), ss):
            SG[slot, s] = r

    if_up(q_dn.wait_recv)
    if_dn(q_up.wait_recv)

    def first(s):
        above, own, below = (x.astype(F32) for x in (LQ[0, s], lat[s], LQ[1, s]))
        rows = [keep_if(has_up, above[k]) for k in DUO] + [own[k] for k in range(ROWS)] + [keep_if(has_dn, below[k]) for k in DUO]
        ext = jnp.concatenate(rows, 1)
        col = lax.broadcasted_iota(jnp.int32, ext.shape, 1) % ROW
        left = jnp.where(col == 0, NIL, pltpu.roll(ext, 1, 1))
        right = jnp.where(col == ROW - 1, NIL, pltpu.roll(ext, ext.shape[1] - 1, 1))
        ext = jnp.concatenate([left, ext, right, jnp.ones_like(ext)], 0)
        mid = pltpu.roll(ext, ext.shape[1] - ROW, 1)
        wide = NP + LANE
        lhs = jnp.concatenate([ext[:, :wide], mid[:, :wide], ext[:, LANE:]], 0).astype(BF)
        r = lax.dot_general(lhs, WI[...].astype(BF), ROWS_DOT, **ACC32)
        acc, acq = no_stats(), no_stats()
        for o in range(ROWS + 2):
            x = r[span(o), :].astype(BF)
            parts = [x[:, span(k, LANE)] for k in TRI]
            if o == 0:
                pack_row(HT.at[0, s], parts)
            elif o > ROWS:
                pack_row(HB.at[0, s], parts)
            else:
                H[s, span(o - 1), :] = x
                HS[s, span(o - 1), :] = x[:, :CH]
                add_stats(acc, acq, parts)
        ST[s] = stats_tile(acc, acq)

    def first_four(i, carry):
        t = SLOTS * i
        for g in TRI:
            pl.when(i == g + 1)(functools.partial(send_rows, 0, g, *EDGES[g]))
        for g in DUO:
            pl.when(i == g + 2)(functools.partial(send_sums, 0, g, *SUMS[g]))
        ss = [lax.rem(t + NS - SLOTS + k, NS) for k in QUAD]
        tiles = [ST[s] for s in ss]
        for k in QUAD:
            first(t + k)
        squeeze(0, ss, tiles)
        return carry

    lax.fori_loop(0, NS // SLOTS, first_four, 0)
    ss = range(NS - SLOTS, NS)
    send_sums(0, 2, *SUMS[2])
    squeeze(0, ss, [ST[s] for s in ss])
    for j in QUAD:
        weight_finish((b1, b2)[j % 2][j // 2:j // 2 + 1, :], W.at[j], WR.at[j], wm_sem.at[j], wr_sem.at[j])
    for g in (3, 4):
        send_sums(0, g, *SUMS[g])
        send_rows(0, g, *EDGES[g])

    def scales(slots, ss):
        tots = []
        for slot, s in zip(slots, ss):
            tots.append(SG[slot, s])
            for k in range(sp - 1):
                tots[-1] = tots[-1] + RS[slot, k, s]
        return affine(tots, [GAIN[pl.ds(k, 1)] for k in slots], [GAIN[pl.ds(k + SLOTS, 1)] for k in slots],
                      [EMB[k, pl.ds(s, 1)] for k, s in zip(slots, ss)], float(sp * NP * GSIZE))

    def prep_of(slot, s, L, a, b):
        def row(r):
            if r == 0:
                return unpack_row(HT.at[slot, s]), has_up
            if r == ROWS + 1:
                return unpack_row(HB.at[slot, s]), has_dn
            return held[slot][s, span(r - 1), :], None
        return prep_gen(row, ROWS, a, b, L)

    def epi_gen(j, s, Y, zero, tiles):
        acc, acq = no_stats(), no_stats()
        edge = {ROWS - 1: PB.at[j, s]}
        if j + 1 < end:
            edge[0] = PT.at[j, s]
        for o in range(ROWS):
            new = [x.astype(BF) for x in conv_row(Y, o, zero)]
            mark = new[2]
            for k in TRI:
                cols = span(k, LANE)
                if j % 2:
                    new[k] = (new[k].astype(F32) + held[j - 1][s, span(o), cols].astype(F32)).astype(BF)
                    cols_out = slice(k * LANE, min(k * LANE + LANE, CH))
                    HS[s, span(o), cols_out] = new[k][:, :cols_out.stop - cols_out.start]
                if j + 1 < end:
                    held[j + 1][s, span(o), cols] = new[k]
            if o in edge:
                pack_row(edge[o], new)
            if j + 1 < end:
                add_stats(acc, acq, new)
            if o == ROWS - 1:
                tiles.append(stats_tile(acc, acq))
            yield mark

    for g in DUO:
        wait_sums(0, g, SUMS[g][1])
    for c, v in enumerate(scales((0,) * 3, TRI)):
        AB[c] = v[:3]
    still = nil(me)
    for _ in prep_of(0, 0, L0, AB[0, :1], AB[1, :1]):
        pass
    for j in QUAD:
        if j % 2:
            for g in range(len(EDGES)):
                out_copy(j - 1, g, *EDGES[g]).wait()

        def body(i, carry, j=j):
            t = 2 * i
            zero = nil(i)
            turn = NS // 2 - 1
            ns = [jnp.minimum(j * NS + t + 3 + k, end * NS - 1) for k in DUO]
            for g in TRI:
                pl.when(i == 2 * g + 1)(functools.partial(wait_sums, j, g + 2, SUMS[g + 2][1]))
            for g in DUO:
                if j + 1 < end:
                    pl.when(i == turn - 1 + g)(functools.partial(wait_sums, j + 1, g, SUMS[g][1]))
            if j > 0:
                for g in TRI:
                    pl.when(i == 2 * g + 1)(functools.partial(wait_rows, j, g + 1, EDGES[g + 1][1]))
                pl.when(i == turn)(functools.partial(wait_rows, j, 4, EDGES[4][1]))
            if j + 1 < end:
                pl.when(i == turn)(functools.partial(wait_rows, j + 1, 0, EDGES[0][1]))
            if j + 1 == end:
                for g, at in enumerate((2, 5, turn)):
                    pl.when(i == at)(functools.partial(send_rows, end, g, *LATE[g]))
            else:
                for parts, send in ((EDGES, send_rows), (SUMS, send_sums)):
                    for g in TRI:
                        pl.when(i == 2 * g + 2)(functools.partial(send, j + 1, g, *parts[g]))
            new = scales([n // NS for n in ns], [lax.rem(n, NS) for n in ns])
            co = [(AB[0, k:k + 1], AB[1, k:k + 1]) for k in (1, 2)]
            tiles = [STC[...]]
            for u, (Lc, Ln, Yc, Yp) in enumerate(((L0, L1, Y0, Y1), (L1, L0, Y1, Y0))):
                nxt = jnp.minimum(t + u + 1, last)
                weave(Lc, W.at[j], Yc, NP, prep_of(j, nxt, Ln, *co[u]), epi_gen(j, lax.rem(t + u + last, NS), Yp, zero, tiles), SHARE)
            for c in DUO:
                AB[c] = jnp.concatenate([co[1][c], new[c][:2]], 0)
            if j + 1 == end:
                return carry
            STC[...] = tiles.pop()
            squeeze(j + 1, [lax.rem(t + last - 1 + k, NS) for k in DUO], tiles)
            return carry

        lax.fori_loop(0, NS // 2, body, 0)
        edges = EDGES if j + 1 < end else LATE
        send_rows(j + 1, 3, *edges[3])
        if j + 1 < end:
            send_sums(j + 1, 3, *SUMS[3])
        tiles = [STC[...]]
        for _ in epi_gen(j, last, Y1, still, tiles):
            pass
        if j + 1 < end:
            for _ in prep_of(j + 1, 0, L0, AB[0, :1], AB[1, :1]):
                pass
            squeeze(j + 1, (last - 1, last), tiles)
            send_sums(j + 1, 4, *SUMS[4])
        send_rows(j + 1, 4, *edges[4])

    fins = []
    for g, (lo, n) in enumerate(LATE):
        wait_rows(end, g, n)
        fins.append(pltpu.make_async_copy(HT.at[end, lo:lo + n], halo.at[lo:lo + n], fin_sem.at[g]))
        fins[-1].start()
    for g in range(len(SUMS)):
        out_copy(end, g, *LATE[g]).wait()
        for slot in QUAD:
            sums_bytes(slot, SUMS[g][1], st_send, g).wait()
            up, down = rows_copies(slot + 1, g, *(EDGES if slot + 1 < end else LATE)[g])
            if up is not None:
                if_up(up.wait_send)
            if_dn(down.wait_send)
    if_dn(q_dn.wait_send)
    if_up(q_up.wait_send)
    for f in fins:
        f.wait()


def tail(hand, halo, bd, dw, h0o, h1o, h2o, do, P0, P1, P2, HA, W, WR, L0, L1, Y0, Y1, OD, DS, in_sem, ha_sem, wm_sem, wr_sem, o_sem, od_sem):
    me = lax.axis_index("sp")
    has_up = (me > 0).astype(jnp.int32)
    held, outs = (P0, P1, P2), (h0o, h1o, h2o)
    ahead = 10

    def take(k, s):
        return pltpu.make_async_copy(hand.at[k, s], held[k].at[s], in_sem.at[k, s])

    def put(k, s):
        return pltpu.make_async_copy(held[k].at[s], outs[k].at[s], o_sem.at[k, s])

    def fetch(s):
        for k in (2, 0, 1):
            take(k, s).start()

    get_halo = pltpu.make_async_copy(halo, HA, ha_sem)
    take(2, 0).start()
    get_halo.start()
    weight_copies(dw, W, WR, wm_sem, wr_sem)
    for k in DUO:
        take(k, 0).start()
    for s in range(1, ahead):
        fetch(s)
    for Y in (Y0, Y1):
        Y[...] = jnp.zeros_like(Y)
    get_halo.wait()
    take(2, 0).wait()
    still = nil(me)

    def row_of(s, r):
        if r == 0:
            return keep_if(has_up, unpack_row(HA.at[s]))
        return widen(P2[s, span(r - 1), :].astype(F32))

    def dprep(s, L):
        for o in QUAD:
            xs = [row_of(s, 2 * o + dy) for dy in TRI]
            for dy in TRI:
                L[span(o), span(dy, MAIN)] = xs[dy][:, :MAIN].astype(BF)
            store_rest(L, o, *(x[:, MAIN:] for x in xs))

    def depi(s, Y, zero):
        for o in QUAD:
            d = conv_row(Y, o, zero)
            for k in TRI:
                DS[o, k] = d[k]
            parts = [DS[o, k, pl.ds(0, ROW // 2, stride=2), :] for k in TRI]
            OD[s, span(o, ROW // 2), :] = jnp.concatenate(parts, 1)[:, :CH].astype(BF)

    def dhalf(t, Lc, Ln, Yc, Yp, zero):
        for n in QUAD:
            dot_chunk(Lc, W, Yc, slice(0, NP // 2), n)
        dprep(jnp.minimum(t + 1, NS - 1), Ln)
        depi(lax.rem(t + NS - 1, NS), Yp, zero)

    dprep(0, L0)
    weight_finish(bd[...].reshape(1, CH), W, WR, wm_sem, wr_sem)

    def dbody(i, carry):
        t = 2 * i
        zero = nil(i)
        for s in (t, t + 1):
            pl.when(s + ahead < NS)(functools.partial(fetch, s + ahead))
            pl.when(s + 1 < NS)(lambda s=s: take(2, s + 1).wait())
            put(2, s).start()
            for k in DUO:
                take(k, s).wait()
                put(k, s).start()
        dhalf(t, L0, L1, Y0, Y1, zero)
        dhalf(t + 1, L1, L0, Y1, Y0, zero)
        return carry

    lax.fori_loop(0, NS // 2, dbody, 0)
    depi(NS - 1, Y1, still)
    dout = pltpu.make_async_copy(OD, do, od_sem)
    dout.start()

    def drain(s, carry):
        for k in TRI:
            put(k, s).wait()
        return carry

    lax.fori_loop(0, NS, drain, 0)
    dout.wait()


def solution(mesh):
    sp = mesh.shape["sp"]

    def program(latent, time_emb, w_in, b_in, gn1_scale, gn1_shift, conv1_w, conv1_b, temb_w, temb_b, gn2_scale, gn2_shift, conv2_w, conv2_b, down_w, down_b):
        dma, vm = pltpu.SemaphoreType.DMA, pltpu.VMEM
        any_, vms = pl.BlockSpec(memory_space=pl.ANY), pl.BlockSpec(memory_space=pltpu.VMEM)
        params = functools.partial(pltpu.CompilerParams, vmem_limit_bytes=66_000_000)

        def big(n=NP, c=CP):
            return vm((NS, n, c), BF)

        def edge(n):
            return vm((n, NS, PK, MAIN), BF)

        def bufs(m):
            return [vm((m, KP), BF)] * 2 + [vm((8, m + 2 * OFF, LANE), F32)] * 2

        def out(*shape):
            return jax.ShapeDtypeStruct(shape, BF)

        hand, halo = pl.pallas_call(
            functools.partial(mega, sp),
            out_shape=(out(3, NS, NP, CH), out(NS, PK, MAIN)),
            in_specs=[vms] * 11 + [any_] * 3, out_specs=(any_, any_),
            scratch_shapes=[big(), big(), big(), big(NP, CH), vm((SLOTS, KP, KP), BF), vm((SLOTS, 9, CH, ROW), BF), vm((2, CH, temb_w.shape[1]), BF), vm((3 * NS, CP), F32)] + bufs(NP)
            + [vm((NS, OFF, LANE), F32), vm((OFF, LANE), F32), vm((SLOTS, NS, 2, LANE), F32), vm((SLOTS, sp - 1, NS, 2, LANE), F32), vm((2, 3, CP), F32), vm((SLOTS, NS, CP), F32), vm((OFF, CP), F32),
               edge(SLOTS + 1), edge(SLOTS), edge(SLOTS - 1), edge(SLOTS), vm((2, NS, 2, 4, ROW), BF),
               dma((SLOTS,)), dma((SLOTS,)), dma] + [dma((2,))] * 2 + [dma((SLOTS + 1, len(SUMS)))] * 7 + [dma((len(SUMS),))],
            compiler_params=params(collective_id=0, has_side_effects=True), name="mega",
        )(latent.transpose(0, 1, 3, 2), w_in, b_in, time_emb, temb_b, gn1_scale, gn1_shift, gn2_scale, gn2_shift, conv1_b, conv2_b, temb_w.transpose(0, 2, 1), conv1_w, conv2_w)
        outs = pl.pallas_call(
            tail,
            out_shape=(out(NS, NP, CH),) * 3 + (out(NS, NP // 4, CH),),
            in_specs=[any_] * 2 + [vms, any_], out_specs=(any_,) * 4,
            scratch_shapes=[big(NP, CH)] * 3 + [big(PK, MAIN), vm((KP, KP), BF), vm((9, CH, ROW), BF)] + bufs(NP // 2)
            + [big(NP // 4, CH), vm((4, 3, ROW, LANE), F32), dma((3, NS)), dma, dma, dma, dma((3, NS)), dma],
            compiler_params=params(), name="tail",
        )(hand, halo, down_b, down_w)
        return tuple(o.reshape(NS, n, m, CH) for o, n, m in zip(outs, [ROWS] * len(TRI) + [ROWS // 2], [ROW] * len(TRI) + [ROW // 2]))

    band = P("dp", "sp", None, None)
    return jax.shard_map(program, mesh=mesh, in_specs=(band, P("dp", None)) + (P(),) * 14, out_specs=(band,) * 4, check_vma=False)
```

```python
import functools

import jax
import jax.numpy as jnp
from jax import lax
from jax.experimental import pallas as pl
from jax.experimental.pallas import tpu as pltpu
from jax.sharding import PartitionSpec as P

F32, BF = jnp.float32, jnp.bfloat16
GN_GROUPS, GN_EPS = 32, 1e-5
NS, ROWS, ROW, LANE, MAIN = 16, 8, 64, 128, 256
NP = ROWS * ROW
CH = 320
CP = CH + ROW
KP = 4 * MAIN
REST = 3 * MAIN
SPARE = 3 * CH
OFF = 8
GSIZE = CH // GN_GROUPS
PK = ROW + NS
MESH = pl.DeviceIdType.MESH
DUO, TRI, QUAD = range(2), range(3), range(4)
SLOTS = len(QUAD)
NIL = 0.0


def groups(n, step):
    cuts = [0, *range(n, NS, step), NS]
    return [(a, b - a) for a, b in zip(cuts, cuts[1:])]


SUMS, EDGES = groups(2, SLOTS), groups(3, SLOTS)
LATE = [(0, 3), (3, 6), (9, 4), (13, 2), (15, 1)]
SHARE = (1, 2, 3, 3)
ACC32 = dict(preferred_element_type=F32)
ROWS_DOT, COLS_DOT = ((((k,), (k,)), ((), ())) for k in DUO)


def nil(i):
    return jnp.minimum(i, 0) * OFF


def span(i, n=ROW, base=0):
    return slice(base + i * n, base + (i + 1) * n)


def low_half():
    return lax.broadcasted_iota(jnp.int32, (ROW, LANE), 1) < ROW


def widen(p):
    return jnp.concatenate([p, p[..., MAIN:]], -1)


def keep_if(flag, x):
    return jnp.where(jnp.full(x.shape, flag, jnp.int32) > 0, x, NIL)


def store_rest(L, o, r0, r1, r2):
    low = low_half()
    L[span(o), REST:REST + LANE] = jnp.where(low, r0, r1).astype(BF)
    L[span(o), REST + LANE:] = jnp.where(low, r2, 1.0).astype(BF)


def prep_gen(x_of_row, nrows, a, b, L):
    ha, hb = a * 0.5, b * 0.5
    rest = []
    for r in range(nrows + 2):
        x, flag = x_of_row(r)
        h = x.astype(F32) * ha + hb
        n = h + h * jnp.tanh(h)
        if flag is not None:
            n = keep_if(flag, n)
        main = n[:, :MAIN].astype(BF)
        rest.append(n[:, MAIN:])
        for dy in TRI:
            if 0 <= r - dy < nrows:
                L[span(r - dy), span(dy, MAIN)] = main
        if r >= 2:
            store_rest(L, r - 2, *rest[r - 2:])
        yield main


def shifted(v, step):
    v = pltpu.roll(v.reshape(OFF, OFF, LANE), step % OFF, 1)
    sub = lax.broadcasted_iota(jnp.int32, v.shape, 1)
    gap = jnp.zeros_like(v[:1])
    if step > 0:
        v = jnp.where(sub == 0, jnp.concatenate([gap, v[:-1]], 0), v)
    else:
        v = jnp.where(sub == OFF - 1, jnp.concatenate([v[1:], gap], 0), v)
    return v.reshape(ROW, LANE)


def conv_row(Y, o, zero):
    def here(k):
        return Y[k, span(o, base=OFF), :]

    out = [shifted(here(k), 1) + here(k + 2) + shifted(here(k + 4), -1) for k in DUO]
    a = here(6)
    mix = jnp.where(low_half(), shifted(a, 1), a)
    return out + [mix + pltpu.roll(mix, ROW, 1) + shifted(here(7), -1)]


def dot_chunk(L, W, Y, rows, n):
    r = jnp.dot(L[rows, :], W[:, span(n, MAIN)], **ACC32)
    for k in DUO:
        Y[2 * n + k, OFF + rows.start:OFF + rows.stop, :] = r[:, span(k, LANE)]


def weave(L, W, Y, m, prep, epi, share):
    work = [prep] * (m // ROW + 2) + [epi] * (m // ROW)
    done = 0
    for n in QUAD:
        dot_chunk(L, W, Y, slice(0, m), n)
        upto = len(work) * share[n] // share[-1]
        for g in work[done:upto]:
            mark = next(g)
        done = upto
        if n < len(QUAD) - 1:
            L[:NS, KP - NS:] = jnp.where(mark[:NS, LANE - NS:LANE].astype(F32) > NIL, 1.0, NIL).astype(BF)
    for g in (prep, epi):
        for _ in g:
            pass


def lane_left(x, k):
    return pltpu.roll(x, CP - k, 1)


def starts(k):
    lane = lax.broadcasted_iota(jnp.int32, (OFF, LANE), 1) + k * LANE
    return (lane % GSIZE == 0) & (lane < CH)


def stacked(rows):
    fill = [jnp.zeros((4 - len(rows), rows[0].shape[1]), F32)] * (len(rows) < 4)
    return jnp.concatenate(list(rows) + fill, 0)


def compact(tiles, embs):
    s = stacked([jnp.concatenate([t[k:k + 1] for k in TRI], 1) for t in tiles])
    q = stacked([jnp.concatenate([t[k + 3:k + 4] for k in TRI], 1) for t in tiles])
    e = stacked(embs)
    x = jnp.concatenate([s + float(NP) * e, q + e * (2.0 * s + float(NP) * e)], 0)
    w2 = x + lane_left(x, 1)
    w4 = w2 + lane_left(w2, 2)
    w8 = w4 + lane_left(w4, 4)
    w10 = w8 + lane_left(w2, 8)
    c = sum(jnp.where(starts(k), w10[:, span(k, LANE)], NIL) for k in TRI)
    return [jnp.concatenate([c[k:k + 1], c[k + 4:k + 5]], 0) for k in range(len(tiles))]


def affine(tots, gains, shifts, embs, count):
    x = jnp.concatenate([stacked([t[k:k + 1] for t in tots]) for k in DUO], 0)
    y = jnp.concatenate([jnp.where(starts(k), x, NIL) for k in TRI], 1)
    r2 = y + pltpu.roll(y, 1, 1)
    r4 = r2 + pltpu.roll(r2, 2, 1)
    r8 = r4 + pltpu.roll(r4, 4, 1)
    r = r8 + pltpu.roll(r2, 8, 1)
    lane = lax.broadcasted_iota(jnp.int32, (OFF, CP), 1)
    r = jnp.where(lane >= CH, pltpu.roll(r, ROW, 1), r) * (1.0 / count)
    mean, msq = r[:4], r[4:]
    a = stacked(gains) * lax.rsqrt(msq - mean * mean + GN_EPS)
    return a, stacked(shifts) + a * (stacked(embs) - mean)


def pack_row(dst, x):
    dst[:ROW, :] = jnp.concatenate(x[:2], 1)
    half = ROW // 2
    p = jnp.where(low_half()[:half], x[2][:half].astype(F32), x[2][half:].astype(F32))
    dst[ROW:, :] = jnp.concatenate([p[:NS], p[NS:]], 1).astype(BF)


def unpack_row(src):
    p = src[ROW:, :].astype(F32)
    p = jnp.concatenate([p[:, :LANE], p[:, LANE:]], 0)
    swap, low = pltpu.roll(p, ROW, 1), low_half()[:ROW // 2]
    rest = jnp.concatenate([jnp.where(low, p, swap), jnp.where(low, swap, p)], 0)
    return jnp.concatenate([src[:ROW, :].astype(F32), rest], 1)


def stats_tile(acc, acq):
    parts = [x.sum(0, keepdims=True) for x in acc + acq]
    return jnp.concatenate(parts + [jnp.zeros((2, LANE), F32)], 0)


def add_stats(acc, acq, new):
    for k, x in enumerate(new):
        v = x.astype(F32).reshape(OFF, OFF, LANE)
        acc[k] = acc[k] + v.sum(0)
        acq[k] = acq[k] + (v * v).sum(0)


def no_stats():
    return [jnp.zeros((OFF, LANE), F32) for _ in TRI]


def weight_copies(src, W, WR, sem_main, sem_rest):
    for dy in TRI:
        for dx in TRI:
            cols = span(dx, MAIN)
            pltpu.make_async_copy(src.at[dy, dx, :MAIN, :MAIN], W.at[span(dy, MAIN), cols], sem_main).start()
            pltpu.make_async_copy(src.at[dy, dx, MAIN:, :MAIN], W.at[span(dy, base=REST), cols], sem_main).start()
            pltpu.make_async_copy(src.at[dy, dx, :, MAIN:], WR.at[dy * 3 + dx], sem_rest).start()


def weight_finish(bias, W, WR, sem_main, sem_rest):
    main = W.at[:SPARE, :REST]
    pltpu.make_async_copy(main, main, sem_main).wait()
    pltpu.make_async_copy(WR, WR, sem_rest).wait()
    for dy in TRI:
        for part, rows in ((slice(0, MAIN), span(dy, MAIN)), (slice(MAIN, CH), span(dy, base=REST))):
            w0, w1, w2 = (WR[dy * 3 + dx, part, :] for dx in TRI)
            W[rows, REST:REST + LANE] = jnp.concatenate([w0, w1], 1)
            W[rows, REST + LANE:] = jnp.concatenate([w2, w2], 1)
    b = widen(bias.astype(F32))
    gap = jnp.zeros((1, MAIN), F32)
    rest = jnp.where(low_half()[:1], 0.0, b[:, MAIN:])
    row = jnp.concatenate([gap, b[:, :MAIN], gap, rest, gap[:, :LANE]], 1)
    first = lax.broadcasted_iota(jnp.int32, (ROW, KP), 0) == 0
    W[SPARE:, :] = jnp.where(first, row, NIL).astype(BF)


def mega(sp, lat, wi, bi, temb, tb, g1, s1, g2, s2, b1, b2, tw, w1, w2, hand, halo,
         H, U, H2, HS, W, WR, TW, WI, L0, L1, Y0, Y1, ST, STC, SG, RS, AB, EMB, GAIN, HT, HB, PT, PB, LQ,
         wm_sem, wr_sem, tw_sem, q_send, q_recv, st_send, st_recv, up_send, dn_send, ht_recv, hb_recv, out_sem, fin_sem):
    me, dp = lax.axis_index("sp"), lax.axis_index("dp")
    has_up, has_dn = (me > 0).astype(jnp.int32), (me < sp - 1).astype(jnp.int32)
    held = (H, U, H2, U)
    end = SLOTS
    last = NS - 1

    get_tw = pltpu.make_async_copy(tw, TW, tw_sem)
    get_tw.start()
    for j, src in enumerate((w1.at[0], w2.at[0], w1.at[1], w2.at[1])):
        weight_copies(src, W.at[j], WR.at[j], wm_sem.at[j], wr_sem.at[j])

    barrier = pltpu.get_barrier_semaphore()
    for k in range(1, sp):
        pl.semaphore_signal(barrier, inc=1, device_id=(dp, lax.rem(me + k, sp)), device_id_type=MESH)
    for k, (ref, l) in enumerate((ref, l) for pair in ((g1, g2), (s1, s2)) for l in DUO for ref in pair):
        GAIN[k:k + 1, :] = widen(ref[l:l + 1, :].astype(F32))
    WI[...] = jnp.zeros_like(WI)
    for dy in TRI:
        for dx in TRI:
            WI[span(4 * dy + dx, 4), :] = widen(wi[dy, dx].astype(F32))
    WI[NS + 12:NS + 13, :] = widen(bi[...].reshape(1, CH).astype(F32))
    get_tw.wait()
    x = temb[...].astype(F32)
    act = (x * jax.nn.sigmoid(x)).astype(BF)
    for l in DUO:
        pr = lax.dot_general(act, TW[l], COLS_DOT, **ACC32)
        EMB[2 * l] = jnp.zeros((NS, CP), F32)
        EMB[2 * l + 1] = widen(pr + tb[l:l + 1, :].astype(F32))
    for Y in (Y0, Y1):
        Y[...] = jnp.zeros_like(Y)
    pl.semaphore_wait(barrier, sp - 1)

    def remote(src, dst, ssem, rsem, dev):
        return pltpu.make_async_remote_copy(src_ref=src, dst_ref=dst, send_sem=ssem, recv_sem=rsem, device_id=(dp, dev), device_id_type=MESH)

    def if_up(f):
        pl.when(me > 0)(f)

    def if_dn(f):
        pl.when(me < sp - 1)(f)

    q_dn = remote(lat.at[:, ROWS - 2:], LQ.at[0], q_send.at[0], q_recv.at[0], me + 1)
    q_up = remote(lat.at[:, :2], LQ.at[1], q_send.at[1], q_recv.at[1], me - 1)
    if_dn(q_dn.start)
    if_up(q_up.start)

    def rows_copies(slot, g, lo, n):
        ss = pl.ds(lo, n)
        down = remote(PB.at[slot - 1, ss], HT.at[slot, ss], dn_send.at[slot, g], ht_recv.at[slot, g], me + 1)
        if slot == end:
            return None, down
        return remote(PT.at[slot - 1, ss], HB.at[slot, ss], up_send.at[slot, g], hb_recv.at[slot, g], me - 1), down

    def out_copy(slot, g, lo, n):
        ss = pl.ds(lo, n)
        return pltpu.make_async_copy(HS.at[ss], hand.at[slot // 2, ss], out_sem.at[slot, g])

    def send_sums(slot, g, lo, n):
        ss = pl.ds(lo, n)
        for k in range(1, sp):
            remote(SG.at[slot, ss], RS.at[slot, k - 1, ss], st_send.at[slot, g], st_recv.at[slot, g], lax.rem(me + k, sp)).start()

    def send_rows(slot, g, lo, n):
        if slot % 2 == 0:
            out_copy(slot, g, lo, n).start()
        if slot > 0:
            up, down = rows_copies(slot, g, lo, n)
            if up is not None:
                if_up(up.start)
            if_dn(down.start)

    def sums_bytes(slot, n, sem, g):
        both = RS.at[slot, :, :n]
        return pltpu.make_async_copy(both, both, sem.at[slot, g])

    def wait_sums(slot, g, n):
        sums_bytes(slot, n, st_recv, g).wait()

    def wait_rows(slot, g, n):
        ss = pl.ds(0, n)
        if_up(lambda: remote(PB.at[0, ss], HT.at[slot, ss], dn_send.at[slot, g], ht_recv.at[slot, g], me).wait_recv())
        if slot is not end:
            if_dn(lambda: remote(PT.at[0, ss], HB.at[slot, ss], up_send.at[slot, g], hb_recv.at[slot, g], me).wait_recv())

    def squeeze(slot, ss, tiles):
        for r, s in zip(compact(tiles, [EMB[slot, pl.ds(s, 1)] for s in ss]), ss):
            SG[slot, s] = r

    if_up(q_dn.wait_recv)
    if_dn(q_up.wait_recv)

    def first(s):
        above, own, below = (x.astype(F32) for x in (LQ[0, s], lat[s], LQ[1, s]))
        rows = [keep_if(has_up, above[k]) for k in DUO] + [own[k] for k in range(ROWS)] + [keep_if(has_dn, below[k]) for k in DUO]
        ext = jnp.concatenate(rows, 1)
        col = lax.broadcasted_iota(jnp.int32, ext.shape, 1) % ROW
        left = jnp.where(col == 0, NIL, pltpu.roll(ext, 1, 1))
        right = jnp.where(col == ROW - 1, NIL, pltpu.roll(ext, ext.shape[1] - 1, 1))
        ext = jnp.concatenate([left, ext, right, jnp.ones_like(ext)], 0)
        mid = pltpu.roll(ext, ext.shape[1] - ROW, 1)
        wide = NP + LANE
        lhs = jnp.concatenate([ext[:, :wide], mid[:, :wide], ext[:, LANE:]], 0).astype(BF)
        r = lax.dot_general(lhs, WI[...].astype(BF), ROWS_DOT, **ACC32)
        acc, acq = no_stats(), no_stats()
        for o in range(ROWS + 2):
            x = r[span(o), :].astype(BF)
            parts = [x[:, span(k, LANE)] for k in TRI]
            if o == 0:
                pack_row(HT.at[0, s], parts)
            elif o > ROWS:
                pack_row(HB.at[0, s], parts)
            else:
                H[s, span(o - 1), :] = x
                HS[s, span(o - 1), :] = x[:, :CH]
                add_stats(acc, acq, parts)
        ST[s] = stats_tile(acc, acq)

    def first_four(i, carry):
        t = SLOTS * i
        for g in TRI:
            pl.when(i == g + 1)(functools.partial(send_rows, 0, g, *EDGES[g]))
        for g in DUO:
            pl.when(i == g + 2)(functools.partial(send_sums, 0, g, *SUMS[g]))
        ss = [lax.rem(t + NS - SLOTS + k, NS) for k in QUAD]
        tiles = [ST[s] for s in ss]
        for k in QUAD:
            first(t + k)
        squeeze(0, ss, tiles)
        return carry

    lax.fori_loop(0, NS // SLOTS, first_four, 0)
    ss = range(NS - SLOTS, NS)
    send_sums(0, 2, *SUMS[2])
    squeeze(0, ss, [ST[s] for s in ss])
    for j in QUAD:
        weight_finish((b1, b2)[j % 2][j // 2:j // 2 + 1, :], W.at[j], WR.at[j], wm_sem.at[j], wr_sem.at[j])
    for g in (3, 4):
        send_sums(0, g, *SUMS[g])
        send_rows(0, g, *EDGES[g])

    def scales(slots, ss):
        tots = []
        for slot, s in zip(slots, ss):
            tots.append(SG[slot, s])
            for k in range(sp - 1):
                tots[-1] = tots[-1] + RS[slot, k, s]
        return affine(tots, [GAIN[pl.ds(k, 1)] for k in slots], [GAIN[pl.ds(k + SLOTS, 1)] for k in slots],
                      [EMB[k, pl.ds(s, 1)] for k, s in zip(slots, ss)], float(sp * NP * GSIZE))

    def prep_of(slot, s, L, a, b):
        def row(r):
            if r == 0:
                return unpack_row(HT.at[slot, s]), has_up
            if r == ROWS + 1:
                return unpack_row(HB.at[slot, s]), has_dn
            return held[slot][s, span(r - 1), :], None
        return prep_gen(row, ROWS, a, b, L)

    def epi_gen(j, s, Y, zero, tiles):
        acc, acq = no_stats(), no_stats()
        edge = {ROWS - 1: PB.at[j, s]}
        if j + 1 < end:
            edge[0] = PT.at[j, s]
        for o in range(ROWS):
            new = [x.astype(BF) for x in conv_row(Y, o, zero)]
            mark = new[2]
            for k in TRI:
                cols = span(k, LANE)
                if j % 2:
                    new[k] = (new[k].astype(F32) + held[j - 1][s, span(o), cols].astype(F32)).astype(BF)
                    cols_out = slice(k * LANE, min(k * LANE + LANE, CH))
                    HS[s, span(o), cols_out] = new[k][:, :cols_out.stop - cols_out.start]
                if j + 1 < end:
                    held[j + 1][s, span(o), cols] = new[k]
            if o in edge:
                pack_row(edge[o], new)
            if j + 1 < end:
                add_stats(acc, acq, new)
            if o == ROWS - 1:
                tiles.append(stats_tile(acc, acq))
            yield mark

    for g in DUO:
        wait_sums(0, g, SUMS[g][1])
    for c, v in enumerate(scales((0,) * 3, TRI)):
        AB[c] = v[:3]
    still = nil(me)
    for _ in prep_of(0, 0, L0, AB[0, :1], AB[1, :1]):
        pass
    for j in QUAD:
        if j % 2:
            for g in range(len(EDGES)):
                out_copy(j - 1, g, *EDGES[g]).wait()

        def body(i, carry, j=j):
            t = 2 * i
            zero = nil(i)
            turn = NS // 2 - 1
            ns = [jnp.minimum(j * NS + t + 3 + k, end * NS - 1) for k in DUO]
            for g in TRI:
                pl.when(i == 2 * g + 1)(functools.partial(wait_sums, j, g + 2, SUMS[g + 2][1]))
            for g in DUO:
                if j + 1 < end:
                    pl.when(i == turn - 1 + g)(functools.partial(wait_sums, j + 1, g, SUMS[g][1]))
            if j > 0:
                for g in TRI:
                    pl.when(i == 2 * g + 1)(functools.partial(wait_rows, j, g + 1, EDGES[g + 1][1]))
                pl.when(i == turn)(functools.partial(wait_rows, j, 4, EDGES[4][1]))
            if j + 1 < end:
                pl.when(i == turn)(functools.partial(wait_rows, j + 1, 0, EDGES[0][1]))
            if j + 1 == end:
                for g, at in enumerate((2, 5, turn)):
                    pl.when(i == at)(functools.partial(send_rows, end, g, *LATE[g]))
            else:
                for parts, send in ((EDGES, send_rows), (SUMS, send_sums)):
                    for g in TRI:
                        pl.when(i == 2 * g + 2)(functools.partial(send, j + 1, g, *parts[g]))
            new = scales([n // NS for n in ns], [lax.rem(n, NS) for n in ns])
            co = [(AB[0, k:k + 1], AB[1, k:k + 1]) for k in (1, 2)]
            tiles = [STC[...]]
            for u, (Lc, Ln, Yc, Yp) in enumerate(((L0, L1, Y0, Y1), (L1, L0, Y1, Y0))):
                nxt = jnp.minimum(t + u + 1, last)
                weave(Lc, W.at[j], Yc, NP, prep_of(j, nxt, Ln, *co[u]), epi_gen(j, lax.rem(t + u + last, NS), Yp, zero, tiles), SHARE)
            for c in DUO:
                AB[c] = jnp.concatenate([co[1][c], new[c][:2]], 0)
            if j + 1 == end:
                return carry
            STC[...] = tiles.pop()
            squeeze(j + 1, [lax.rem(t + last - 1 + k, NS) for k in DUO], tiles)
            return carry

        lax.fori_loop(0, NS // 2, body, 0)
        edges = EDGES if j + 1 < end else LATE
        send_rows(j + 1, 3, *edges[3])
        if j + 1 < end:
            send_sums(j + 1, 3, *SUMS[3])
        tiles = [STC[...]]
        for _ in epi_gen(j, last, Y1, still, tiles):
            pass
        if j + 1 < end:
            for _ in prep_of(j + 1, 0, L0, AB[0, :1], AB[1, :1]):
                pass
            squeeze(j + 1, (last - 1, last), tiles)
            send_sums(j + 1, 4, *SUMS[4])
        send_rows(j + 1, 4, *edges[4])

    fins = []
    for g, (lo, n) in enumerate(LATE):
        wait_rows(end, g, n)
        fins.append(pltpu.make_async_copy(HT.at[end, lo:lo + n], halo.at[lo:lo + n], fin_sem.at[g]))
        fins[-1].start()
    for g in range(len(SUMS)):
        out_copy(end, g, *LATE[g]).wait()
        for slot in QUAD:
            sums_bytes(slot, SUMS[g][1], st_send, g).wait()
            up, down = rows_copies(slot + 1, g, *(EDGES if slot + 1 < end else LATE)[g])
            if up is not None:
                if_up(up.wait_send)
            if_dn(down.wait_send)
    if_dn(q_dn.wait_send)
    if_up(q_up.wait_send)
    for f in fins:
        f.wait()


def tail(hand, halo, bd, dw, h0o, h1o, h2o, do, P0, P1, P2, HA, W, WR, L0, L1, Y0, Y1, OD, DS, in_sem, ha_sem, wm_sem, wr_sem, o_sem, od_sem):
    me = lax.axis_index("sp")
    has_up = (me > 0).astype(jnp.int32)
    held, outs = (P0, P1, P2), (h0o, h1o, h2o)
    ahead = 6

    def take(k, s):
        return pltpu.make_async_copy(hand.at[k, s], held[k].at[s], in_sem.at[k, s])

    def put(k, s):
        return pltpu.make_async_copy(held[k].at[s], outs[k].at[s], o_sem.at[k, s])

    def fetch(s):
        for k in (2, 0, 1):
            take(k, s).start()

    get_halo = pltpu.make_async_copy(halo, HA, ha_sem)
    take(2, 0).start()
    get_halo.start()
    weight_copies(dw, W, WR, wm_sem, wr_sem)
    for k in DUO:
        take(k, 0).start()
    for s in range(1, ahead):
        fetch(s)
    for Y in (Y0, Y1):
        Y[...] = jnp.zeros_like(Y)
    def pass_on(s):
        for k in DUO:
            take(k, s).wait()
            put(k, s).start()

    def dput(s):
        return pltpu.make_async_copy(OD.at[s], do.at[s], od_sem.at[s])

    get_halo.wait()
    take(2, 0).wait()
    still = nil(me)

    def row_of(s, r):
        if r == 0:
            return keep_if(has_up, unpack_row(HA.at[s]))
        return widen(P2[s, span(r - 1), :].astype(F32))

    def dprep(s, L):
        for o in QUAD:
            xs = [row_of(s, 2 * o + dy) for dy in TRI]
            for dy in TRI:
                L[span(o), span(dy, MAIN)] = xs[dy][:, :MAIN].astype(BF)
            store_rest(L, o, *(x[:, MAIN:] for x in xs))

    def depi(s, Y, zero):
        for o in QUAD:
            d = conv_row(Y, o, zero)
            for k in TRI:
                DS[o, k] = d[k]
            parts = [DS[o, k, pl.ds(0, ROW // 2, stride=2), :] for k in TRI]
            OD[s, span(o, ROW // 2), :] = jnp.concatenate(parts, 1)[:, :CH].astype(BF)

    def dhalf(t, Lc, Ln, Yc, Yp, zero):
        for n in QUAD:
            dot_chunk(Lc, W, Yc, slice(0, NP // 2), n)
        dprep(jnp.minimum(t + 1, NS - 1), Ln)
        depi(lax.rem(t + NS - 1, NS), Yp, zero)

    dprep(0, L0)
    for s in DUO:
        pass_on(s)
    weight_finish(bd[...].reshape(1, CH), W, WR, wm_sem, wr_sem)

    def dbody(i, carry):
        t = 2 * i
        zero = nil(i)
        for s in (t, t + 1):
            pl.when(s + ahead < NS)(functools.partial(fetch, s + ahead))
            pl.when(s + 1 < NS)(lambda s=s: take(2, s + 1).wait())
            put(2, s).start()
            pl.when(s + 2 < NS)(functools.partial(pass_on, s + 2))
            pl.when(s > 2)(lambda s=s: dput(s - 3).start())
        dhalf(t, L0, L1, Y0, Y1, zero)
        dhalf(t + 1, L1, L0, Y1, Y0, zero)
        return carry

    lax.fori_loop(0, NS // 2, dbody, 0)
    depi(NS - 1, Y1, still)
    for s in range(NS - 3, NS):
        dput(s).start()

    def drain(s, carry):
        for k in TRI:
            put(k, s).wait()
        dput(s).wait()
        return carry

    lax.fori_loop(0, NS, drain, 0)


def solution(mesh):
    sp = mesh.shape["sp"]

    def program(latent, time_emb, w_in, b_in, gn1_scale, gn1_shift, conv1_w, conv1_b, temb_w, temb_b, gn2_scale, gn2_shift, conv2_w, conv2_b, down_w, down_b):
        dma, vm = pltpu.SemaphoreType.DMA, pltpu.VMEM
        any_, vms = pl.BlockSpec(memory_space=pl.ANY), pl.BlockSpec(memory_space=pltpu.VMEM)
        params = functools.partial(pltpu.CompilerParams, vmem_limit_bytes=66_000_000)

        def big(n=NP, c=CP):
            return vm((NS, n, c), BF)

        def edge(n):
            return vm((n, NS, PK, MAIN), BF)

        def bufs(m):
            return [vm((m, KP), BF)] * 2 + [vm((8, m + 2 * OFF, LANE), F32)] * 2

        def out(*shape):
            return jax.ShapeDtypeStruct(shape, BF)

        hand, halo = pl.pallas_call(
            functools.partial(mega, sp),
            out_shape=(out(3, NS, NP, CH), out(NS, PK, MAIN)),
            in_specs=[vms] * 11 + [any_] * 3, out_specs=(any_, any_),
            scratch_shapes=[big(), big(), big(), big(NP, CH), vm((SLOTS, KP, KP), BF), vm((SLOTS, 9, CH, ROW), BF), vm((2, CH, temb_w.shape[1]), BF), vm((3 * NS, CP), F32)] + bufs(NP)
            + [vm((NS, OFF, LANE), F32), vm((OFF, LANE), F32), vm((SLOTS, NS, 2, LANE), F32), vm((SLOTS, sp - 1, NS, 2, LANE), F32), vm((2, 3, CP), F32), vm((SLOTS, NS, CP), F32), vm((OFF, CP), F32),
               edge(SLOTS + 1), edge(SLOTS), edge(SLOTS - 1), edge(SLOTS), vm((2, NS, 2, 4, ROW), BF),
               dma((SLOTS,)), dma((SLOTS,)), dma] + [dma((2,))] * 2 + [dma((SLOTS + 1, len(SUMS)))] * 7 + [dma((len(SUMS),))],
            compiler_params=params(collective_id=0, has_side_effects=True), name="mega",
        )(latent.transpose(0, 1, 3, 2), w_in, b_in, time_emb, temb_b, gn1_scale, gn1_shift, gn2_scale, gn2_shift, conv1_b, conv2_b, temb_w.transpose(0, 2, 1), conv1_w, conv2_w)
        outs = pl.pallas_call(
            tail,
            out_shape=(out(NS, NP, CH),) * 3 + (out(NS, NP // 4, CH),),
            in_specs=[any_] * 2 + [vms, any_], out_specs=(any_,) * 4,
            scratch_shapes=[big(NP, CH)] * 3 + [big(PK, MAIN), vm((KP, KP), BF), vm((9, CH, ROW), BF)] + bufs(NP // 2)
            + [big(NP // 4, CH), vm((4, 3, ROW, LANE), F32), dma((3, NS)), dma, dma, dma, dma((3, NS)), dma((NS,))],
            compiler_params=params(), name="tail",
        )(hand, halo, down_b, down_w)
        return tuple(o.reshape(NS, n, m, CH) for o, n, m in zip(outs, [ROWS] * len(TRI) + [ROWS // 2], [ROW] * len(TRI) + [ROW // 2]))

    band = P("dp", "sp", None, None)
    return jax.shard_map(program, mesh=mesh, in_specs=(band, P("dp", None)) + (P(),) * 14, out_specs=(band,) * 4, check_vma=False)
```

```python
import functools

import jax
import jax.numpy as jnp
from jax import lax
from jax.experimental import pallas as pl
from jax.experimental.pallas import tpu as pltpu
from jax.sharding import PartitionSpec as P

F32, BF = jnp.float32, jnp.bfloat16
GN_GROUPS, GN_EPS = 32, 1e-5
NS, ROWS, ROW, LANE, MAIN = 16, 8, 64, 128, 256
NP = ROWS * ROW
CH = 320
CP = CH + ROW
KP = 4 * MAIN
REST = 3 * MAIN
SPARE = 3 * CH
OFF = 8
GSIZE = CH // GN_GROUPS
PK = ROW + NS
MESH = pl.DeviceIdType.MESH
DUO, TRI, QUAD = range(2), range(3), range(4)
SLOTS = len(QUAD)
NIL = 0.0


def groups(n, step):
    cuts = [0, *range(n, NS, step), NS]
    return [(a, b - a) for a, b in zip(cuts, cuts[1:])]


SUMS, EDGES = groups(2, SLOTS), groups(3, SLOTS)
LATE = [(0, 3), (3, 6), (9, 4), (13, 2), (15, 1)]
SHARE = (1, 2, 3, 3)
ACC32 = dict(preferred_element_type=F32)
ROWS_DOT, COLS_DOT = ((((k,), (k,)), ((), ())) for k in DUO)


def nil(i):
    return jnp.minimum(i, 0) * OFF


def span(i, n=ROW, base=0):
    return slice(base + i * n, base + (i + 1) * n)


def low_half():
    return lax.broadcasted_iota(jnp.int32, (ROW, LANE), 1) < ROW


def widen(p):
    return jnp.concatenate([p, p[..., MAIN:]], -1)


def keep_if(flag, x):
    return jnp.where(jnp.full(x.shape, flag, jnp.int32) > 0, x, NIL)


def store_rest(L, o, r0, r1, r2):
    low = low_half()
    L[span(o), REST:REST + LANE] = jnp.where(low, r0, r1).astype(BF)
    L[span(o), REST + LANE:] = jnp.where(low, r2, 1.0).astype(BF)


def prep_gen(x_of_row, nrows, a, b, L):
    ha, hb = a * 0.5, b * 0.5
    rest = []
    for r in range(nrows + 2):
        x, flag = x_of_row(r)
        h = x.astype(F32) * ha + hb
        n = h + h * jnp.tanh(h)
        if flag is not None:
            n = keep_if(flag, n)
        main = n[:, :MAIN].astype(BF)
        rest.append(n[:, MAIN:])
        for dy in TRI:
            if 0 <= r - dy < nrows:
                L[span(r - dy), span(dy, MAIN)] = main
        if r >= 2:
            store_rest(L, r - 2, *rest[r - 2:])
        yield main


def shifted(v, step):
    v = pltpu.roll(v.reshape(OFF, OFF, LANE), step % OFF, 1)
    sub = lax.broadcasted_iota(jnp.int32, v.shape, 1)
    gap = jnp.zeros_like(v[:1])
    if step > 0:
        v = jnp.where(sub == 0, jnp.concatenate([gap, v[:-1]], 0), v)
    else:
        v = jnp.where(sub == OFF - 1, jnp.concatenate([v[1:], gap], 0), v)
    return v.reshape(ROW, LANE)


def conv_row(Y, o, zero):
    def here(k):
        return Y[k, span(o, base=OFF), :]

    out = [shifted(here(k), 1) + here(k + 2) + shifted(here(k + 4), -1) for k in DUO]
    a = here(6)
    mix = jnp.where(low_half(), shifted(a, 1), a)
    return out + [mix + pltpu.roll(mix, ROW, 1) + shifted(here(7), -1)]


def dot_chunk(L, W, Y, rows, n):
    r = jnp.dot(L[rows, :], W[:, span(n, MAIN)], **ACC32)
    for k in DUO:
        Y[2 * n + k, OFF + rows.start:OFF + rows.stop, :] = r[:, span(k, LANE)]


def weave(L, W, Y, m, prep, epi, share):
    work = [prep] * (m // ROW + 2) + [epi] * (m // ROW)
    done = 0
    for n in QUAD:
        dot_chunk(L, W, Y, slice(0, m), n)
        upto = len(work) * share[n] // share[-1]
        for g in work[done:upto]:
            mark = next(g)
        done = upto
        if n < len(QUAD) - 1:
            L[:NS, KP - NS:] = jnp.where(mark[:NS, LANE - NS:LANE].astype(F32) > NIL, 1.0, NIL).astype(BF)
    for g in (prep, epi):
        for _ in g:
            pass


def lane_left(x, k):
    return pltpu.roll(x, CP - k, 1)


def starts(k):
    lane = lax.broadcasted_iota(jnp.int32, (OFF, LANE), 1) + k * LANE
    return (lane % GSIZE == 0) & (lane < CH)


def stacked(rows):
    fill = [jnp.zeros((4 - len(rows), rows[0].shape[1]), F32)] * (len(rows) < 4)
    return jnp.concatenate(list(rows) + fill, 0)


def compact(tiles, embs):
    s = stacked([jnp.concatenate([t[k:k + 1] for k in TRI], 1) for t in tiles])
    q = stacked([jnp.concatenate([t[k + 3:k + 4] for k in TRI], 1) for t in tiles])
    e = stacked(embs)
    x = jnp.concatenate([s + float(NP) * e, q + e * (2.0 * s + float(NP) * e)], 0)
    w2 = x + lane_left(x, 1)
    w4 = w2 + lane_left(w2, 2)
    w8 = w4 + lane_left(w4, 4)
    w10 = w8 + lane_left(w2, 8)
    c = sum(jnp.where(starts(k), w10[:, span(k, LANE)], NIL) for k in TRI)
    return [jnp.concatenate([c[k:k + 1], c[k + 4:k + 5]], 0) for k in range(len(tiles))]


def affine(tots, gains, shifts, embs, count):
    x = jnp.concatenate([stacked([t[k:k + 1] for t in tots]) for k in DUO], 0)
    y = jnp.concatenate([jnp.where(starts(k), x, NIL) for k in TRI], 1)
    r2 = y + pltpu.roll(y, 1, 1)
    r4 = r2 + pltpu.roll(r2, 2, 1)
    r8 = r4 + pltpu.roll(r4, 4, 1)
    r = r8 + pltpu.roll(r2, 8, 1)
    lane = lax.broadcasted_iota(jnp.int32, (OFF, CP), 1)
    r = jnp.where(lane >= CH, pltpu.roll(r, ROW, 1), r) * (1.0 / count)
    mean, msq = r[:4], r[4:]
    a = stacked(gains) * lax.rsqrt(msq - mean * mean + GN_EPS)
    return a, stacked(shifts) + a * (stacked(embs) - mean)


def pack_row(dst, x):
    dst[:ROW, :] = jnp.concatenate(x[:2], 1)
    half = ROW // 2
    p = jnp.where(low_half()[:half], x[2][:half].astype(F32), x[2][half:].astype(F32))
    dst[ROW:, :] = jnp.concatenate([p[:NS], p[NS:]], 1).astype(BF)


def unpack_row(src):
    p = src[ROW:, :].astype(F32)
    p = jnp.concatenate([p[:, :LANE], p[:, LANE:]], 0)
    swap, low = pltpu.roll(p, ROW, 1), low_half()[:ROW // 2]
    rest = jnp.concatenate([jnp.where(low, p, swap), jnp.where(low, swap, p)], 0)
    return jnp.concatenate([src[:ROW, :].astype(F32), rest], 1)


def stats_tile(acc, acq):
    parts = [x.sum(0, keepdims=True) for x in acc + acq]
    return jnp.concatenate(parts + [jnp.zeros((2, LANE), F32)], 0)


def add_stats(acc, acq, new):
    for k, x in enumerate(new):
        v = x.astype(F32).reshape(OFF, OFF, LANE)
        acc[k] = acc[k] + v.sum(0)
        acq[k] = acq[k] + (v * v).sum(0)


def no_stats():
    return [jnp.zeros((OFF, LANE), F32) for _ in TRI]


def weight_copies(src, W, WR, sem_main, sem_rest):
    for dy in TRI:
        for dx in TRI:
            cols = span(dx, MAIN)
            pltpu.make_async_copy(src.at[dy, dx, :MAIN, :MAIN], W.at[span(dy, MAIN), cols], sem_main).start()
            pltpu.make_async_copy(src.at[dy, dx, MAIN:, :MAIN], W.at[span(dy, base=REST), cols], sem_main).start()
            pltpu.make_async_copy(src.at[dy, dx, :, MAIN:], WR.at[dy * 3 + dx], sem_rest).start()


def weight_finish(bias, W, WR, sem_main, sem_rest):
    main = W.at[:SPARE, :REST]
    pltpu.make_async_copy(main, main, sem_main).wait()
    pltpu.make_async_copy(WR, WR, sem_rest).wait()
    for dy in TRI:
        for part, rows in ((slice(0, MAIN), span(dy, MAIN)), (slice(MAIN, CH), span(dy, base=REST))):
            w0, w1, w2 = (WR[dy * 3 + dx, part, :] for dx in TRI)
            W[rows, REST:REST + LANE] = jnp.concatenate([w0, w1], 1)
            W[rows, REST + LANE:] = jnp.concatenate([w2, w2], 1)
    b = widen(bias.astype(F32))
    gap = jnp.zeros((1, MAIN), F32)
    rest = jnp.where(low_half()[:1], 0.0, b[:, MAIN:])
    row = jnp.concatenate([gap, b[:, :MAIN], gap, rest, gap[:, :LANE]], 1)
    first = lax.broadcasted_iota(jnp.int32, (ROW, KP), 0) == 0
    W[SPARE:, :] = jnp.where(first, row, NIL).astype(BF)


def mega(sp, lat, wi, bi, temb, tb, g1, s1, g2, s2, b1, b2, tw, w1, w2, hand, halo,
         H, U, H2, HS, W, WR, TW, WI, L0, L1, Y0, Y1, ST, STC, SG, RS, AB, EMB, GAIN, HT, HB, PT, PB, LQ,
         wm_sem, wr_sem, tw_sem, q_send, q_recv, st_send, st_recv, up_send, dn_send, ht_recv, hb_recv, out_sem, fin_sem):
    me, dp = lax.axis_index("sp"), lax.axis_index("dp")
    has_up, has_dn = (me > 0).astype(jnp.int32), (me < sp - 1).astype(jnp.int32)
    held = (H, U, H2, U)
    end = SLOTS
    last = NS - 1

    get_tw = pltpu.make_async_copy(tw, TW, tw_sem)
    get_tw.start()
    for j, src in enumerate((w1.at[0], w2.at[0], w1.at[1], w2.at[1])):
        weight_copies(src, W.at[j], WR.at[j], wm_sem.at[j], wr_sem.at[j])

    barrier = pltpu.get_barrier_semaphore()
    for k in range(1, sp):
        pl.semaphore_signal(barrier, inc=1, device_id=(dp, lax.rem(me + k, sp)), device_id_type=MESH)
    for k, (ref, l) in enumerate((ref, l) for pair in ((g1, g2), (s1, s2)) for l in DUO for ref in pair):
        GAIN[k:k + 1, :] = widen(ref[l:l + 1, :].astype(F32))
    WI[...] = jnp.zeros_like(WI)
    for dy in TRI:
        for dx in TRI:
            WI[span(4 * dy + dx, 4), :] = widen(wi[dy, dx].astype(F32))
    WI[NS + 12:NS + 13, :] = widen(bi[...].reshape(1, CH).astype(F32))
    get_tw.wait()
    x = temb[...].astype(F32)
    act = (x * jax.nn.sigmoid(x)).astype(BF)
    for l in DUO:
        pr = lax.dot_general(act, TW[l], COLS_DOT, **ACC32)
        EMB[2 * l] = jnp.zeros((NS, CP), F32)
        EMB[2 * l + 1] = widen(pr + tb[l:l + 1, :].astype(F32))
    for Y in (Y0, Y1):
        Y[...] = jnp.zeros_like(Y)
    pl.semaphore_wait(barrier, sp - 1)

    def remote(src, dst, ssem, rsem, dev):
        return pltpu.make_async_remote_copy(src_ref=src, dst_ref=dst, send_sem=ssem, recv_sem=rsem, device_id=(dp, dev), device_id_type=MESH)

    def if_up(f):
        pl.when(me > 0)(f)

    def if_dn(f):
        pl.when(me < sp - 1)(f)

    q_dn = remote(lat.at[:, ROWS - 2:], LQ.at[0], q_send.at[0], q_recv.at[0], me + 1)
    q_up = remote(lat.at[:, :2], LQ.at[1], q_send.at[1], q_recv.at[1], me - 1)
    if_dn(q_dn.start)
    if_up(q_up.start)

    def rows_copies(slot, g, lo, n):
        ss = pl.ds(lo, n)
        down = remote(PB.at[slot - 1, ss], HT.at[slot, ss], dn_send.at[slot, g], ht_recv.at[slot, g], me + 1)
        if slot == end:
            return None, down
        return remote(PT.at[slot - 1, ss], HB.at[slot, ss], up_send.at[slot, g], hb_recv.at[slot, g], me - 1), down

    def out_copy(slot, g, lo, n):
        ss = pl.ds(lo, n)
        return pltpu.make_async_copy(HS.at[ss], hand.at[slot // 2, ss], out_sem.at[slot, g])

    def send_sums(slot, g, lo, n):
        ss = pl.ds(lo, n)
        for k in range(1, sp):
            remote(SG.at[slot, ss], RS.at[slot, k - 1, ss], st_send.at[slot, g], st_recv.at[slot, g], lax.rem(me + k, sp)).start()

    def send_rows(slot, g, lo, n):
        if slot % 2 == 0:
            out_copy(slot, g, lo, n).start()
        if slot > 0:
            up, down = rows_copies(slot, g, lo, n)
            if up is not None:
                if_up(up.start)
            if_dn(down.start)

    def sums_bytes(slot, n, sem, g):
        both = RS.at[slot, :, :n]
        return pltpu.make_async_copy(both, both, sem.at[slot, g])

    def wait_sums(slot, g, n):
        sums_bytes(slot, n, st_recv, g).wait()

    def wait_rows(slot, g, n):
        ss = pl.ds(0, n)
        if_up(lambda: remote(PB.at[0, ss], HT.at[slot, ss], dn_send.at[slot, g], ht_recv.at[slot, g], me).wait_recv())
        if slot is not end:
            if_dn(lambda: remote(PT.at[0, ss], HB.at[slot, ss], up_send.at[slot, g], hb_recv.at[slot, g], me).wait_recv())

    def squeeze(slot, ss, tiles):
        for r, s in zip(compact(tiles, [EMB[slot, pl.ds(s, 1)] for s in ss]), ss):
            SG[slot, s] = r

    if_up(q_dn.wait_recv)
    if_dn(q_up.wait_recv)

    def first(s):
        above, own, below = (x.astype(F32) for x in (LQ[0, s], lat[s], LQ[1, s]))
        rows = [keep_if(has_up, above[k]) for k in DUO] + [own[k] for k in range(ROWS)] + [keep_if(has_dn, below[k]) for k in DUO]
        ext = jnp.concatenate(rows, 1)
        col = lax.broadcasted_iota(jnp.int32, ext.shape, 1) % ROW
        left = jnp.where(col == 0, NIL, pltpu.roll(ext, 1, 1))
        right = jnp.where(col == ROW - 1, NIL, pltpu.roll(ext, ext.shape[1] - 1, 1))
        ext = jnp.concatenate([left, ext, right, jnp.ones_like(ext)], 0)
        mid = pltpu.roll(ext, ext.shape[1] - ROW, 1)
        wide = NP + LANE
        lhs = jnp.concatenate([ext[:, :wide], mid[:, :wide], ext[:, LANE:]], 0).astype(BF)
        r = lax.dot_general(lhs, WI[...].astype(BF), ROWS_DOT, **ACC32)
        acc, acq = no_stats(), no_stats()
        for o in range(ROWS + 2):
            x = r[span(o), :].astype(BF)
            parts = [x[:, span(k, LANE)] for k in TRI]
            if o == 0:
                pack_row(HT.at[0, s], parts)
            elif o > ROWS:
                pack_row(HB.at[0, s], parts)
            else:
                H[s, span(o - 1), :] = x
                HS[s, span(o - 1), :] = x[:, :CH]
                add_stats(acc, acq, parts)
        ST[s] = stats_tile(acc, acq)

    def first_four(i, carry):
        t = SLOTS * i
        for g in TRI:
            pl.when(i == g + 1)(functools.partial(send_rows, 0, g, *EDGES[g]))
        for g in DUO:
            pl.when(i == g + 2)(functools.partial(send_sums, 0, g, *SUMS[g]))
        ss = [lax.rem(t + NS - SLOTS + k, NS) for k in QUAD]
        tiles = [ST[s] for s in ss]
        for k in QUAD:
            first(t + k)
        squeeze(0, ss, tiles)
        return carry

    lax.fori_loop(0, NS // SLOTS, first_four, 0)
    ss = range(NS - SLOTS, NS)
    send_sums(0, 2, *SUMS[2])
    squeeze(0, ss, [ST[s] for s in ss])
    for j in QUAD:
        weight_finish((b1, b2)[j % 2][j // 2:j // 2 + 1, :], W.at[j], WR.at[j], wm_sem.at[j], wr_sem.at[j])
    for g in (3, 4):
        send_sums(0, g, *SUMS[g])
        send_rows(0, g, *EDGES[g])

    def scales(slots, ss):
        tots = []
        for slot, s in zip(slots, ss):
            tots.append(SG[slot, s])
            for k in range(sp - 1):
                tots[-1] = tots[-1] + RS[slot, k, s]
        return affine(tots, [GAIN[pl.ds(k, 1)] for k in slots], [GAIN[pl.ds(k + SLOTS, 1)] for k in slots],
                      [EMB[k, pl.ds(s, 1)] for k, s in zip(slots, ss)], float(sp * NP * GSIZE))

    def prep_of(slot, s, L, a, b):
        def row(r):
            if r == 0:
                return unpack_row(HT.at[slot, s]), has_up
            if r == ROWS + 1:
                return unpack_row(HB.at[slot, s]), has_dn
            return held[slot][s, span(r - 1), :], None
        return prep_gen(row, ROWS, a, b, L)

    def epi_gen(j, s, Y, zero, tiles):
        acc, acq = no_stats(), no_stats()
        edge = {ROWS - 1: PB.at[j, s]}
        if j + 1 < end:
            edge[0] = PT.at[j, s]
        for o in range(ROWS):
            new = [x.astype(BF) for x in conv_row(Y, o, zero)]
            mark = new[2]
            for k in TRI:
                cols = span(k, LANE)
                if j % 2:
                    new[k] = (new[k].astype(F32) + held[j - 1][s, span(o), cols].astype(F32)).astype(BF)
                    cols_out = slice(k * LANE, min(k * LANE + LANE, CH))
                    HS[s, span(o), cols_out] = new[k][:, :cols_out.stop - cols_out.start]
                if j + 1 < end:
                    held[j + 1][s, span(o), cols] = new[k]
            if o in edge:
                pack_row(edge[o], new)
            if j + 1 < end:
                add_stats(acc, acq, new)
            if o == ROWS - 1:
                tiles.append(stats_tile(acc, acq))
            yield mark

    for g in DUO:
        wait_sums(0, g, SUMS[g][1])
    for c, v in enumerate(scales((0,) * 3, TRI)):
        AB[c] = v[:3]
    still = nil(me)
    for _ in prep_of(0, 0, L0, AB[0, :1], AB[1, :1]):
        pass
    for j in QUAD:
        if j % 2:
            for g in range(len(EDGES)):
                out_copy(j - 1, g, *EDGES[g]).wait()

        def body(i, carry, j=j):
            t = 2 * i
            zero = nil(i)
            turn = NS // 2 - 1
            ns = [jnp.minimum(j * NS + t + 3 + k, end * NS - 1) for k in DUO]
            for g in TRI:
                pl.when(i == 2 * g + 1)(functools.partial(wait_sums, j, g + 2, SUMS[g + 2][1]))
            for g in DUO:
                if j + 1 < end:
                    pl.when(i == turn - 1 + g)(functools.partial(wait_sums, j + 1, g, SUMS[g][1]))
            if j > 0:
                for g in TRI:
                    pl.when(i == 2 * g + 1)(functools.partial(wait_rows, j, g + 1, EDGES[g + 1][1]))
                pl.when(i == turn)(functools.partial(wait_rows, j, 4, EDGES[4][1]))
            if j + 1 < end:
                pl.when(i == turn)(functools.partial(wait_rows, j + 1, 0, EDGES[0][1]))
            if j + 1 == end:
                for g, at in enumerate((2, 5, turn)):
                    pl.when(i == at)(functools.partial(send_rows, end, g, *LATE[g]))
            else:
                for parts, send in ((EDGES, send_rows), (SUMS, send_sums)):
                    for g in TRI:
                        pl.when(i == 2 * g + 2)(functools.partial(send, j + 1, g, *parts[g]))
            new = scales([n // NS for n in ns], [lax.rem(n, NS) for n in ns])
            co = [(AB[0, k:k + 1], AB[1, k:k + 1]) for k in (1, 2)]
            tiles = [STC[...]]
            for u, (Lc, Ln, Yc, Yp) in enumerate(((L0, L1, Y0, Y1), (L1, L0, Y1, Y0))):
                nxt = jnp.minimum(t + u + 1, last)
                weave(Lc, W.at[j], Yc, NP, prep_of(j, nxt, Ln, *co[u]), epi_gen(j, lax.rem(t + u + last, NS), Yp, zero, tiles), SHARE)
            for c in DUO:
                AB[c] = jnp.concatenate([co[1][c], new[c][:2]], 0)
            if j + 1 == end:
                return carry
            STC[...] = tiles.pop()
            squeeze(j + 1, [lax.rem(t + last - 1 + k, NS) for k in DUO], tiles)
            return carry

        lax.fori_loop(0, NS // 2, body, 0)
        edges = EDGES if j + 1 < end else LATE
        send_rows(j + 1, 3, *edges[3])
        if j + 1 < end:
            send_sums(j + 1, 3, *SUMS[3])
        tiles = [STC[...]]
        for _ in epi_gen(j, last, Y1, still, tiles):
            pass
        if j + 1 < end:
            for _ in prep_of(j + 1, 0, L0, AB[0, :1], AB[1, :1]):
                pass
            squeeze(j + 1, (last - 1, last), tiles)
            send_sums(j + 1, 4, *SUMS[4])
        send_rows(j + 1, 4, *edges[4])

    fins = []
    for g, (lo, n) in enumerate(LATE):
        wait_rows(end, g, n)
        fins.append(pltpu.make_async_copy(HT.at[end, lo:lo + n], halo.at[lo:lo + n], fin_sem.at[g]))
        fins[-1].start()
    for g in range(len(SUMS)):
        out_copy(end, g, *LATE[g]).wait()
        for slot in QUAD:
            sums_bytes(slot, SUMS[g][1], st_send, g).wait()
            up, down = rows_copies(slot + 1, g, *(EDGES if slot + 1 < end else LATE)[g])
            if up is not None:
                if_up(up.wait_send)
            if_dn(down.wait_send)
    if_dn(q_dn.wait_send)
    if_up(q_up.wait_send)
    for f in fins:
        f.wait()


def tail(hand, halo, bd, dw, h0o, h1o, h2o, do, P0, P1, P2, HA, W, WR, L0, L1, Y0, Y1, OD, DS, in_sem, ha_sem, wm_sem, wr_sem, o_sem, od_sem):
    me = lax.axis_index("sp")
    has_up = (me > 0).astype(jnp.int32)
    held, outs = (P0, P1, P2), (h0o, h1o, h2o)
    ahead = 6

    def take(k, s):
        return pltpu.make_async_copy(hand.at[k, s], held[k].at[s], in_sem.at[k, s])

    def put(k, s):
        return pltpu.make_async_copy(held[k].at[s], outs[k].at[s], o_sem.at[k, s])

    def fetch(s):
        for k in (2, 0, 1):
            take(k, s).start()

    get_halo = pltpu.make_async_copy(halo, HA, ha_sem)
    take(2, 0).start()
    get_halo.start()
    weight_copies(dw, W, WR, wm_sem, wr_sem)
    for k in DUO:
        take(k, 0).start()
    for s in range(1, ahead):
        fetch(s)
    for Y in (Y0, Y1):
        Y[...] = jnp.zeros_like(Y)
    def pass_on(s):
        for k in DUO:
            take(k, s).wait()
            put(k, s).start()

    def dput(s):
        return pltpu.make_async_copy(OD.at[s], do.at[s], od_sem.at[s])

    get_halo.wait()
    take(2, 0).wait()
    still = nil(me)

    def row_of(s, r):
        if r == 0:
            return keep_if(has_up, unpack_row(HA.at[s]))
        return widen(P2[s, span(r - 1), :].astype(F32))

    def dprep(s, L):
        for o in QUAD:
            xs = [row_of(s, 2 * o + dy) for dy in TRI]
            for dy in TRI:
                L[span(o), span(dy, MAIN)] = xs[dy][:, :MAIN].astype(BF)
            store_rest(L, o, *(x[:, MAIN:] for x in xs))

    def depi(s, Y, zero):
        for o in QUAD:
            d = conv_row(Y, o, zero)
            for k in TRI:
                DS[o, k] = d[k]
            parts = [DS[o, k, pl.ds(0, ROW // 2, stride=2), :] for k in TRI]
            OD[s, span(o, ROW // 2), :] = jnp.concatenate(parts, 1)[:, :CH].astype(BF)

    def dhalf(t, Lc, Ln, Yc, Yp, zero):
        for n in QUAD:
            dot_chunk(Lc, W, Yc, slice(0, NP // 2), n)
        dprep(jnp.minimum(t + 1, NS - 1), Ln)
        depi(lax.rem(t + NS - 1, NS), Yp, zero)

    dprep(0, L0)
    weight_finish(bd[...].reshape(1, CH), W, WR, wm_sem, wr_sem)

    def dbody(i, carry):
        t = 2 * i
        zero = nil(i)
        for s in (t, t + 1):
            pl.when(s + ahead < NS)(functools.partial(fetch, s + ahead))
            pl.when(s + 1 < NS)(lambda s=s: take(2, s + 1).wait())
            put(2, s).start()
            pass_on(s)
            pl.when(s > 2)(lambda s=s: dput(s - 3).start())
        dhalf(t, L0, L1, Y0, Y1, zero)
        dhalf(t + 1, L1, L0, Y1, Y0, zero)
        return carry

    lax.fori_loop(0, NS // 2, dbody, 0)
    depi(NS - 1, Y1, still)
    for s in range(NS - 3, NS):
        dput(s).start()

    def drain(s, carry):
        for k in TRI:
            put(k, s).wait()
        dput(s).wait()
        return carry

    lax.fori_loop(0, NS, drain, 0)


def solution(mesh):
    sp = mesh.shape["sp"]

    def program(latent, time_emb, w_in, b_in, gn1_scale, gn1_shift, conv1_w, conv1_b, temb_w, temb_b, gn2_scale, gn2_shift, conv2_w, conv2_b, down_w, down_b):
        dma, vm = pltpu.SemaphoreType.DMA, pltpu.VMEM
        any_, vms = pl.BlockSpec(memory_space=pl.ANY), pl.BlockSpec(memory_space=pltpu.VMEM)
        params = functools.partial(pltpu.CompilerParams, vmem_limit_bytes=66_000_000)

        def big(n=NP, c=CP):
            return vm((NS, n, c), BF)

        def edge(n):
            return vm((n, NS, PK, MAIN), BF)

        def bufs(m):
            return [vm((m, KP), BF)] * 2 + [vm((8, m + 2 * OFF, LANE), F32)] * 2

        def out(*shape):
            return jax.ShapeDtypeStruct(shape, BF)

        hand, halo = pl.pallas_call(
            functools.partial(mega, sp),
            out_shape=(out(3, NS, NP, CH), out(NS, PK, MAIN)),
            in_specs=[vms] * 11 + [any_] * 3, out_specs=(any_, any_),
            scratch_shapes=[big(), big(), big(), big(NP, CH), vm((SLOTS, KP, KP), BF), vm((SLOTS, 9, CH, ROW), BF), vm((2, CH, temb_w.shape[1]), BF), vm((3 * NS, CP), F32)] + bufs(NP)
            + [vm((NS, OFF, LANE), F32), vm((OFF, LANE), F32), vm((SLOTS, NS, 2, LANE), F32), vm((SLOTS, sp - 1, NS, 2, LANE), F32), vm((2, 3, CP), F32), vm((SLOTS, NS, CP), F32), vm((OFF, CP), F32),
               edge(SLOTS + 1), edge(SLOTS), edge(SLOTS - 1), edge(SLOTS), vm((2, NS, 2, 4, ROW), BF),
               dma((SLOTS,)), dma((SLOTS,)), dma] + [dma((2,))] * 2 + [dma((SLOTS + 1, len(SUMS)))] * 7 + [dma((len(SUMS),))],
            compiler_params=params(collective_id=0, has_side_effects=True), name="mega",
        )(latent.transpose(0, 1, 3, 2), w_in, b_in, time_emb, temb_b, gn1_scale, gn1_shift, gn2_scale, gn2_shift, conv1_b, conv2_b, temb_w.transpose(0, 2, 1), conv1_w, conv2_w)
        outs = pl.pallas_call(
            tail,
            out_shape=(out(NS, NP, CH),) * 3 + (out(NS, NP // 4, CH),),
            in_specs=[any_] * 2 + [vms, any_], out_specs=(any_,) * 4,
            scratch_shapes=[big(NP, CH)] * 3 + [big(PK, MAIN), vm((KP, KP), BF), vm((9, CH, ROW), BF)] + bufs(NP // 2)
            + [big(NP // 4, CH), vm((4, 3, ROW, LANE), F32), dma((3, NS)), dma, dma, dma, dma((3, NS)), dma((NS,))],
            compiler_params=params(), name="tail",
        )(hand, halo, down_b, down_w)
        return tuple(o.reshape(NS, n, m, CH) for o, n, m in zip(outs, [ROWS] * len(TRI) + [ROWS // 2], [ROW] * len(TRI) + [ROW // 2]))

    band = P("dp", "sp", None, None)
    return jax.shard_map(program, mesh=mesh, in_specs=(band, P("dp", None)) + (P(),) * 14, out_specs=(band,) * 4, check_vma=False)
```

```python
import functools

import jax
import jax.numpy as jnp
from jax import lax
from jax.experimental import pallas as pl
from jax.experimental.pallas import tpu as pltpu
from jax.sharding import PartitionSpec as P

F32, BF = jnp.float32, jnp.bfloat16
GN_GROUPS, GN_EPS = 32, 1e-5
NS, ROWS, ROW, LANE, MAIN = 16, 8, 64, 128, 256
NP = ROWS * ROW
CH = 320
CP = CH + ROW
KP = 4 * MAIN
REST = 3 * MAIN
SPARE = 3 * CH
OFF = 8
GSIZE = CH // GN_GROUPS
PK = ROW + NS
MESH = pl.DeviceIdType.MESH
DUO, TRI, QUAD = range(2), range(3), range(4)
SLOTS = len(QUAD)
NIL = 0.0


def groups(n, step):
    cuts = [0, *range(n, NS, step), NS]
    return [(a, b - a) for a, b in zip(cuts, cuts[1:])]


SUMS, EDGES = groups(2, SLOTS), groups(3, SLOTS)
LATE = [(0, 3), (3, 6), (9, 4), (13, 2), (15, 1)]
SHARE = (1, 2, 3, 3)
ACC32 = dict(preferred_element_type=F32)
ROWS_DOT, COLS_DOT = ((((k,), (k,)), ((), ())) for k in DUO)


def nil(i):
    return jnp.minimum(i, 0) * OFF


def span(i, n=ROW, base=0):
    return slice(base + i * n, base + (i + 1) * n)


def low_half():
    return lax.broadcasted_iota(jnp.int32, (ROW, LANE), 1) < ROW


def widen(p):
    return jnp.concatenate([p, p[..., MAIN:]], -1)


def keep_if(flag, x):
    return jnp.where(jnp.full(x.shape, flag, jnp.int32) > 0, x, NIL)


def store_rest(L, o, r0, r1, r2):
    low = low_half()
    L[span(o), REST:REST + LANE] = jnp.where(low, r0, r1).astype(BF)
    L[span(o), REST + LANE:] = jnp.where(low, r2, 1.0).astype(BF)


def prep_gen(x_of_row, nrows, a, b, L):
    ha, hb = a * 0.5, b * 0.5
    rest = []
    for r in range(nrows + 2):
        x, flag = x_of_row(r)
        h = x.astype(F32) * ha + hb
        n = h + h * jnp.tanh(h)
        if flag is not None:
            n = keep_if(flag, n)
        main = n[:, :MAIN].astype(BF)
        rest.append(n[:, MAIN:])
        for dy in TRI:
            if 0 <= r - dy < nrows:
                L[span(r - dy), span(dy, MAIN)] = main
        if r >= 2:
            store_rest(L, r - 2, *rest[r - 2:])
        yield main


def shifted(v, step):
    v = pltpu.roll(v.reshape(OFF, OFF, LANE), step % OFF, 1)
    sub = lax.broadcasted_iota(jnp.int32, v.shape, 1)
    gap = jnp.zeros_like(v[:1])
    if step > 0:
        v = jnp.where(sub == 0, jnp.concatenate([gap, v[:-1]], 0), v)
    else:
        v = jnp.where(sub == OFF - 1, jnp.concatenate([v[1:], gap], 0), v)
    return v.reshape(ROW, LANE)


def conv_row(Y, o, zero):
    def here(k):
        return Y[k, span(o, base=OFF), :]

    out = [shifted(here(k), 1) + here(k + 2) + shifted(here(k + 4), -1) for k in DUO]
    a = here(6)
    mix = jnp.where(low_half(), shifted(a, 1), a)
    return out + [mix + pltpu.roll(mix, ROW, 1) + shifted(here(7), -1)]


def dot_chunk(L, W, Y, rows, n):
    r = jnp.dot(L[rows, :], W[:, span(n, MAIN)], **ACC32)
    for k in DUO:
        Y[2 * n + k, OFF + rows.start:OFF + rows.stop, :] = r[:, span(k, LANE)]


def weave(L, W, Y, m, prep, epi, share):
    work = [prep] * (m // ROW + 2) + [epi] * (m // ROW)
    done = 0
    for n in QUAD:
        dot_chunk(L, W, Y, slice(0, m), n)
        upto = len(work) * share[n] // share[-1]
        for g in work[done:upto]:
            mark = next(g)
        done = upto
        if n < len(QUAD) - 1:
            L[:NS, KP - NS:] = jnp.where(mark[:NS, LANE - NS:LANE].astype(F32) > NIL, 1.0, NIL).astype(BF)
    for g in (prep, epi):
        for _ in g:
            pass


def lane_left(x, k):
    return pltpu.roll(x, CP - k, 1)


def starts(k):
    lane = lax.broadcasted_iota(jnp.int32, (OFF, LANE), 1) + k * LANE
    return (lane % GSIZE == 0) & (lane < CH)


def stacked(rows):
    fill = [jnp.zeros((4 - len(rows), rows[0].shape[1]), F32)] * (len(rows) < 4)
    return jnp.concatenate(list(rows) + fill, 0)


def compact(tiles, embs):
    s = stacked([jnp.concatenate([t[k:k + 1] for k in TRI], 1) for t in tiles])
    q = stacked([jnp.concatenate([t[k + 3:k + 4] for k in TRI], 1) for t in tiles])
    e = stacked(embs)
    x = jnp.concatenate([s + float(NP) * e, q + e * (2.0 * s + float(NP) * e)], 0)
    w2 = x + lane_left(x, 1)
    w4 = w2 + lane_left(w2, 2)
    w8 = w4 + lane_left(w4, 4)
    w10 = w8 + lane_left(w2, 8)
    c = sum(jnp.where(starts(k), w10[:, span(k, LANE)], NIL) for k in TRI)
    return [jnp.concatenate([c[k:k + 1], c[k + 4:k + 5]], 0) for k in range(len(tiles))]


def affine(tots, gains, shifts, embs, count):
    x = jnp.concatenate([stacked([t[k:k + 1] for t in tots]) for k in DUO], 0)
    y = jnp.concatenate([jnp.where(starts(k), x, NIL) for k in TRI], 1)
    r2 = y + pltpu.roll(y, 1, 1)
    r4 = r2 + pltpu.roll(r2, 2, 1)
    r8 = r4 + pltpu.roll(r4, 4, 1)
    r = r8 + pltpu.roll(r2, 8, 1)
    lane = lax.broadcasted_iota(jnp.int32, (OFF, CP), 1)
    r = jnp.where(lane >= CH, pltpu.roll(r, ROW, 1), r) * (1.0 / count)
    mean, msq = r[:4], r[4:]
    a = stacked(gains) * lax.rsqrt(msq - mean * mean + GN_EPS)
    return a, stacked(shifts) + a * (stacked(embs) - mean)


def pack_row(dst, x):
    dst[:ROW, :] = jnp.concatenate(x[:2], 1)
    half = ROW // 2
    p = jnp.where(low_half()[:half], x[2][:half].astype(F32), x[2][half:].astype(F32))
    dst[ROW:, :] = jnp.concatenate([p[:NS], p[NS:]], 1).astype(BF)


def unpack_row(src):
    p = src[ROW:, :].astype(F32)
    p = jnp.concatenate([p[:, :LANE], p[:, LANE:]], 0)
    swap, low = pltpu.roll(p, ROW, 1), low_half()[:ROW // 2]
    rest = jnp.concatenate([jnp.where(low, p, swap), jnp.where(low, swap, p)], 0)
    return jnp.concatenate([src[:ROW, :].astype(F32), rest], 1)


def stats_tile(acc, acq):
    parts = [x.sum(0, keepdims=True) for x in acc + acq]
    return jnp.concatenate(parts + [jnp.zeros((2, LANE), F32)], 0)


def add_stats(acc, acq, new):
    for k, x in enumerate(new):
        v = x.astype(F32).reshape(OFF, OFF, LANE)
        acc[k] = acc[k] + v.sum(0)
        acq[k] = acq[k] + (v * v).sum(0)


def no_stats():
    return [jnp.zeros((OFF, LANE), F32) for _ in TRI]


def weight_copies(src, W, WR, sem_main, sem_rest):
    for dy in TRI:
        for dx in TRI:
            cols = span(dx, MAIN)
            pltpu.make_async_copy(src.at[dy, dx, :MAIN, :MAIN], W.at[span(dy, MAIN), cols], sem_main).start()
            pltpu.make_async_copy(src.at[dy, dx, MAIN:, :MAIN], W.at[span(dy, base=REST), cols], sem_main).start()
            pltpu.make_async_copy(src.at[dy, dx, :, MAIN:], WR.at[dy * 3 + dx], sem_rest).start()


def weight_finish(bias, W, WR, sem_main, sem_rest):
    main = W.at[:SPARE, :REST]
    pltpu.make_async_copy(main, main, sem_main).wait()
    pltpu.make_async_copy(WR, WR, sem_rest).wait()
    for dy in TRI:
        for part, rows in ((slice(0, MAIN), span(dy, MAIN)), (slice(MAIN, CH), span(dy, base=REST))):
            w0, w1, w2 = (WR[dy * 3 + dx, part, :] for dx in TRI)
            W[rows, REST:REST + LANE] = jnp.concatenate([w0, w1], 1)
            W[rows, REST + LANE:] = jnp.concatenate([w2, w2], 1)
    b = widen(bias.astype(F32))
    gap = jnp.zeros((1, MAIN), F32)
    rest = jnp.where(low_half()[:1], 0.0, b[:, MAIN:])
    row = jnp.concatenate([gap, b[:, :MAIN], gap, rest, gap[:, :LANE]], 1)
    first = lax.broadcasted_iota(jnp.int32, (ROW, KP), 0) == 0
    W[SPARE:, :] = jnp.where(first, row, NIL).astype(BF)


def mega(sp, lat, wi, bi, temb, tb, g1, s1, g2, s2, b1, b2, tw, w1, w2, hand, halo,
         H, U, H2, HS, W, WR, TW, WI, L0, L1, Y0, Y1, ST, STC, SG, RS, AB, EMB, GAIN, HT, HB, PT, PB, LQ,
         wm_sem, wr_sem, tw_sem, q_send, q_recv, st_send, st_recv, up_send, dn_send, ht_recv, hb_recv, out_sem, fin_sem):
    me, dp = lax.axis_index("sp"), lax.axis_index("dp")
    has_up, has_dn = (me > 0).astype(jnp.int32), (me < sp - 1).astype(jnp.int32)
    held = (H, U, H2, U)
    end = SLOTS
    last = NS - 1

    get_tw = pltpu.make_async_copy(tw, TW, tw_sem)
    get_tw.start()
    for j, src in enumerate((w1.at[0], w2.at[0], w1.at[1], w2.at[1])):
        weight_copies(src, W.at[j], WR.at[j], wm_sem.at[j], wr_sem.at[j])

    barrier = pltpu.get_barrier_semaphore()
    for k in range(1, sp):
        pl.semaphore_signal(barrier, inc=1, device_id=(dp, lax.rem(me + k, sp)), device_id_type=MESH)
    for k, (ref, l) in enumerate((ref, l) for pair in ((g1, g2), (s1, s2)) for l in DUO for ref in pair):
        GAIN[k:k + 1, :] = widen(ref[l:l + 1, :].astype(F32))
    WI[...] = jnp.zeros_like(WI)
    for dy in TRI:
        for dx in TRI:
            WI[span(4 * dy + dx, 4), :] = widen(wi[dy, dx].astype(F32))
    WI[NS + 12:NS + 13, :] = widen(bi[...].reshape(1, CH).astype(F32))
    get_tw.wait()
    x = temb[...].astype(F32)
    act = (x * jax.nn.sigmoid(x)).astype(BF)
    for l in DUO:
        pr = lax.dot_general(act, TW[l], COLS_DOT, **ACC32)
        EMB[2 * l] = jnp.zeros((NS, CP), F32)
        EMB[2 * l + 1] = widen(pr + tb[l:l + 1, :].astype(F32))
    for Y in (Y0, Y1):
        Y[...] = jnp.zeros_like(Y)
    pl.semaphore_wait(barrier, sp - 1)

    def remote(src, dst, ssem, rsem, dev):
        return pltpu.make_async_remote_copy(src_ref=src, dst_ref=dst, send_sem=ssem, recv_sem=rsem, device_id=(dp, dev), device_id_type=MESH)

    def if_up(f):
        pl.when(me > 0)(f)

    def if_dn(f):
        pl.when(me < sp - 1)(f)

    q_dn = remote(lat.at[:, ROWS - 2:], LQ.at[0], q_send.at[0], q_recv.at[0], me + 1)
    q_up = remote(lat.at[:, :2], LQ.at[1], q_send.at[1], q_recv.at[1], me - 1)
    if_dn(q_dn.start)
    if_up(q_up.start)

    def rows_copies(slot, g, lo, n):
        ss = pl.ds(lo, n)
        down = remote(PB.at[slot - 1, ss], HT.at[slot, ss], dn_send.at[slot, g], ht_recv.at[slot, g], me + 1)
        if slot == end:
            return None, down
        return remote(PT.at[slot - 1, ss], HB.at[slot, ss], up_send.at[slot, g], hb_recv.at[slot, g], me - 1), down

    def out_copy(slot, g, lo, n):
        ss = pl.ds(lo, n)
        return pltpu.make_async_copy(HS.at[ss], hand.at[slot // 2, ss], out_sem.at[slot, g])

    def send_sums(slot, g, lo, n):
        ss = pl.ds(lo, n)
        for k in range(1, sp):
            remote(SG.at[slot, ss], RS.at[slot, k - 1, ss], st_send.at[slot, g], st_recv.at[slot, g], lax.rem(me + k, sp)).start()

    def send_rows(slot, g, lo, n):
        if slot % 2 == 0:
            out_copy(slot, g, lo, n).start()
        if slot > 0:
            up, down = rows_copies(slot, g, lo, n)
            if up is not None:
                if_up(up.start)
            if_dn(down.start)

    def sums_bytes(slot, n, sem, g):
        both = RS.at[slot, :, :n]
        return pltpu.make_async_copy(both, both, sem.at[slot, g])

    def wait_sums(slot, g, n):
        sums_bytes(slot, n, st_recv, g).wait()

    def wait_rows(slot, g, n):
        ss = pl.ds(0, n)
        if_up(lambda: remote(PB.at[0, ss], HT.at[slot, ss], dn_send.at[slot, g], ht_recv.at[slot, g], me).wait_recv())
        if slot is not end:
            if_dn(lambda: remote(PT.at[0, ss], HB.at[slot, ss], up_send.at[slot, g], hb_recv.at[slot, g], me).wait_recv())

    def squeeze(slot, ss, tiles):
        for r, s in zip(compact(tiles, [EMB[slot, pl.ds(s, 1)] for s in ss]), ss):
            SG[slot, s] = r

    if_up(q_dn.wait_recv)
    if_dn(q_up.wait_recv)

    def first(s):
        above, own, below = (x.astype(F32) for x in (LQ[0, s], lat[s], LQ[1, s]))
        rows = [keep_if(has_up, above[k]) for k in DUO] + [own[k] for k in range(ROWS)] + [keep_if(has_dn, below[k]) for k in DUO]
        ext = jnp.concatenate(rows, 1)
        col = lax.broadcasted_iota(jnp.int32, ext.shape, 1) % ROW
        left = jnp.where(col == 0, NIL, pltpu.roll(ext, 1, 1))
        right = jnp.where(col == ROW - 1, NIL, pltpu.roll(ext, ext.shape[1] - 1, 1))
        ext = jnp.concatenate([left, ext, right, jnp.ones_like(ext)], 0)
        mid = pltpu.roll(ext, ext.shape[1] - ROW, 1)
        wide = NP + LANE
        lhs = jnp.concatenate([ext[:, :wide], mid[:, :wide], ext[:, LANE:]], 0).astype(BF)
        r = lax.dot_general(lhs, WI[...].astype(BF), ROWS_DOT, **ACC32)
        acc, acq = no_stats(), no_stats()
        for o in range(ROWS + 2):
            x = r[span(o), :].astype(BF)
            parts = [x[:, span(k, LANE)] for k in TRI]
            if o == 0:
                pack_row(HT.at[0, s], parts)
            elif o > ROWS:
                pack_row(HB.at[0, s], parts)
            else:
                H[s, span(o - 1), :] = x
                HS[s, span(o - 1), :] = x[:, :CH]
                add_stats(acc, acq, parts)
        ST[s] = stats_tile(acc, acq)

    def first_four(i, carry):
        t = SLOTS * i
        for g in TRI:
            pl.when(i == g + 1)(functools.partial(send_rows, 0, g, *EDGES[g]))
        for g in DUO:
            pl.when(i == g + 2)(functools.partial(send_sums, 0, g, *SUMS[g]))
        ss = [lax.rem(t + NS - SLOTS + k, NS) for k in QUAD]
        tiles = [ST[s] for s in ss]
        for k in QUAD:
            first(t + k)
        squeeze(0, ss, tiles)
        return carry

    lax.fori_loop(0, NS // SLOTS, first_four, 0)
    ss = range(NS - SLOTS, NS)
    send_sums(0, 2, *SUMS[2])
    squeeze(0, ss, [ST[s] for s in ss])
    for j in QUAD:
        weight_finish((b1, b2)[j % 2][j // 2:j // 2 + 1, :], W.at[j], WR.at[j], wm_sem.at[j], wr_sem.at[j])
    for g in (3, 4):
        send_sums(0, g, *SUMS[g])
        send_rows(0, g, *EDGES[g])

    def scales(slots, ss):
        tots = []
        for slot, s in zip(slots, ss):
            tots.append(SG[slot, s])
            for k in range(sp - 1):
                tots[-1] = tots[-1] + RS[slot, k, s]
        return affine(tots, [GAIN[pl.ds(k, 1)] for k in slots], [GAIN[pl.ds(k + SLOTS, 1)] for k in slots],
                      [EMB[k, pl.ds(s, 1)] for k, s in zip(slots, ss)], float(sp * NP * GSIZE))

    def prep_of(slot, s, L, a, b):
        def row(r):
            if r == 0:
                return unpack_row(HT.at[slot, s]), has_up
            if r == ROWS + 1:
                return unpack_row(HB.at[slot, s]), has_dn
            return held[slot][s, span(r - 1), :], None
        return prep_gen(row, ROWS, a, b, L)

    def epi_gen(j, s, Y, zero, tiles):
        acc, acq = no_stats(), no_stats()
        edge = {ROWS - 1: PB.at[j, s]}
        if j + 1 < end:
            edge[0] = PT.at[j, s]
        for o in range(ROWS):
            new = [x.astype(BF) for x in conv_row(Y, o, zero)]
            mark = new[2]
            for k in TRI:
                cols = span(k, LANE)
                if j % 2:
                    new[k] = (new[k].astype(F32) + held[j - 1][s, span(o), cols].astype(F32)).astype(BF)
                    cols_out = slice(k * LANE, min(k * LANE + LANE, CH))
                    HS[s, span(o), cols_out] = new[k][:, :cols_out.stop - cols_out.start]
                if j + 1 < end:
                    held[j + 1][s, span(o), cols] = new[k]
            if o in edge:
                pack_row(edge[o], new)
            if j + 1 < end:
                add_stats(acc, acq, new)
            if o == ROWS - 1:
                tiles.append(stats_tile(acc, acq))
            yield mark

    for g in DUO:
        wait_sums(0, g, SUMS[g][1])
    for c, v in enumerate(scales((0,) * 3, TRI)):
        AB[c] = v[:3]
    still = nil(me)
    for _ in prep_of(0, 0, L0, AB[0, :1], AB[1, :1]):
        pass
    for j in QUAD:
        if j % 2:
            for g in range(len(EDGES)):
                out_copy(j - 1, g, *EDGES[g]).wait()

        def body(i, carry, j=j):
            t = 2 * i
            zero = nil(i)
            turn = NS // 2 - 1
            ns = [jnp.minimum(j * NS + t + 3 + k, end * NS - 1) for k in DUO]
            for g in TRI:
                pl.when(i == 2 * g + 1)(functools.partial(wait_sums, j, g + 2, SUMS[g + 2][1]))
            for g in DUO:
                if j + 1 < end:
                    pl.when(i == turn - 1 + g)(functools.partial(wait_sums, j + 1, g, SUMS[g][1]))
            if j > 0:
                for g in TRI:
                    pl.when(i == 2 * g + 1)(functools.partial(wait_rows, j, g + 1, EDGES[g + 1][1]))
                pl.when(i == turn)(functools.partial(wait_rows, j, 4, EDGES[4][1]))
            if j + 1 < end:
                pl.when(i == turn)(functools.partial(wait_rows, j + 1, 0, EDGES[0][1]))
            if j + 1 == end:
                for g, at in enumerate((2, 5, turn)):
                    pl.when(i == at)(functools.partial(send_rows, end, g, *LATE[g]))
            else:
                for parts, send in ((EDGES, send_rows), (SUMS, send_sums)):
                    for g in TRI:
                        pl.when(i == 2 * g + 2)(functools.partial(send, j + 1, g, *parts[g]))
            new = scales([n // NS for n in ns], [lax.rem(n, NS) for n in ns])
            co = [(AB[0, k:k + 1], AB[1, k:k + 1]) for k in (1, 2)]
            tiles = [STC[...]]
            for u, (Lc, Ln, Yc, Yp) in enumerate(((L0, L1, Y0, Y1), (L1, L0, Y1, Y0))):
                nxt = jnp.minimum(t + u + 1, last)
                weave(Lc, W.at[j], Yc, NP, prep_of(j, nxt, Ln, *co[u]), epi_gen(j, lax.rem(t + u + last, NS), Yp, zero, tiles), SHARE)
            for c in DUO:
                AB[c] = jnp.concatenate([co[1][c], new[c][:2]], 0)
            if j + 1 == end:
                return carry
            STC[...] = tiles.pop()
            squeeze(j + 1, [lax.rem(t + last - 1 + k, NS) for k in DUO], tiles)
            return carry

        lax.fori_loop(0, NS // 2, body, 0)
        edges = EDGES if j + 1 < end else LATE
        send_rows(j + 1, 3, *edges[3])
        if j + 1 < end:
            send_sums(j + 1, 3, *SUMS[3])
        tiles = [STC[...]]
        for _ in epi_gen(j, last, Y1, still, tiles):
            pass
        if j + 1 < end:
            for _ in prep_of(j + 1, 0, L0, AB[0, :1], AB[1, :1]):
                pass
            squeeze(j + 1, (last - 1, last), tiles)
            send_sums(j + 1, 4, *SUMS[4])
        send_rows(j + 1, 4, *edges[4])

    fins = []
    for g, (lo, n) in enumerate(LATE):
        wait_rows(end, g, n)
        fins.append(pltpu.make_async_copy(HT.at[end, lo:lo + n], halo.at[lo:lo + n], fin_sem.at[g]))
        fins[-1].start()
    for g in range(len(SUMS)):
        out_copy(end, g, *LATE[g]).wait()
        for slot in QUAD:
            sums_bytes(slot, SUMS[g][1], st_send, g).wait()
            up, down = rows_copies(slot + 1, g, *(EDGES if slot + 1 < end else LATE)[g])
            if up is not None:
                if_up(up.wait_send)
            if_dn(down.wait_send)
    if_dn(q_dn.wait_send)
    if_up(q_up.wait_send)
    for f in fins:
        f.wait()


def tail(hand, halo, bd, dw, h0o, h1o, h2o, do, P0, P1, P2, HA, W, WR, L0, L1, Y0, Y1, OD, DS, in_sem, ha_sem, wm_sem, wr_sem, o_sem, od_sem):
    me = lax.axis_index("sp")
    has_up = (me > 0).astype(jnp.int32)
    held, outs = (P0, P1, P2), (h0o, h1o, h2o)
    ahead = 6

    def take(k, s):
        return pltpu.make_async_copy(hand.at[k, s], held[k].at[s], in_sem.at[k, s])

    def put(k, s):
        return pltpu.make_async_copy(held[k].at[s], outs[k].at[s], o_sem.at[k, s])

    def fetch(s):
        for k in (2, 0, 1):
            take(k, s).start()

    get_halo = pltpu.make_async_copy(halo, HA, ha_sem)
    take(2, 0).start()
    get_halo.start()
    weight_copies(dw, W, WR, wm_sem, wr_sem)
    for k in DUO:
        take(k, 0).start()
    for s in range(1, ahead):
        fetch(s)
    for Y in (Y0, Y1):
        Y[...] = jnp.zeros_like(Y)
    get_halo.wait()
    take(2, 0).wait()
    still = nil(me)

    def row_of(s, r):
        if r == 0:
            return keep_if(has_up, unpack_row(HA.at[s]))
        return widen(P2[s, span(r - 1), :].astype(F32))

    def dprep(s, L):
        for o in QUAD:
            xs = [row_of(s, 2 * o + dy) for dy in TRI]
            for dy in TRI:
                L[span(o), span(dy, MAIN)] = xs[dy][:, :MAIN].astype(BF)
            store_rest(L, o, *(x[:, MAIN:] for x in xs))

    def depi(s, Y, zero):
        for o in QUAD:
            d = conv_row(Y, o, zero)
            for k in TRI:
                DS[o, k] = d[k]
            parts = [DS[o, k, pl.ds(0, ROW // 2, stride=2), :] for k in TRI]
            OD[s, span(o, ROW // 2), :] = jnp.concatenate(parts, 1)[:, :CH].astype(BF)

    def dhalf(t, Lc, Ln, Yc, Yp, zero):
        for n in QUAD:
            dot_chunk(Lc, W, Yc, slice(0, NP // 2), n)
        dprep(jnp.minimum(t + 1, NS - 1), Ln)
        depi(lax.rem(t + NS - 1, NS), Yp, zero)

    dprep(0, L0)
    weight_finish(bd[...].reshape(1, CH), W, WR, wm_sem, wr_sem)

    def dbody(i, carry):
        t = 2 * i
        zero = nil(i)
        for s in (t, t + 1):
            pl.when(s + ahead < NS)(functools.partial(fetch, s + ahead))
            pl.when(s + 1 < NS)(lambda s=s: take(2, s + 1).wait())
            put(2, s).start()
            for k in DUO:
                take(k, s).wait()
                put(k, s).start()
        dhalf(t, L0, L1, Y0, Y1, zero)
        dhalf(t + 1, L1, L0, Y1, Y0, zero)
        return carry

    lax.fori_loop(0, NS // 2, dbody, 0)
    depi(NS - 1, Y1, still)
    dout = pltpu.make_async_copy(OD, do, od_sem)
    dout.start()

    def drain(s, carry):
        for k in TRI:
            put(k, s).wait()
        return carry

    lax.fori_loop(0, NS, drain, 0)
    dout.wait()


def solution(mesh):
    sp = mesh.shape["sp"]

    def program(latent, time_emb, w_in, b_in, gn1_scale, gn1_shift, conv1_w, conv1_b, temb_w, temb_b, gn2_scale, gn2_shift, conv2_w, conv2_b, down_w, down_b):
        dma, vm = pltpu.SemaphoreType.DMA, pltpu.VMEM
        any_, vms = pl.BlockSpec(memory_space=pl.ANY), pl.BlockSpec(memory_space=pltpu.VMEM)
        params = functools.partial(pltpu.CompilerParams, vmem_limit_bytes=66_000_000)

        def big(n=NP, c=CP):
            return vm((NS, n, c), BF)

        def edge(n):
            return vm((n, NS, PK, MAIN), BF)

        def bufs(m):
            return [vm((m, KP), BF)] * 2 + [vm((8, m + 2 * OFF, LANE), F32)] * 2

        def out(*shape):
            return jax.ShapeDtypeStruct(shape, BF)

        hand, halo = pl.pallas_call(
            functools.partial(mega, sp),
            out_shape=(out(3, NS, NP, CH), out(NS, PK, MAIN)),
            in_specs=[vms] * 11 + [any_] * 3, out_specs=(any_, any_),
            scratch_shapes=[big(), big(), big(), big(NP, CH), vm((SLOTS, KP, KP), BF), vm((SLOTS, 9, CH, ROW), BF), vm((2, CH, temb_w.shape[1]), BF), vm((3 * NS, CP), F32)] + bufs(NP)
            + [vm((NS, OFF, LANE), F32), vm((OFF, LANE), F32), vm((SLOTS, NS, 2, LANE), F32), vm((SLOTS, sp - 1, NS, 2, LANE), F32), vm((2, 3, CP), F32), vm((SLOTS, NS, CP), F32), vm((OFF, CP), F32),
               edge(SLOTS + 1), edge(SLOTS), edge(SLOTS - 1), edge(SLOTS), vm((2, NS, 2, 4, ROW), BF),
               dma((SLOTS,)), dma((SLOTS,)), dma] + [dma((2,))] * 2 + [dma((SLOTS + 1, len(SUMS)))] * 7 + [dma((len(SUMS),))],
            compiler_params=params(collective_id=0, has_side_effects=True), name="mega",
        )(latent.transpose(0, 1, 3, 2), w_in, b_in, time_emb, temb_b, gn1_scale, gn1_shift, gn2_scale, gn2_shift, conv1_b, conv2_b, temb_w.transpose(0, 2, 1), conv1_w, conv2_w)
        outs = pl.pallas_call(
            tail,
            out_shape=(out(NS, NP, CH),) * 3 + (out(NS, NP // 4, CH),),
            in_specs=[any_] * 2 + [vms, any_], out_specs=(any_,) * 4,
            scratch_shapes=[big(NP, CH)] * 3 + [big(PK, MAIN), vm((KP, KP), BF), vm((9, CH, ROW), BF)] + bufs(NP // 2)
            + [big(NP // 4, CH), vm((4, 3, ROW, LANE), F32), dma((3, NS)), dma, dma, dma, dma((3, NS)), dma],
            compiler_params=params(), name="tail",
        )(hand, halo, down_b, down_w)
        return tuple(o.reshape(NS, n, m, CH) for o, n, m in zip(outs, [ROWS] * len(TRI) + [ROWS // 2], [ROW] * len(TRI) + [ROW // 2]))

    band = P("dp", "sp", None, None)
    return jax.shard_map(program, mesh=mesh, in_specs=(band, P("dp", None)) + (P(),) * 14, out_specs=(band,) * 4, check_vma=False)
```
